32 devices in a mesh: dp: 1 (over z), ri: 4 (over y), co: 4 (over x), ro: 2 (over core).
Axes of the slice: x: 4, y: 4, z: 1, core: 2. Of those that a mesh axis runs over, the one named last changes fastest.
The devices are a block of a 4x4x8 slice.
Arguments:
- x_act: bfloat16 [16384, 4096], P(('dp', 'ro', 'ri'), 'co')
- w_proj: bfloat16 [4096, 14336], P(('ro', 'ri'), 'co')
- grad_out: bfloat16 [16384, 14336], P(('dp', 'ro', 'ri'), 'co')
Outputs:
- output 1: bfloat16 [16384, 4096], P(('dp', 'ro', 'ri'), 'co')
- output 2: float32 [4096, 14336], P(('dp', 'ro', 'ri'), 'co')
All inputs are finite; a program needn't handle non-finite values.
Results may differ from the reference program's by a relative error of at most 0.001.
Values are sent between devices in bfloat16 or wider.
A program may use at most 768 MiB of HBM per device.

```python
import jax
import jax.numpy as jnp

MODEL_DIM = 4096
FFN_DIM = 14336
TOK_PART = 16384


def setup_inputs(seed: int = 0, part: int = 0) -> dict:
    base_key = jax.random.key(seed)
    key_w, key_rest = jax.random.split(base_key)
    part_key = jax.random.fold_in(key_rest, part)
    key_x, key_g = jax.random.split(part_key)
    act_scale = TOK_PART ** -0.25
    w_scale = TOK_PART ** 0.25 * FFN_DIM ** -0.5
    x_act = (jax.random.normal(key_x, (TOK_PART, MODEL_DIM), jnp.float32) * act_scale).astype(jnp.bfloat16)
    w_proj = (jax.random.normal(key_w, (MODEL_DIM, FFN_DIM), jnp.float32) * w_scale).astype(jnp.bfloat16)
    grad_out = (jax.random.normal(key_g, (TOK_PART, FFN_DIM), jnp.float32) * act_scale).astype(jnp.bfloat16)
    return {"x_act": x_act, "w_proj": w_proj, "grad_out": grad_out}


def reference(x_act, w_proj, grad_out):
    grad_x = jnp.dot(grad_out, w_proj.T, preferred_element_type=jnp.float32).astype(jnp.bfloat16)
    grad_w = jnp.dot(x_act.T, grad_out, preferred_element_type=jnp.float32)
    return grad_x, grad_w
```

```python
import functools

import jax
import jax.numpy as jnp
from jax import lax
from jax.experimental import pallas as pl
from jax.experimental.pallas import tpu as pltpu
from jax.sharding import PartitionSpec as P

MESH = pl.DeviceIdType.MESH
BF16, F32 = jnp.bfloat16, jnp.float32
NC = 8


def kernel(x, w, g, dx, dw, pp, qq, xa, rx, ry, gv, wv,
           loc, d2d, dr, wr, xr, swd, swf, sxd, sxf, sx, rxs, sy, rys, fxs, fxr, fys, fyr, pos, qos, ins, ads):
    h, y, c = lax.axis_index("ro"), lax.axis_index("ri"), lax.axis_index("co")
    o = 1 - h
    tb, dcols = x.shape
    wrows, f = w.shape
    q = wrows // 2
    cr, qr = tb // NC, q // NC
    ft = f // 7
    yn = [lax.rem(y + 1, 4), lax.rem(y + 3, 4)]
    cn = [lax.rem(c + 1, 4), lax.rem(c + 3, 4)]
    y2, c2 = lax.rem(y + 2, 4), lax.rem(c + 2, 4)
    sib = {"ro": o}

    def rc(src, dst, ss, rs, dev):
        return pltpu.make_async_remote_copy(src_ref=src, dst_ref=dst, send_sem=ss, recv_sem=rs, device_id=dev, device_id_type=MESH)

    def lc(src, dst, sem):
        return pltpu.make_async_copy(src, dst, sem)

    def xor(a, b):
        return 2 * lax.rem(a // 2 + b // 2, 2) + lax.rem(lax.rem(a, 2) + lax.rem(b, 2), 2)

    bar = pltpu.get_barrier_semaphore()
    partners = [sib]
    for e in range(2):
        for k in (h, o):
            partners += [{"ri": yn[e], "ro": k}, {"co": cn[e], "ro": k}]
    for dev in partners:
        pl.semaphore_signal(bar, 1, device_id=dev, device_id_type=MESH)
    pl.semaphore_wait(bar, len(partners))

    def xcols(i, k):
        return x.at[:, pl.ds(pl.multiple_of(i * 2 * q + k * q, q), q)]

    def wrow(k):
        return w.at[pl.ds(pl.multiple_of(k * q, q), q)]

    gc = tb // 4
    w_d2d = rc(wrow(o), wv.at[y, h], d2d.at[0], wr.at[y, h], sib)
    g_d2d = [rc(g.at[pl.ds(n * gc, gc)], gv.at[h, pl.ds(n * gc, gc)], d2d.at[1 + n], dr.at[n], sib) for n in range(4)]
    x_d2d = [rc(xcols(i, o), xa.at[c, h, i], d2d.at[5 + i], xr.at[c, h, i], sib) for i in range(2)]
    w_dir, x_dir = [], []
    for n in range(2):
        for e in range(2):
            k = h if n == e else o
            w_dir.append(rc(wrow(k), wv.at[y, h], swd.at[e, n], wr.at[y, h], {"ri": yn[e], "ro": k}))
            for i in range(2):
                x_dir.append(rc(xcols(i, k), xa.at[c, h, i], sxd.at[e, n, i], xr.at[c, h, i], {"co": cn[e], "ro": k}))
    w_loc = lc(wrow(h), wv.at[y, h], loc.at[0])
    g_loc = [lc(g.at[pl.ds(n * gc, gc)], gv.at[h, pl.ds(n * gc, gc)], loc.at[1 + n]) for n in range(4)]
    w_loc.start()
    g_loc[0].start()
    w_d2d.start()
    for cp in w_dir + x_dir:
        cp.start()
    for cp in g_loc[1:] + g_d2d + x_d2d:
        cp.start()

    w_fwd = [rc(wv.at[yn[1 - e], k], wv.at[yn[1 - e], k], swf.at[e], wr.at[yn[1 - e], k], {"ri": yn[e]}) for e, k in ((0, h), (1, o))]
    x_fwd = [rc(xa.at[cn[1 - e], k, i], xa.at[cn[1 - e], k, i], sxf.at[e, i], xr.at[cn[1 - e], k, i], {"co": cn[e]})
             for e, k in ((0, h), (1, o)) for i in range(2)]

    def got_w(yy, k):
        rc(wv.at[yy, k], wv.at[yy, k], swf.at[0], wr.at[yy, k], sib).wait_recv()

    def got_x(cc, k):
        for i in range(2):
            rc(xa.at[cc, k, i], xa.at[cc, k, i], sxf.at[0, i], xr.at[cc, k, i], sib).wait_recv()

    def sends(part, recv, ss, rs, me, axis, nbr, d):
        k = lax.rem(d - me + 4, 4)

        @pl.when(k == 2)
        def _():
            @pl.loop(0, NC)
            def _(j):
                for e in range(2):
                    rc(part.at[d, e, j], recv.at[0, e, j], ss.at[0, e, j], rs.at[0, e, j], {axis: nbr[e]}).start()

        for e in range(2):
            @pl.when(k == 1 + 2 * e)
            def _():
                @pl.loop(0, NC)
                def _(j):
                    rc(part.at[d, 1 - e, j], recv.at[1, e, j], ss.at[1, e, j], rs.at[1, e, j], {axis: nbr[e]}).start()

    x_sends = functools.partial(sends, pp, rx, sx, rxs, c, "co", cn)
    y_sends = functools.partial(sends, qq, ry, sy, rys, y, "ri", yn)

    def compute(xin, xt, pst, qst):
        xo_in = [lc(xcols(i, h), xin.at[i, 0], ins.at[i, 0]) for i in range(2)]
        xo_out = [lc(xin.at[i, 0], xa.at[c, h, i], ins.at[i, 1]) for i in range(2)]
        for cp in xo_in:
            cp.start()

        def p_out(slot, r, yy, m):
            s, ab, hf = 1 - m // 4, lax.rem(m // 2, 2), lax.rem(m, 2)
            return lc(pst.at[slot, r], pp.at[2 * r + yy // 2, ab, pl.ds(s * 4 + hf * 2, 2), :, pl.ds(pl.multiple_of(lax.rem(yy, 2) * q, q), q)], pos.at[slot, r])

        def p_step(yy, first):
            @pl.loop(0, 8)
            def _(m):
                @pl.when(first & (m == 4))
                def _():
                    for n in range(4):
                        rc(g.at[pl.ds(n * gc, gc)], gv.at[o, pl.ds(n * gc, gc)], d2d.at[1 + n], dr.at[n], sib).wait_recv()

                s, ab, hf = 1 - m // 4, lax.rem(m // 2, 2), lax.rem(m, 2)
                t = s * h + (1 - s) * o
                row = pl.multiple_of(ab * (tb // 2) + hf * (tb // 4), tb // 4)
                slot = lax.rem(m, 2)

                @pl.when(m >= 2)
                def _():
                    for r in range(2):
                        p_out(slot, r, yy, m).wait()

                a = gv[t, pl.ds(row, tb // 4), :]
                b = wv[yy].reshape(2 * q, f)
                res = lax.dot_general(a, b, (((1,), (1,)), ((), ())), preferred_element_type=F32)
                for r in range(2):
                    pst[slot, r] = res[:, r * q:(r + 1) * q].reshape(2, cr, q)
                for r in range(2):
                    p_out(slot, r, yy, m).start()

            for slot in range(2):
                for r in range(2):
                    p_out(slot, r, yy, 6 + slot).wait()

        def q_out(slot, r, yy, n):
            s = r * h + (1 - r) * o
            return lc(qst.at[slot, r], qq.at[yy, :, pl.ds(s * 4, 4), :, pl.ds(pl.multiple_of(n * ft, ft), ft)], qos.at[slot, r])

        def q_step(yy):
            cps = [lc(xa.at[2 * r + yy // 2, t, lax.rem(yy, 2)], xin.at[r, t], ins.at[r, t]) for r in range(2) for t in range(2)]
            for cp in cps:
                cp.start()
            for cp in cps:
                cp.wait()

            @pl.loop(0, NC)
            def _(n):
                at = pl.ds(pl.multiple_of(n * cr, cr), cr)
                for r in range(2):
                    for t in range(2):
                        xt[t, r * q:(r + 1) * q, at] = xin[r, t, at, :].T

            @pl.loop(0, 7)
            def _(n):
                slot = lax.rem(n, 2)

                @pl.when(n >= 2)
                def _():
                    for r in range(2):
                        q_out(slot, r, yy, n).wait()

                at = pl.ds(pl.multiple_of(n * ft, ft), ft)
                res = jnp.dot(xt[0], gv[0, :, at], preferred_element_type=F32)
                res += jnp.dot(xt[1], gv[1, :, at], preferred_element_type=F32)
                for r in range(2):
                    qst[slot, r] = res[r * q:(r + 1) * q].reshape(2, 4, qr, ft)
                for r in range(2):
                    q_out(slot, r, yy, n).start()

            for slot in range(2):
                for r in range(2):
                    q_out(slot, r, yy, 0).wait()

        op = lax.rem(y // 2 + c + 1, 2)
        even = 1 - lax.rem(y, 2)
        rem1 = even * h + (1 - even) * o

        @pl.loop(0, 8)
        def _(step):
            @pl.when(step == 0)
            def _():
                w_loc.wait()
                for cp in g_loc:
                    cp.wait()
                got_w(y, o)

            @pl.when(step == 1)
            def _():
                for i in range(2):
                    xo_in[i].wait()
                    xo_out[i].start()
                got_w(yn[1], h)
                w_fwd[0].start()
                got_w(yn[0], o)
                w_fwd[1].start()
                got_x(cn[1], h)
                x_fwd[0].start()
                x_fwd[1].start()
                got_x(cn[0], o)
                x_fwd[2].start()
                x_fwd[3].start()
                got_w(xor(y, 1), rem1)

            @pl.when(step == 2)
            def _():
                x_sends(y // 2)
                x_sends(2 + y // 2)
                got_x(cn[1], o)
                got_x(cn[0], h)
                for i in range(2):
                    xo_out[i].wait()

            @pl.when(step == 3)
            def _():
                got_x(c, o)
                got_x(c2, 0)
                got_x(c2, 1)

            @pl.when(step == 5)
            def _():
                got_w(3 - y, 1 - rem1)

            @pl.when(step == 6)
            def _():
                got_w(y2, 0)
                got_w(y2, 1)

            late = step // 5
            is_p = (step < 2) | ((step >= 5) & (step < 7))
            pn = step - 3 * late
            qn = step - 2 - 2 * (step // 7)
            pcode = pn + pn // 2 - 2 * (pn // 3)
            qa = qn // 2
            qcode = op * ((1 - qa) * (2 + qn) + qa * (3 - qn)) + (1 - op) * lax.rem(qn + 1, 4)

            @pl.when(is_p)
            def _():
                p_step(xor(y, pcode), step == 0)

            @pl.when(jnp.logical_not(is_p))
            def _():
                yy = xor(y, qcode)
                q_step(yy)
                y_sends(yy)

            @pl.when(step == 6)
            def _():
                x_sends(1 - y // 2)
                x_sends(3 - y // 2)

    pl.run_scoped(compute, pltpu.VMEM((2, 2, tb, q), BF16), pltpu.VMEM((2, 2 * q, tb), BF16),
                  pltpu.VMEM((2, 2, 2, cr, q), F32), pltpu.VMEM((2, 2, 2, 4, qr, ft), F32))

    def reduce(ax, ay, bx, by):
        rings = ((pp, rx, sx, rxs, c, cn, "co", ax), (qq, ry, sy, rys, y, yn, "ri", ay))

        @pl.loop(0, NC)
        def _(j):
            for a, (part, recv, ss, rs, me, nbr, axis, buf) in enumerate(rings):
                for e in range(2):
                    rc(recv.at[0, e, j], recv.at[0, e, j], ss.at[0, e, j], rs.at[0, e, j], {axis: nbr[e]}).wait_recv()
                    lc(part.at[nbr[e], e, j], buf.at[e, 0], ads.at[a, e, 0]).start()
                    lc(recv.at[0, e, j], buf.at[e, 1], ads.at[a, e, 1]).start()
            for a, (part, recv, ss, rs, me, nbr, axis, buf) in enumerate(rings):
                for e in range(2):
                    lc(part.at[nbr[e], e, j], buf.at[e, 0], ads.at[a, e, 0]).wait()
                    lc(recv.at[0, e, j], buf.at[e, 1], ads.at[a, e, 1]).wait()
                    buf[e, 2] = buf[e, 0] + buf[e, 1]
                    lc(buf.at[e, 2], part.at[nbr[e], e, j], ads.at[a, e, 2]).start()
            for a, (part, recv, ss, rs, me, nbr, axis, buf) in enumerate(rings):
                for e in range(2):
                    lc(buf.at[e, 2], part.at[nbr[e], e, j], ads.at[a, e, 2]).wait()
                    rc(part.at[nbr[e], e, j], recv.at[2, e, j], ss.at[2, e, j], rs.at[2, e, j], {axis: nbr[e]}).start()

        def x_out(e, j, i, k):
            return dx.at[pl.ds(pl.multiple_of(e * (tb // 2) + lax.rem(j, 4) * cr, cr), cr), pl.ds(pl.multiple_of(i * 2 * q + k * q, q), q)]

        def y_out(e, j, k):
            return dw.at[pl.ds(pl.multiple_of(k * q + e * (q // 2) + lax.rem(j, 4) * qr, qr), qr)]

        def x_rc(e, j, i):
            return rc(bx.at[e, j, :, i * q:(i + 1) * q], x_out(e, j, i, h), fxs.at[e, j, i], fxr.at[e, lax.rem(j, 4), i], sib)

        def x_lc(e, j, i):
            return lc(bx.at[e, j, :, i * q:(i + 1) * q], x_out(e, j, i, h), fxs.at[e, j, i])

        def y_rc(e, j):
            return rc(by.at[e, j], y_out(e, j, h), fys.at[e, j], fyr.at[e, lax.rem(j, 4)], sib)

        def y_lc(e, j):
            return lc(by.at[e, j], y_out(e, j, h), fys.at[e, j])

        @pl.loop(0, NC)
        def _(j):
            for a, (part, recv, ss, rs, me, nbr, axis, buf) in enumerate(rings):
                for e in range(2):
                    rc(recv.at[1, 1 - e, j], recv.at[1, 1 - e, j], ss.at[1, 1 - e, j], rs.at[1, 1 - e, j], {axis: nbr[e]}).wait_recv()
                    lc(part.at[me, e, j], buf.at[e, 0], ads.at[a, e, 0]).start()
                    lc(recv.at[1, 1 - e, j], buf.at[e, 1], ads.at[a, e, 1]).start()
            for a in (1, 0):
                part, recv, ss, rs, me, nbr, axis, buf = rings[a]
                for e in range(2):
                    rc(recv.at[2, e, j], recv.at[2, e, j], ss.at[2, e, j], rs.at[2, e, j], {axis: nbr[e]}).wait_recv()
                    lc(recv.at[2, e, j], buf.at[e, 2], ads.at[a, e, 2]).start()
                for e in range(2):
                    lc(part.at[me, e, j], buf.at[e, 0], ads.at[a, e, 0]).wait()
                    lc(recv.at[1, 1 - e, j], buf.at[e, 1], ads.at[a, e, 1]).wait()
                    lc(recv.at[2, e, j], buf.at[e, 2], ads.at[a, e, 2]).wait()
                    tot = buf[e, 0] + buf[e, 1] + buf[e, 2]
                    if a == 0:
                        bx[e, j] = tot.astype(BF16)
                    else:
                        by[e, j] = tot

                    @pl.when(j < 4)
                    def _():
                        if a == 0:
                            for i in range(2):
                                x_rc(e, j, i).start()
                        else:
                            y_rc(e, j).start()

                    @pl.when(j >= 4)
                    def _():
                        if a == 0:
                            for i in range(2):
                                x_lc(e, j, i).start()
                        else:
                            y_lc(e, j).start()

        @pl.loop(0, NC)
        def _(j):
            for a, (part, recv, ss, rs, me, nbr, axis, buf) in enumerate(rings):
                for e in range(2):
                    for n in range(3):
                        rc(part.at[me, e, j], recv.at[n, e, j], ss.at[n, e, j], rs.at[n, e, j], {axis: nbr[e]}).wait_send()
            for e in range(2):
                @pl.when(j < 4)
                def _():
                    for i in range(2):
                        x_rc(e, j, i).wait()
                    y_rc(e, j).wait()

                @pl.when(j >= 4)
                def _():
                    for i in range(2):
                        x_lc(e, j, i).wait()
                    y_lc(e, j).wait()

        for cp in [w_d2d] + g_d2d + x_d2d + w_dir + x_dir + w_fwd + x_fwd:
            cp.wait_send()

    pl.run_scoped(reduce, pltpu.VMEM((2, 3, cr, 2 * q), F32), pltpu.VMEM((2, 3, qr, f), F32),
                  pltpu.VMEM((2, NC, cr, 2 * q), BF16), pltpu.VMEM((2, NC, qr, f), F32))


def solution(mesh):
    spec_act = P(("dp", "ro", "ri"), "co")
    spec_w = P(("ro", "ri"), "co")

    def local_step(x, w, g):
        tb, dcols = x.shape
        wrows, f = w.shape
        q = wrows // 2
        cr, qr = tb // NC, q // NC
        dma = lambda *s: pltpu.SemaphoreType.DMA(s)
        any_ = pl.BlockSpec(memory_space=pl.ANY)
        shapes = [
            jax.ShapeDtypeStruct((tb, dcols), BF16),
            jax.ShapeDtypeStruct((wrows, f), F32),
            jax.ShapeDtypeStruct((4, 2, NC, cr, 2 * q), F32),
            jax.ShapeDtypeStruct((4, 2, NC, qr, f), F32),
            jax.ShapeDtypeStruct((4, 2, 2, tb, q), BF16),
            jax.ShapeDtypeStruct((3, 2, NC, cr, 2 * q), F32),
            jax.ShapeDtypeStruct((3, 2, NC, qr, f), F32),
        ]
        res = pl.pallas_call(
            kernel,
            out_shape=shapes,
            in_specs=[any_] * 3,
            out_specs=[any_] * len(shapes),
            scratch_shapes=[
                pltpu.VMEM((2, tb, f), BF16),
                pltpu.VMEM((4, 2, q, f), BF16),
                dma(5), dma(7), dma(4), dma(4, 2), dma(4, 2, 2), dma(2, 2), dma(2), dma(2, 2, 2), dma(2, 2),
                dma(3, 2, NC), dma(3, 2, NC), dma(3, 2, NC), dma(3, 2, NC),
                dma(2, NC, 2), dma(2, 4, 2), dma(2, NC), dma(2, 4), dma(2, 2), dma(2, 2), dma(2, 2), dma(2, 2, 3),
            ],
            compiler_params=pltpu.CompilerParams(collective_id=0, has_side_effects=True, vmem_limit_bytes=67043328),
            name="linear_grads",
        )(x, w, g)
        return res[0], res[1]

    return jax.shard_map(local_step, mesh=mesh, in_specs=(spec_act, spec_w, spec_act), out_specs=(spec_act, spec_act), check_vma=False)
```

```python
import functools

import jax
import jax.numpy as jnp
from jax import lax
from jax.experimental import pallas as pl
from jax.experimental.pallas import tpu as pltpu
from jax.sharding import PartitionSpec as P

MESH = pl.DeviceIdType.MESH
BF16, F32 = jnp.bfloat16, jnp.float32
NC = 8


def kernel(x, w, g, dx, dw, pp, qq, xa, wa, rx, ry, gv,
           loc, d2d, dr, wr, xr, swd, swf, sxd, sxf, sx, rxs, sy, rys, fxs, fxr, fys, fyr, pos, qos, ins, wis, ads):
    h, y, c = lax.axis_index("ro"), lax.axis_index("ri"), lax.axis_index("co")
    o = 1 - h
    tb, dcols = x.shape
    wrows, f = w.shape
    q = wrows // 2
    cr, qr = tb // NC, q // NC
    ft = f // 7
    yn = [lax.rem(y + 1, 4), lax.rem(y + 3, 4)]
    cn = [lax.rem(c + 1, 4), lax.rem(c + 3, 4)]
    y2, c2 = lax.rem(y + 2, 4), lax.rem(c + 2, 4)
    sib = {"ro": o}

    def rc(src, dst, ss, rs, dev):
        return pltpu.make_async_remote_copy(src_ref=src, dst_ref=dst, send_sem=ss, recv_sem=rs, device_id=dev, device_id_type=MESH)

    def lc(src, dst, sem):
        return pltpu.make_async_copy(src, dst, sem)

    def xor(a, b):
        return 2 * lax.rem(a // 2 + b // 2, 2) + lax.rem(lax.rem(a, 2) + lax.rem(b, 2), 2)

    bar = pltpu.get_barrier_semaphore()
    partners = [sib]
    for e in range(2):
        for k in (h, o):
            partners += [{"ri": yn[e], "ro": k}, {"co": cn[e], "ro": k}]
    for dev in partners:
        pl.semaphore_signal(bar, 1, device_id=dev, device_id_type=MESH)
    pl.semaphore_wait(bar, len(partners))

    def xcols(i, k):
        return x.at[:, pl.ds(pl.multiple_of(i * 2 * q + k * q, q), q)]

    def wrow(k):
        return w.at[pl.ds(pl.multiple_of(k * q, q), q)]

    gc = tb // 4
    w_d2d = rc(wrow(o), wa.at[y, h], d2d.at[0], wr.at[y, h], sib)
    g_d2d = [rc(g.at[pl.ds(n * gc, gc)], gv.at[h, pl.ds(n * gc, gc)], d2d.at[1 + n], dr.at[n], sib) for n in range(4)]
    x_d2d = [rc(xcols(i, o), xa.at[c, h, i], d2d.at[5 + i], xr.at[c, h, i], sib) for i in range(2)]
    w_dir, x_dir = [], []
    for n in range(2):
        for e in range(2):
            k = h if n == e else o
            w_dir.append(rc(wrow(k), wa.at[y, h], swd.at[e, n], wr.at[y, h], {"ri": yn[e], "ro": k}))
            for i in range(2):
                x_dir.append(rc(xcols(i, k), xa.at[c, h, i], sxd.at[e, n, i], xr.at[c, h, i], {"co": cn[e], "ro": k}))
    g_loc = [lc(g.at[pl.ds(n * gc, gc)], gv.at[h, pl.ds(n * gc, gc)], loc.at[1 + n]) for n in range(4)]
    g_loc[0].start()
    w_d2d.start()
    for cp in w_dir + x_dir:
        cp.start()
    for cp in g_loc[1:] + g_d2d + x_d2d:
        cp.start()

    w_fwd = [rc(wa.at[yn[1 - e], k], wa.at[yn[1 - e], k], swf.at[e], wr.at[yn[1 - e], k], {"ri": yn[e]}) for e, k in ((0, h), (1, o))]
    x_fwd = [rc(xa.at[cn[1 - e], k, i], xa.at[cn[1 - e], k, i], sxf.at[e, i], xr.at[cn[1 - e], k, i], {"co": cn[e]})
             for e, k in ((0, h), (1, o)) for i in range(2)]

    def got_w(yy, k):
        rc(wa.at[yy, k], wa.at[yy, k], swf.at[0], wr.at[yy, k], sib).wait_recv()

    def got_x(cc, k):
        for i in range(2):
            rc(xa.at[cc, k, i], xa.at[cc, k, i], sxf.at[0, i], xr.at[cc, k, i], sib).wait_recv()

    def sends(part, recv, ss, rs, me, axis, nbr, d):
        k = lax.rem(d - me + 4, 4)

        @pl.when(k == 2)
        def _():
            @pl.loop(0, NC)
            def _(j):
                for e in range(2):
                    rc(part.at[d, e, j], recv.at[0, e, j], ss.at[0, e, j], rs.at[0, e, j], {axis: nbr[e]}).start()

        for e in range(2):
            @pl.when(k == 1 + 2 * e)
            def _():
                @pl.loop(0, NC)
                def _(j):
                    rc(part.at[d, 1 - e, j], recv.at[1, e, j], ss.at[1, e, j], rs.at[1, e, j], {axis: nbr[e]}).start()

    x_sends = functools.partial(sends, pp, rx, sx, rxs, c, "co", cn)
    y_sends = functools.partial(sends, qq, ry, sy, rys, y, "ri", yn)

    def compute(wv, xin, xt, pst, qst):
        xo_in = [lc(xcols(i, h), xin.at[i, 0], ins.at[i, 0]) for i in range(2)]
        xo_out = [lc(xin.at[i, 0], xa.at[c, h, i], ins.at[i, 1]) for i in range(2)]
        for cp in xo_in:
            cp.start()

        def p_out(slot, r, yy, m):
            s, ab, hf = 1 - m // 4, lax.rem(m // 2, 2), lax.rem(m, 2)
            return lc(pst.at[slot, r], pp.at[2 * r + yy // 2, ab, pl.ds(s * 4 + hf * 2, 2), :, pl.ds(pl.multiple_of(lax.rem(yy, 2) * q, q), q)], pos.at[slot, r])

        def p_step(yy, first):
            cps = [lc(wa.at[yy, r], wv.at[pl.ds(r * q, q)], wis.at[r]) for r in range(2)]
            w_own = lc(wrow(h), wv.at[pl.ds(pl.multiple_of(h * q, q), q)], wis.at[h])
            w_oth = lc(wa.at[yy, o], wv.at[pl.ds(pl.multiple_of(o * q, q), q)], wis.at[o])

            @pl.when(first)
            def _():
                w_own.start()
                w_oth.start()

            @pl.when(jnp.logical_not(first))
            def _():
                for cp in cps:
                    cp.start()

            for cp in cps:
                cp.wait()

            @pl.loop(0, 8)
            def _(m):
                @pl.when(first & (m == 4))
                def _():
                    for n in range(4):
                        rc(g.at[pl.ds(n * gc, gc)], gv.at[o, pl.ds(n * gc, gc)], d2d.at[1 + n], dr.at[n], sib).wait_recv()

                s, ab, hf = 1 - m // 4, lax.rem(m // 2, 2), lax.rem(m, 2)
                t = s * h + (1 - s) * o
                row = pl.multiple_of(ab * (tb // 2) + hf * (tb // 4), tb // 4)
                slot = lax.rem(m, 2)

                @pl.when(m >= 2)
                def _():
                    for r in range(2):
                        p_out(slot, r, yy, m).wait()

                a = gv[t, pl.ds(row, tb // 4), :]
                res = lax.dot_general(a, wv[...], (((1,), (1,)), ((), ())), preferred_element_type=F32)
                for r in range(2):
                    pst[slot, r] = res[:, r * q:(r + 1) * q].reshape(2, cr, q)
                for r in range(2):
                    p_out(slot, r, yy, m).start()

            for slot in range(2):
                for r in range(2):
                    p_out(slot, r, yy, 6 + slot).wait()

        def q_out(slot, r, yy, n):
            s = r * h + (1 - r) * o
            return lc(qst.at[slot, r], qq.at[yy, :, pl.ds(s * 4, 4), :, pl.ds(pl.multiple_of(n * ft, ft), ft)], qos.at[slot, r])

        def q_step(yy):
            cps = [lc(xa.at[2 * r + yy // 2, t, lax.rem(yy, 2)], xin.at[r, t], ins.at[r, t]) for r in range(2) for t in range(2)]
            for cp in cps:
                cp.start()
            for cp in cps:
                cp.wait()

            @pl.loop(0, NC)
            def _(n):
                at = pl.ds(pl.multiple_of(n * cr, cr), cr)
                for r in range(2):
                    for t in range(2):
                        xt[t, r * q:(r + 1) * q, at] = xin[r, t, at, :].T

            @pl.loop(0, 7)
            def _(n):
                slot = lax.rem(n, 2)

                @pl.when(n >= 2)
                def _():
                    for r in range(2):
                        q_out(slot, r, yy, n).wait()

                at = pl.ds(pl.multiple_of(n * ft, ft), ft)
                res = jnp.dot(xt[0], gv[0, :, at], preferred_element_type=F32)
                res += jnp.dot(xt[1], gv[1, :, at], preferred_element_type=F32)
                for r in range(2):
                    qst[slot, r] = res[r * q:(r + 1) * q].reshape(2, 4, qr, ft)
                for r in range(2):
                    q_out(slot, r, yy, n).start()

            for slot in range(2):
                for r in range(2):
                    q_out(slot, r, yy, 0).wait()

        op = lax.rem(y // 2 + c + 1, 2)
        even = 1 - lax.rem(y, 2)
        rem1 = even * h + (1 - even) * o

        @pl.loop(0, 8)
        def _(step):
            @pl.when(step == 0)
            def _():
                for cp in g_loc:
                    cp.wait()
                got_w(y, o)

            @pl.when(step == 1)
            def _():
                for i in range(2):
                    xo_in[i].wait()
                    xo_out[i].start()
                got_w(yn[1], h)
                w_fwd[0].start()
                got_w(yn[0], o)
                w_fwd[1].start()
                got_x(cn[1], h)
                x_fwd[0].start()
                x_fwd[1].start()
                got_x(cn[0], o)
                x_fwd[2].start()
                x_fwd[3].start()
                got_w(xor(y, 1), rem1)

            @pl.when(step == 2)
            def _():
                x_sends(y // 2)
                x_sends(2 + y // 2)
                got_x(cn[1], o)
                got_x(cn[0], h)
                for i in range(2):
                    xo_out[i].wait()

            @pl.when(step == 3)
            def _():
                got_x(c, o)
                got_x(c2, 0)
                got_x(c2, 1)

            @pl.when(step == 5)
            def _():
                got_w(3 - y, 1 - rem1)

            @pl.when(step == 6)
            def _():
                got_w(y2, 0)
                got_w(y2, 1)

            late = step // 5
            is_p = (step < 2) | ((step >= 5) & (step < 7))
            pn = step - 3 * late
            qn = step - 2 - 2 * (step // 7)
            pcode = pn + pn // 2 - 2 * (pn // 3)
            qa = qn // 2
            qcode = op * ((1 - qa) * (2 + qn) + qa * (3 - qn)) + (1 - op) * lax.rem(qn + 1, 4)

            @pl.when(is_p)
            def _():
                p_step(xor(y, pcode), step == 0)

            @pl.when(jnp.logical_not(is_p))
            def _():
                yy = xor(y, qcode)
                q_step(yy)
                y_sends(yy)

            @pl.when(step == 6)
            def _():
                x_sends(1 - y // 2)
                x_sends(3 - y // 2)

    pl.run_scoped(compute, pltpu.VMEM((2 * q, f), BF16), pltpu.VMEM((2, 2, tb, q), BF16), pltpu.VMEM((2, 2 * q, tb), BF16),
                  pltpu.VMEM((2, 2, 2, cr, q), F32), pltpu.VMEM((2, 2, 2, 4, qr, ft), F32))

    def reduce(ax, ay, bx, by):
        rings = ((pp, rx, sx, rxs, c, cn, "co", ax), (qq, ry, sy, rys, y, yn, "ri", ay))

        @pl.loop(0, NC)
        def _(j):
            for a, (part, recv, ss, rs, me, nbr, axis, buf) in enumerate(rings):
                for e in range(2):
                    rc(recv.at[0, e, j], recv.at[0, e, j], ss.at[0, e, j], rs.at[0, e, j], {axis: nbr[e]}).wait_recv()
                    lc(part.at[nbr[e], e, j], buf.at[e, 0], ads.at[a, e, 0]).start()
                    lc(recv.at[0, e, j], buf.at[e, 1], ads.at[a, e, 1]).start()
            for a, (part, recv, ss, rs, me, nbr, axis, buf) in enumerate(rings):
                for e in range(2):
                    lc(part.at[nbr[e], e, j], buf.at[e, 0], ads.at[a, e, 0]).wait()
                    lc(recv.at[0, e, j], buf.at[e, 1], ads.at[a, e, 1]).wait()
                    buf[e, 2] = buf[e, 0] + buf[e, 1]
                    lc(buf.at[e, 2], part.at[nbr[e], e, j], ads.at[a, e, 2]).start()
            for a, (part, recv, ss, rs, me, nbr, axis, buf) in enumerate(rings):
                for e in range(2):
                    lc(buf.at[e, 2], part.at[nbr[e], e, j], ads.at[a, e, 2]).wait()
                    rc(part.at[nbr[e], e, j], recv.at[2, e, j], ss.at[2, e, j], rs.at[2, e, j], {axis: nbr[e]}).start()

        def x_at(e, j, i):
            return (pl.ds(pl.multiple_of(e * (tb // 2) + lax.rem(j, 4) * cr, cr), cr), pl.ds(pl.multiple_of(i * 2 * q + h * q, q), q))

        def y_at(e, j):
            return pl.ds(pl.multiple_of(h * q + e * (q // 2) + lax.rem(j, 4) * qr, qr), qr)

        def x_rc(e, j, i):
            return rc(bx.at[e, j, :, i * q:(i + 1) * q], dx.at[x_at(e, j, i)], fxs.at[e, j, i], fxr.at[e, j, i], sib)

        def y_rc(e, j):
            return rc(by.at[e, j], dw.at[y_at(e, j)], fys.at[e, j], fyr.at[e, j], sib)

        @pl.loop(0, NC)
        def _(j):
            for a, (part, recv, ss, rs, me, nbr, axis, buf) in enumerate(rings):
                for e in range(2):
                    rc(recv.at[1, 1 - e, j], recv.at[1, 1 - e, j], ss.at[1, 1 - e, j], rs.at[1, 1 - e, j], {axis: nbr[e]}).wait_recv()
                    lc(part.at[me, e, j], buf.at[e, 0], ads.at[a, e, 0]).start()
                    lc(recv.at[1, 1 - e, j], buf.at[e, 1], ads.at[a, e, 1]).start()
            for a in (1, 0):
                part, recv, ss, rs, me, nbr, axis, buf = rings[a]
                for e in range(2):
                    rc(recv.at[2, e, j], recv.at[2, e, j], ss.at[2, e, j], rs.at[2, e, j], {axis: nbr[e]}).wait_recv()
                    lc(recv.at[2, e, j], buf.at[e, 2], ads.at[a, e, 2]).start()
                for e in range(2):
                    lc(part.at[me, e, j], buf.at[e, 0], ads.at[a, e, 0]).wait()
                    lc(recv.at[1, 1 - e, j], buf.at[e, 1], ads.at[a, e, 1]).wait()
                    lc(recv.at[2, e, j], buf.at[e, 2], ads.at[a, e, 2]).wait()
                    tot = buf[e, 0] + buf[e, 1] + buf[e, 2]

                    @pl.when(j < 4)
                    def _():
                        if a == 0:
                            bx[e, j] = tot.astype(BF16)
                            for i in range(2):
                                x_rc(e, j, i).start()
                        else:
                            by[e, j] = tot
                            y_rc(e, j).start()

                    @pl.when(j >= 4)
                    def _():
                        if a == 0:
                            for i in range(2):
                                dx[x_at(e, j, i)] = tot[:, i * q:(i + 1) * q].astype(BF16)
                        else:
                            dw[y_at(e, j)] = tot

        @pl.loop(0, NC)
        def _(j):
            for a, (part, recv, ss, rs, me, nbr, axis, buf) in enumerate(rings):
                for e in range(2):
                    for n in range(3):
                        rc(part.at[me, e, j], recv.at[n, e, j], ss.at[n, e, j], rs.at[n, e, j], {axis: nbr[e]}).wait_send()

        @pl.loop(0, 4)
        def _(j):
            for e in range(2):
                for i in range(2):
                    x_rc(e, j, i).wait()
                y_rc(e, j).wait()

        for cp in [w_d2d] + g_d2d + x_d2d + w_dir + x_dir + w_fwd + x_fwd:
            cp.wait_send()

    pl.run_scoped(reduce, pltpu.VMEM((2, 3, cr, 2 * q), F32), pltpu.VMEM((2, 3, qr, f), F32),
                  pltpu.VMEM((2, 4, cr, 2 * q), BF16), pltpu.VMEM((2, 4, qr, f), F32))


def solution(mesh):
    spec_act = P(("dp", "ro", "ri"), "co")
    spec_w = P(("ro", "ri"), "co")

    def local_step(x, w, g):
        tb, dcols = x.shape
        wrows, f = w.shape
        q = wrows // 2
        cr, qr = tb // NC, q // NC
        dma = lambda *s: pltpu.SemaphoreType.DMA(s)
        any_ = pl.BlockSpec(memory_space=pl.ANY)
        shapes = [
            pltpu.VMEM((tb, dcols), BF16),
            pltpu.VMEM((wrows, f), F32),
            jax.ShapeDtypeStruct((4, 2, NC, cr, 2 * q), F32),
            jax.ShapeDtypeStruct((4, 2, NC, qr, f), F32),
            jax.ShapeDtypeStruct((4, 2, 2, tb, q), BF16),
            jax.ShapeDtypeStruct((4, 2, q, f), BF16),
            jax.ShapeDtypeStruct((3, 2, NC, cr, 2 * q), F32),
            jax.ShapeDtypeStruct((3, 2, NC, qr, f), F32),
        ]
        res = pl.pallas_call(
            kernel,
            out_shape=shapes,
            in_specs=[any_] * 3,
            out_specs=[pl.BlockSpec(memory_space=pltpu.VMEM)] * 2 + [any_] * (len(shapes) - 2),
            scratch_shapes=[
                pltpu.VMEM((2, tb, f), BF16),
                dma(5), dma(7), dma(4), dma(4, 2), dma(4, 2, 2), dma(2, 2), dma(2), dma(2, 2, 2), dma(2, 2),
                dma(3, 2, NC), dma(3, 2, NC), dma(3, 2, NC), dma(3, 2, NC),
                dma(2, 4, 2), dma(2, 4, 2), dma(2, 4), dma(2, 4), dma(2, 2), dma(2, 2), dma(2, 2), dma(2), dma(2, 2, 3),
            ],
            compiler_params=pltpu.CompilerParams(collective_id=0, has_side_effects=True, vmem_limit_bytes=52 << 20),
            name="linear_grads",
        )(x, w, g)
        return res[0], res[1]

    return jax.shard_map(local_step, mesh=mesh, in_specs=(spec_act, spec_w, spec_act), out_specs=(spec_act, spec_act), check_vma=False)
```

```python
import functools

import jax
import jax.numpy as jnp
from jax import lax
from jax.experimental import pallas as pl
from jax.experimental.pallas import tpu as pltpu
from jax.sharding import PartitionSpec as P

MESH = pl.DeviceIdType.MESH
BF16, F32 = jnp.bfloat16, jnp.float32
NC = 8
NH = NC // 2


def kernel(x, w, g, dx, dw, pp, qq, xa, wa, rx, ry, gv, vx,
           ls, ss, dr, wr, xr, ring_s, opp_r, pure_r, xacc_r, yacc_r, fin, outs, ads, told):
    h, y, c = lax.axis_index("ro"), lax.axis_index("ri"), lax.axis_index("co")
    o = 1 - h
    tb, dcols = x.shape
    wrows, f = w.shape
    q = wrows // 2
    cr, qr = tb // NC, q // NC
    ft = f // 7
    yn = [lax.rem(y + 1, 4), lax.rem(y + 3, 4)]
    cn = [lax.rem(c + 1, 4), lax.rem(c + 3, 4)]
    y2, c2 = lax.rem(y + 2, 4), lax.rem(c + 2, 4)
    sib = {"ro": o}

    def rc(src, dst, ssem, rsem, dev):
        return pltpu.make_async_remote_copy(src_ref=src, dst_ref=dst, send_sem=ssem, recv_sem=rsem, device_id=dev, device_id_type=MESH)

    def lc(src, dst, sem):
        return pltpu.make_async_copy(src, dst, sem)

    def done(ref, sem):
        lc(ref, ref, sem).wait()

    def xor(a, b):
        return 2 * lax.rem(a // 2 + b // 2, 2) + lax.rem(lax.rem(a, 2) + lax.rem(b, 2), 2)

    bar = pltpu.get_barrier_semaphore()
    partners = [{"co": cn[0], "ro": 0}, {"co": cn[1], "ro": 0}, sib, {"ri": yn[0], "ro": 1}, {"ri": yn[1], "ro": 1}]
    for dev in partners:
        pl.semaphore_signal(bar, 1, device_id=dev, device_id_type=MESH)

    def heard(core):
        @pl.when(h == core)
        def _():
            pl.semaphore_wait(bar, 5)
            pl.semaphore_signal(told, 1, device_id=sib, device_id_type=MESH)

        @pl.when(h != core)
        def _():
            pl.semaphore_wait(told, 1)

    heard(0)

    def xcols(i, k):
        return x.at[:, pl.ds(pl.multiple_of(i * 2 * q + k * q, q), q)]

    def wrow(k):
        return w.at[pl.ds(pl.multiple_of(k * q, q), q)]

    w_dir, x_dir = [], []
    for n in range(2):
        for e in range(2):
            k = h if n == e else o
            w_dir.append(rc(wrow(k), wa.at[y, h], ss.at[3], wr.at[y, h], {"ri": yn[e], "ro": k}))
            for i in range(2):
                x_dir.append(rc(xcols(i, k), xa.at[c, h, i], ss.at[5], xr.at[c, h], {"co": cn[e], "ro": k}))
    w_d2d = rc(wrow(o), wa.at[y, h], ss.at[0], wr.at[y, h], sib)
    g_loc = lc(g, gv.at[h], ls.at[0])
    g_d2d = rc(g, gv.at[h], ss.at[1], dr.at[0], sib)
    x_d2d = [rc(xcols(i, o), xa.at[c, h, i], ss.at[2], xr.at[c, h], sib) for i in range(2)]
    for cp in x_dir + [w_d2d, g_loc, g_d2d] + x_d2d:
        cp.start()
    heard(1)
    for cp in w_dir:
        cp.start()

    w_fwd = [rc(wa.at[yn[1 - e], k], wa.at[yn[1 - e], k], ss.at[4], wr.at[yn[1 - e], k], {"ri": yn[e]}) for e, k in ((0, h), (1, o))]
    x_fwd = [rc(xa.at[cn[1 - e], k], xa.at[cn[1 - e], k], ss.at[6], xr.at[cn[1 - e], k], {"co": cn[e]}) for e, k in ((0, h), (1, o))]

    def got_w(yy, k):
        done(wa.at[yy, k], wr.at[yy, k])

    def got_x(cc, k):
        done(xa.at[cc, k], xr.at[cc, k])

    def sends(a, part, recv, me, axis, nbr, d):
        k = lax.rem(d - me + 4, 4)

        @pl.when(k == 2)
        def _():
            for n in range(2):
                for e in range(2):
                    half = pl.ds(n * NH, NH)
                    rc(part.at[d, e, half], recv.at[0, e, half], ring_s.at[a, 0, e], opp_r.at[a, e, n], {axis: nbr[e]}).start()

        for e in range(2):
            @pl.when(k == 1 + 2 * e)
            def _():
                rc(part.at[d, 1 - e], recv.at[1, e], ring_s.at[a, 1, e], pure_r.at[a, e], {axis: nbr[e]}).start()

    x_sends = functools.partial(sends, 0, pp, rx, c, "co", cn)
    y_sends = functools.partial(sends, 1, qq, ry, y, "ri", yn)

    def compute(wv, xin, xt, pst, qst):
        for i in range(2):
            lc(xcols(i, h), xin.at[0, i], ls.at[2]).start()

        def p_out(slot, r, yy, m):
            s, ab, hf = 1 - m // 4, lax.rem(m // 2, 2), lax.rem(m, 2)
            return lc(pst.at[slot, r], pp.at[2 * r + yy // 2, ab, pl.ds(s * 4 + hf * 2, 2), :, pl.ds(pl.multiple_of(lax.rem(yy, 2) * q, q), q)], outs.at[slot])

        def p_step(yy, first):
            @pl.when(first)
            def _():
                lc(wrow(h), wv.at[pl.ds(pl.multiple_of(h * q, q), q)], ls.at[1]).start()
                lc(wa.at[yy, o], wv.at[pl.ds(pl.multiple_of(o * q, q), q)], ls.at[1]).start()

            @pl.when(jnp.logical_not(first))
            def _():
                for r in range(2):
                    lc(wa.at[yy, r], wv.at[pl.ds(r * q, q)], ls.at[1]).start()

            done(wv, ls.at[1])

            @pl.loop(0, 8)
            def _(m):
                @pl.when(first & (m == 4))
                def _():
                    done(gv.at[o], dr.at[0])

                s, ab, hf = 1 - m // 4, lax.rem(m // 2, 2), lax.rem(m, 2)
                t = s * h + (1 - s) * o
                row = pl.multiple_of(ab * (tb // 2) + hf * (tb // 4), tb // 4)
                slot = lax.rem(m, 2)

                @pl.when(m >= 2)
                def _():
                    done(pst.at[slot], outs.at[slot])

                res = lax.dot_general(gv[t, pl.ds(row, tb // 4), :], wv[...], (((1,), (1,)), ((), ())), preferred_element_type=F32)
                for r in range(2):
                    pst[slot, r] = res[:, r * q:(r + 1) * q].reshape(2, cr, q)
                for r in range(2):
                    p_out(slot, r, yy, m).start()

            for slot in range(2):
                done(pst.at[slot], outs.at[slot])

        def q_out(slot, r, yy, n):
            s = r * h + (1 - r) * o
            return lc(qst.at[slot, r], qq.at[yy, :, pl.ds(s * 4, 4), :, pl.ds(pl.multiple_of(n * ft, ft), ft)], outs.at[slot])

        def q_step(yy):
            for r in range(2):
                for t in range(2):
                    lc(xa.at[2 * r + yy // 2, t, lax.rem(yy, 2)], xin.at[r, t], ls.at[3]).start()
            done(xin, ls.at[3])

            @pl.loop(0, NC)
            def _(n):
                at = pl.ds(pl.multiple_of(n * cr, cr), cr)
                for r in range(2):
                    for t in range(2):
                        xt[t, r * q:(r + 1) * q, at] = xin[r, t, at, :].T

            @pl.loop(0, 7)
            def _(n):
                slot = lax.rem(n, 2)

                @pl.when(n >= 2)
                def _():
                    done(qst.at[slot], outs.at[slot])

                at = pl.ds(pl.multiple_of(n * ft, ft), ft)
                res = jnp.dot(xt[0], gv[0, :, at], preferred_element_type=F32)
                res += jnp.dot(xt[1], gv[1, :, at], preferred_element_type=F32)
                for r in range(2):
                    qst[slot, r] = res[r * q:(r + 1) * q].reshape(2, 4, qr, ft)
                for r in range(2):
                    q_out(slot, r, yy, n).start()

            for slot in range(2):
                done(qst.at[slot], outs.at[slot])

        op = lax.rem(y // 2 + c + 1, 2)
        even = 1 - lax.rem(y, 2)
        rem1 = even * h + (1 - even) * o

        @pl.loop(0, 8)
        def _(step):
            @pl.when(step == 0)
            def _():
                done(gv.at[h], ls.at[0])
                got_w(y, o)

            @pl.when(step == 1)
            def _():
                done(xin.at[0], ls.at[2])
                for i in range(2):
                    lc(xin.at[0, i], xa.at[c, h, i], ls.at[2]).start()
                got_w(yn[1], h)
                w_fwd[0].start()
                got_w(yn[0], o)
                w_fwd[1].start()
                got_x(cn[1], h)
                x_fwd[0].start()
                got_x(cn[0], o)
                x_fwd[1].start()
                got_w(xor(y, 1), rem1)

            @pl.when(step == 2)
            def _():
                x_sends(y // 2)
                x_sends(2 + y // 2)
                got_x(cn[1], o)
                got_x(cn[0], h)
                done(xin.at[0], ls.at[2])

            @pl.when(step == 3)
            def _():
                got_x(c, o)
                got_x(c2, 0)
                got_x(c2, 1)

            @pl.when(step == 5)
            def _():
                got_w(3 - y, 1 - rem1)

            @pl.when(step == 6)
            def _():
                got_w(y2, 0)
                got_w(y2, 1)

            late = step // 5
            is_p = (step < 2) | ((step >= 5) & (step < 7))
            pn = step - 3 * late
            qn = step - 2 - 2 * (step // 7)
            pcode = pn + pn // 2 - 2 * (pn // 3)
            qa = qn // 2
            qcode = op * ((1 - qa) * (2 + qn) + qa * (3 - qn)) + (1 - op) * lax.rem(qn + 1, 4)

            @pl.when(is_p)
            def _():
                p_step(xor(y, pcode), step == 0)

            @pl.when(jnp.logical_not(is_p))
            def _():
                yy = xor(y, qcode)
                q_step(yy)
                y_sends(yy)

            @pl.when(step == 6)
            def _():
                x_sends(1 - y // 2)
                x_sends(3 - y // 2)

    pl.run_scoped(compute, pltpu.VMEM((2 * q, f), BF16), pltpu.VMEM((2, 2, tb, q), BF16), pltpu.VMEM((2, 2 * q, tb), BF16),
                  pltpu.VMEM((2, 2, 2, cr, q), F32), pltpu.VMEM((2, 2, 2, 4, qr, ft), F32))

    def reduce(ax, ay, bx, by, px):
        rings = ((0, pp, rx, c, cn, "co", ax), (1, qq, ry, y, yn, "ri", ay))

        @pl.loop(0, 2)
        def _(n):
            for a, part, recv, me, nbr, axis, buf in rings:
                for e in range(2):
                    done(recv.at[0, e, pl.ds(0, NH)], opp_r.at[a, e, n])

            @pl.loop(0, NH)
            def _(i):
                j = n * NH + i
                for a, part, recv, me, nbr, axis, buf in rings:
                    for e in range(2):
                        lc(part.at[nbr[e], e, j], buf.at[e, 0], ads.at[a, 0]).start()
                        lc(recv.at[0, e, j], buf.at[e, 1], ads.at[a, 0]).start()
                for a, part, recv, me, nbr, axis, buf in rings:
                    done(buf.at[:, pl.ds(0, 2)], ads.at[a, 0])
                    for e in range(2):
                        buf[e, 2] = buf[e, 0] + buf[e, 1]
                        lc(buf.at[e, 2], part.at[nbr[e], e, j], ads.at[a, 1]).start()
                for a, part, recv, me, nbr, axis, buf in rings:
                    done(buf.at[:, 2], ads.at[a, 1])

                @pl.when(n == 1)
                def _():
                    for e in range(2):
                        rc(pp.at[cn[e], e, j], vx.at[e, i], ring_s.at[0, 2, e], xacc_r.at[e, 1 + i], {"co": cn[e]}).start()

            half = pl.ds(n * NH, NH)

            @pl.when(n == 0)
            def _():
                for e in range(2):
                    rc(pp.at[cn[e], e, half], rx.at[2, e, half], ring_s.at[0, 2, e], xacc_r.at[e, 0], {"co": cn[e]}).start()

            for e in range(2):
                rc(qq.at[yn[e], e, half], ry.at[2, e, half], ring_s.at[1, 2, e], yacc_r.at[e, n], {"ri": yn[e]}).start()

        def x_at(e, j, i):
            return (pl.ds(pl.multiple_of(e * (tb // 2) + j * cr, cr), cr), pl.ds(pl.multiple_of(i * 2 * q + h * q, q), q))

        def y_at(e, j):
            return pl.ds(pl.multiple_of(h * q + e * (q // 2) + j * qr, qr), qr)

        def load(ring, j, third):
            a, part, recv, me, nbr, axis, buf = ring
            for e in range(2):
                lc(part.at[me, e, j], buf.at[e, 0], ads.at[a, 0]).start()
                lc(recv.at[1, 1 - e, j], buf.at[e, 1], ads.at[a, 0]).start()
                if third:
                    lc(recv.at[2, e, j], buf.at[e, 2], ads.at[a, 0]).start()
            done(buf if third else buf.at[:, pl.ds(0, 2)], ads.at[a, 0])

        for a, part, recv, me, nbr, axis, buf in rings:
            for e in range(2):
                done(recv.at[1, e], pure_r.at[a, e])
                done(part.at[0, e], ring_s.at[a, 0, e])
                done(part.at[0, e], ring_s.at[a, 1, e])
        done(wa.at[0, 0], ss.at[0])
        done(gv.at[0], ss.at[1])
        done(xa.at[0, 0], ss.at[2])
        done(wa.at[pl.ds(0, 2)], ss.at[3])
        done(wa.at[0], ss.at[4])
        done(xa.at[pl.ds(0, 2)], ss.at[5])
        done(xa.at[0], ss.at[6])

        for e in range(2):
            done(ry.at[2, e, pl.ds(0, NH)], yacc_r.at[e, 0])

        @pl.loop(0, NH)
        def _(j):
            load(rings[1], j, True)
            for e in range(2):
                by[e, j] = ay[e, 0] + ay[e, 1] + ay[e, 2]
                rc(by.at[e, j], dw.at[y_at(e, j)], fin.at[2], fin.at[3], sib).start()
            load(rings[1], NH + j, False)
            for e in range(2):
                dw[y_at(e, j)] = ay[e, 0] + ay[e, 1]

        for e in range(2):
            done(rx.at[2, e, pl.ds(0, NH)], xacc_r.at[e, 0])

        @pl.loop(0, NH)
        def _(j):
            load(rings[0], j, True)
            for e in range(2):
                bx[e, j] = (ax[e, 0] + ax[e, 1] + ax[e, 2]).astype(BF16)
                for i in range(2):
                    rc(bx.at[e, j, :, i * q:(i + 1) * q], dx.at[x_at(e, j, i)], fin.at[0], fin.at[1], sib).start()
            load(rings[0], NH + j, False)
            for e in range(2):
                px[e, j] = ax[e, 0] + ax[e, 1]

        for e in range(2):
            done(ry.at[2, e, pl.ds(0, NH)], yacc_r.at[e, 1])

        @pl.loop(0, NH)
        def _(j):
            for e in range(2):
                lc(ry.at[2, e, NH + j], ay.at[e, 2], ads.at[1, 0]).start()
            done(ay.at[:, 2], ads.at[1, 0])
            for e in range(2):
                dw[y_at(e, j)] += ay[e, 2]

        for n in range(4):
            done(by if n >= 2 else bx, fin.at[n])
        for e in range(2):
            done(qq.at[0, e], ring_s.at[1, 2, e])

        @pl.loop(0, NH)
        def _(j):
            for e in range(2):
                done(vx.at[e, j], xacc_r.at[e, 1 + j])
                tot = px[e, j] + vx[e, j]
                for i in range(2):
                    dx[x_at(e, j, i)] = tot[:, i * q:(i + 1) * q].astype(BF16)

        for e in range(2):
            done(pp.at[0, e], ring_s.at[0, 2, e])

    pl.run_scoped(reduce, pltpu.VMEM((2, 3, cr, 2 * q), F32), pltpu.VMEM((2, 3, qr, f), F32),
                  pltpu.VMEM((2, NH, cr, 2 * q), BF16), pltpu.VMEM((2, NH, qr, f), F32), pltpu.VMEM((2, NH, cr, 2 * q), F32))


def put_kernel(a, b, u, v, sems):
    for i, (src, dst) in enumerate(((b, v), (a, u))):
        rows = src.shape[0] // 4
        for n in range(4):
            pltpu.make_async_copy(src.at[pl.ds(n * rows, rows)], dst.at[pl.ds(n * rows, rows)], sems.at[i]).start()
    for i, (src, dst) in enumerate(((b, v), (a, u))):
        pltpu.make_async_copy(src, dst, sems.at[i]).wait()


def solution(mesh):
    spec_act = P(("dp", "ro", "ri"), "co")
    spec_w = P(("ro", "ri"), "co")

    def local_step(x, w, g):
        tb, dcols = x.shape
        wrows, f = w.shape
        q = wrows // 2
        cr, qr = tb // NC, q // NC
        dma = lambda *s: pltpu.SemaphoreType.DMA(s)
        any_ = pl.BlockSpec(memory_space=pl.ANY)
        vmem = pl.BlockSpec(memory_space=pltpu.VMEM)
        shapes = [
            pltpu.VMEM((tb, dcols), BF16),
            pltpu.VMEM((wrows, f), F32),
            jax.ShapeDtypeStruct((4, 2, NC, cr, 2 * q), F32),
            jax.ShapeDtypeStruct((4, 2, NC, qr, f), F32),
            jax.ShapeDtypeStruct((4, 2, 2, tb, q), BF16),
            jax.ShapeDtypeStruct((4, 2, q, f), BF16),
            jax.ShapeDtypeStruct((3, 2, NC, cr, 2 * q), F32),
            jax.ShapeDtypeStruct((3, 2, NC, qr, f), F32),
        ]
        res = pl.pallas_call(
            kernel,
            out_shape=shapes,
            in_specs=[any_] * 3,
            out_specs=[vmem] * 2 + [any_] * (len(shapes) - 2),
            scratch_shapes=[
                pltpu.VMEM((2, tb, f), BF16),
                pltpu.VMEM((2, NH, cr, 2 * q), F32),
                dma(4), dma(7), dma(1), dma(4, 2), dma(4, 2), dma(2, 3, 2), dma(2, 2, 2), dma(2, 2), dma(2, 1 + NH), dma(2, 2), dma(4), dma(2), dma(2, 2), pltpu.SemaphoreType.REGULAR,
            ],
            compiler_params=pltpu.CompilerParams(collective_id=0, has_side_effects=True, vmem_limit_bytes=52 << 20),
            name="linear_grads",
        )(x, w, g)
        return pl.pallas_call(
            put_kernel,
            out_shape=[jax.ShapeDtypeStruct(r.shape, r.dtype) for r in res[:2]],
            in_specs=[vmem] * 2,
            out_specs=[any_] * 2,
            scratch_shapes=[dma(2)],
            compiler_params=pltpu.CompilerParams(vmem_limit_bytes=16 << 20),
            name="put",
        )(res[0], res[1])

    return jax.shard_map(local_step, mesh=mesh, in_specs=(spec_act, spec_w, spec_act), out_specs=(spec_act, spec_act), check_vma=False)
```

```python
import functools

import jax
import jax.numpy as jnp
from jax import lax
from jax.experimental import pallas as pl
from jax.experimental.pallas import tpu as pltpu
from jax.sharding import PartitionSpec as P

MESH = pl.DeviceIdType.MESH
BF16, F32 = jnp.bfloat16, jnp.float32
NC = 8
NH = NC // 2


def kernel(x, w, g, dx, dw, pp, qq, xa, wa, rx, ry, gv, vx,
           ss, dr, wr, xr, opp_r, pure_r, xacc_r, yacc_r, fin_r, told):
    h, y, c = lax.axis_index("ro"), lax.axis_index("ri"), lax.axis_index("co")
    o = 1 - h
    tb, dcols = x.shape
    wrows, f = w.shape
    q = wrows // 2
    cr, qr = tb // NC, q // NC
    ft = f // 7
    yn = [lax.rem(y + 1, 4), lax.rem(y + 3, 4)]
    cn = [lax.rem(c + 1, 4), lax.rem(c + 3, 4)]
    y2, c2 = lax.rem(y + 2, 4), lax.rem(c + 2, 4)
    sib = {"ro": o}

    def rc(src, dst, ssem, rsem, dev):
        return pltpu.make_async_remote_copy(src_ref=src, dst_ref=dst, send_sem=ssem, recv_sem=rsem, device_id=dev, device_id_type=MESH)

    def lc(src, dst, sem):
        return pltpu.make_async_copy(src, dst, sem)

    def done(ref, sem):
        lc(ref, ref, sem).wait()

    def xor(a, b):
        return 2 * lax.rem(a // 2 + b // 2, 2) + lax.rem(lax.rem(a, 2) + lax.rem(b, 2), 2)

    bar = pltpu.get_barrier_semaphore()
    partners = [{"co": cn[0], "ro": 0}, {"co": cn[1], "ro": 0}, sib, {"ri": yn[0], "ro": 1}, {"ri": yn[1], "ro": 1}]
    for dev in partners:
        pl.semaphore_signal(bar, 1, device_id=dev, device_id_type=MESH)

    def heard(core):
        @pl.when(h == core)
        def _():
            pl.semaphore_wait(bar, 5)
            pl.semaphore_signal(told, 1, device_id=sib, device_id_type=MESH)

        @pl.when(h != core)
        def _():
            pl.semaphore_wait(told, 1)

    heard(0)

    def xcols(i, k):
        return x.at[:, pl.ds(pl.multiple_of(i * 2 * q + k * q, q), q)]

    def wrow(k):
        return w.at[pl.ds(pl.multiple_of(k * q, q), q)]

    w_dir, x_dir = [], []
    for n in range(2):
        for e in range(2):
            k = h if n == e else o
            w_dir.append(rc(wrow(k), wa.at[y, h], ss.at[0], wr.at[y, h], {"ri": yn[e], "ro": k}))
            for i in range(2):
                x_dir.append(rc(xcols(i, k), xa.at[c, h, i], ss.at[1], xr.at[c, h], {"co": cn[e], "ro": k}))
    for cp in x_dir:
        cp.start()

    def rest(ring_s, fin, ls, outs, ads):
        w_d2d = rc(wrow(o), wa.at[y, h], ss.at[2], wr.at[y, h], sib)
        g_loc = lc(g, gv.at[h], ls.at[0])
        g_d2d = rc(g, gv.at[h], ss.at[3], dr.at[0], sib)
        x_d2d = [rc(xcols(i, o), xa.at[c, h, i], ss.at[4], xr.at[c, h], sib) for i in range(2)]
        for cp in [w_d2d, g_loc, g_d2d] + x_d2d:
            cp.start()
        heard(1)
        for cp in w_dir:
            cp.start()

        w_fwd = [rc(wa.at[yn[1 - e], k], wa.at[yn[1 - e], k], ss.at[0], wr.at[yn[1 - e], k], {"ri": yn[e]}) for e, k in ((0, h), (1, o))]
        x_fwd = [rc(xa.at[cn[1 - e], k], xa.at[cn[1 - e], k], ss.at[1], xr.at[cn[1 - e], k], {"co": cn[e]}) for e, k in ((0, h), (1, o))]

        def got_w(yy, k):
            done(wa.at[yy, k], wr.at[yy, k])

        def got_x(cc, k):
            done(xa.at[cc, k], xr.at[cc, k])

        def sends(a, part, recv, me, axis, nbr, d):
            k = lax.rem(d - me + 4, 4)

            @pl.when(k == 2)
            def _():
                for n in range(2):
                    for e in range(2):
                        half = pl.ds(n * NH, NH)
                        rc(part.at[d, e, half], recv.at[0, e, half], ring_s.at[a], opp_r.at[a, e, n], {axis: nbr[e]}).start()

            for e in range(2):
                @pl.when(k == 1 + 2 * e)
                def _():
                    rc(part.at[d, 1 - e], recv.at[1, e], ring_s.at[a], pure_r.at[a, e], {axis: nbr[e]}).start()

        x_sends = functools.partial(sends, 0, pp, rx, c, "co", cn)
        y_sends = functools.partial(sends, 1, qq, ry, y, "ri", yn)

        def compute(wv, xin, xt, pst, qst):
            for i in range(2):
                lc(xcols(i, h), xin.at[0, i], ls.at[2]).start()

            def p_out(slot, r, yy, m):
                s, ab, hf = 1 - m // 4, lax.rem(m // 2, 2), lax.rem(m, 2)
                return lc(pst.at[slot, r], pp.at[2 * r + yy // 2, ab, pl.ds(s * 4 + hf * 2, 2), :, pl.ds(pl.multiple_of(lax.rem(yy, 2) * q, q), q)], outs.at[slot])

            def p_step(yy, first):
                @pl.when(first)
                def _():
                    lc(wrow(h), wv.at[pl.ds(pl.multiple_of(h * q, q), q)], ls.at[1]).start()
                    lc(wa.at[yy, o], wv.at[pl.ds(pl.multiple_of(o * q, q), q)], ls.at[1]).start()

                @pl.when(jnp.logical_not(first))
                def _():
                    for r in range(2):
                        lc(wa.at[yy, r], wv.at[pl.ds(r * q, q)], ls.at[1]).start()

                done(wv, ls.at[1])

                @pl.loop(0, 8)
                def _(m):
                    @pl.when(first & (m == 4))
                    def _():
                        done(gv.at[o], dr.at[0])

                    s, ab, hf = 1 - m // 4, lax.rem(m // 2, 2), lax.rem(m, 2)
                    t = s * h + (1 - s) * o
                    row = pl.multiple_of(ab * (tb // 2) + hf * (tb // 4), tb // 4)
                    slot = lax.rem(m, 2)

                    @pl.when(m >= 2)
                    def _():
                        done(pst.at[slot], outs.at[slot])

                    res = lax.dot_general(gv[t, pl.ds(row, tb // 4), :], wv[...], (((1,), (1,)), ((), ())), preferred_element_type=F32)
                    for r in range(2):
                        pst[slot, r] = res[:, r * q:(r + 1) * q].reshape(2, cr, q)
                    for r in range(2):
                        p_out(slot, r, yy, m).start()

                for slot in range(2):
                    done(pst.at[slot], outs.at[slot])

            def q_out(slot, r, yy, n):
                s = r * h + (1 - r) * o
                return lc(qst.at[slot, r], qq.at[yy, :, pl.ds(s * 4, 4), :, pl.ds(pl.multiple_of(n * ft, ft), ft)], outs.at[slot])

            def q_step(yy):
                for r in range(2):
                    for t in range(2):
                        lc(xa.at[2 * r + yy // 2, t, lax.rem(yy, 2)], xin.at[r, t], ls.at[3]).start()
                done(xin, ls.at[3])

                @pl.loop(0, NC)
                def _(n):
                    at = pl.ds(pl.multiple_of(n * cr, cr), cr)
                    for r in range(2):
                        for t in range(2):
                            xt[t, r * q:(r + 1) * q, at] = xin[r, t, at, :].T

                @pl.loop(0, 7)
                def _(n):
                    slot = lax.rem(n, 2)

                    @pl.when(n >= 2)
                    def _():
                        done(qst.at[slot], outs.at[slot])

                    at = pl.ds(pl.multiple_of(n * ft, ft), ft)
                    res = jnp.dot(xt[0], gv[0, :, at], preferred_element_type=F32)
                    res += jnp.dot(xt[1], gv[1, :, at], preferred_element_type=F32)
                    for r in range(2):
                        qst[slot, r] = res[r * q:(r + 1) * q].reshape(2, 4, qr, ft)
                    for r in range(2):
                        q_out(slot, r, yy, n).start()

                for slot in range(2):
                    done(qst.at[slot], outs.at[slot])

            op = lax.rem(y // 2 + c + 1, 2)
            even = 1 - lax.rem(y, 2)
            rem1 = even * h + (1 - even) * o

            @pl.loop(0, 8)
            def _(step):
                @pl.when(step == 0)
                def _():
                    done(gv.at[h], ls.at[0])
                    got_w(y, o)

                @pl.when(step == 1)
                def _():
                    done(xin.at[0], ls.at[2])
                    for i in range(2):
                        lc(xin.at[0, i], xa.at[c, h, i], ls.at[2]).start()
                    got_w(yn[1], h)
                    w_fwd[0].start()
                    got_w(yn[0], o)
                    w_fwd[1].start()
                    got_x(cn[1], h)
                    x_fwd[0].start()
                    got_x(cn[0], o)
                    x_fwd[1].start()
                    got_w(xor(y, 1), rem1)

                @pl.when(step == 2)
                def _():
                    x_sends(y // 2)
                    x_sends(2 + y // 2)
                    got_x(cn[1], o)
                    got_x(cn[0], h)
                    done(xin.at[0], ls.at[2])

                @pl.when(step == 3)
                def _():
                    got_x(c, o)
                    got_x(c2, 0)
                    got_x(c2, 1)

                @pl.when(step == 5)
                def _():
                    got_w(3 - y, 1 - rem1)

                @pl.when(step == 6)
                def _():
                    got_w(y2, 0)
                    got_w(y2, 1)

                late = step // 5
                is_p = (step < 2) | ((step >= 5) & (step < 7))
                pn = step - 3 * late
                qn = step - 2 - 2 * (step // 7)
                pcode = pn + pn // 2 - 2 * (pn // 3)
                qa = qn // 2
                qcode = op * ((1 - qa) * (2 + qn) + qa * (3 - qn)) + (1 - op) * lax.rem(qn + 1, 4)

                @pl.when(is_p)
                def _():
                    p_step(xor(y, pcode), step == 0)

                @pl.when(jnp.logical_not(is_p))
                def _():
                    yy = xor(y, qcode)
                    q_step(yy)
                    y_sends(yy)

                @pl.when(step == 6)
                def _():
                    x_sends(1 - y // 2)
                    x_sends(3 - y // 2)

        pl.run_scoped(compute, pltpu.VMEM((2 * q, f), BF16), pltpu.VMEM((2, 2, tb, q), BF16), pltpu.VMEM((2, 2 * q, tb), BF16),
                      pltpu.VMEM((2, 2, 2, cr, q), F32), pltpu.VMEM((2, 2, 2, 4, qr, ft), F32))

        def reduce(ax, ay, bx, by, px):
            rings = ((0, pp, rx, c, cn, "co", ax), (1, qq, ry, y, yn, "ri", ay))

            @pl.loop(0, 2)
            def _(n):
                for a, part, recv, me, nbr, axis, buf in rings:
                    for e in range(2):
                        done(recv.at[0, e, pl.ds(0, NH)], opp_r.at[a, e, n])

                @pl.loop(0, NH)
                def _(i):
                    j = n * NH + i
                    for a, part, recv, me, nbr, axis, buf in rings:
                        for e in range(2):
                            lc(part.at[nbr[e], e, j], buf.at[e, 0], ads.at[a, 0]).start()
                            lc(recv.at[0, e, j], buf.at[e, 1], ads.at[a, 0]).start()
                    for a, part, recv, me, nbr, axis, buf in rings:
                        done(buf.at[:, pl.ds(0, 2)], ads.at[a, 0])
                        for e in range(2):
                            buf[e, 2] = buf[e, 0] + buf[e, 1]
                            lc(buf.at[e, 2], part.at[nbr[e], e, j], ads.at[a, 1]).start()
                    for a, part, recv, me, nbr, axis, buf in rings:
                        done(buf.at[:, 2], ads.at[a, 1])

                    @pl.when(n == 1)
                    def _():
                        for e in range(2):
                            rc(pp.at[cn[e], e, j], vx.at[e, i], ring_s.at[0], xacc_r.at[e, 1 + i], {"co": cn[e]}).start()

                half = pl.ds(n * NH, NH)

                @pl.when(n == 0)
                def _():
                    for e in range(2):
                        rc(pp.at[cn[e], e, half], rx.at[2, e, half], ring_s.at[0], xacc_r.at[e, 0], {"co": cn[e]}).start()

                for e in range(2):
                    rc(qq.at[yn[e], e, half], ry.at[2, e, half], ring_s.at[1], yacc_r.at[e, n], {"ri": yn[e]}).start()

            def x_at(e, j, i):
                return (pl.ds(pl.multiple_of(e * (tb // 2) + j * cr, cr), cr), pl.ds(pl.multiple_of(i * 2 * q + h * q, q), q))

            def y_at(e, j):
                return pl.ds(pl.multiple_of(h * q + e * (q // 2) + j * qr, qr), qr)

            def load(ring, j, third):
                a, part, recv, me, nbr, axis, buf = ring
                for e in range(2):
                    lc(part.at[me, e, j], buf.at[e, 0], ads.at[a, 0]).start()
                    lc(recv.at[1, 1 - e, j], buf.at[e, 1], ads.at[a, 0]).start()
                    if third:
                        lc(recv.at[2, e, j], buf.at[e, 2], ads.at[a, 0]).start()
                done(buf if third else buf.at[:, pl.ds(0, 2)], ads.at[a, 0])

            for a, part, recv, me, nbr, axis, buf in rings:
                for e in range(2):
                    done(recv.at[1, e], pure_r.at[a, e])
            done(wa.at[pl.ds(0, 3)], ss.at[0])
            done(xa.at[pl.ds(0, 3)], ss.at[1])
            done(wa.at[0, 0], ss.at[2])
            done(gv.at[0], ss.at[3])
            done(xa.at[0, 0], ss.at[4])

            for e in range(2):
                done(ry.at[2, e, pl.ds(0, NH)], yacc_r.at[e, 0])

            @pl.loop(0, NH)
            def _(j):
                load(rings[1], j, True)
                for e in range(2):
                    by[e, j] = ay[e, 0] + ay[e, 1] + ay[e, 2]
                    rc(by.at[e, j], dw.at[y_at(e, j)], fin.at[1], fin_r.at[1], sib).start()
                load(rings[1], NH + j, False)
                for e in range(2):
                    dw[y_at(e, j)] = ay[e, 0] + ay[e, 1]

            for e in range(2):
                done(rx.at[2, e, pl.ds(0, NH)], xacc_r.at[e, 0])

            @pl.loop(0, NH)
            def _(j):
                load(rings[0], j, True)
                for e in range(2):
                    bx[e, j] = (ax[e, 0] + ax[e, 1] + ax[e, 2]).astype(BF16)
                    for i in range(2):
                        rc(bx.at[e, j, :, i * q:(i + 1) * q], dx.at[x_at(e, j, i)], fin.at[0], fin_r.at[0], sib).start()
                load(rings[0], NH + j, False)
                for e in range(2):
                    px[e, j] = ax[e, 0] + ax[e, 1]

            for e in range(2):
                done(ry.at[2, e, pl.ds(0, NH)], yacc_r.at[e, 1])

            @pl.loop(0, NH)
            def _(j):
                for e in range(2):
                    lc(ry.at[2, e, NH + j], ay.at[e, 2], ads.at[1, 0]).start()
                done(ay.at[:, 2], ads.at[1, 0])
                for e in range(2):
                    dw[y_at(e, j)] += ay[e, 2]

            for n, ref in enumerate((bx, by)):
                done(ref, fin.at[n])
                done(ref, fin_r.at[n])
            done(ry, ring_s.at[1])

            @pl.loop(0, NH)
            def _(j):
                for e in range(2):
                    done(vx.at[e, j], xacc_r.at[e, 1 + j])
                    tot = px[e, j] + vx[e, j]
                    for i in range(2):
                        dx[x_at(e, j, i)] = tot[:, i * q:(i + 1) * q].astype(BF16)

            done(rx, ring_s.at[0])

        pl.run_scoped(reduce, pltpu.VMEM((2, 3, cr, 2 * q), F32), pltpu.VMEM((2, 3, qr, f), F32),
                      pltpu.VMEM((2, NH, cr, 2 * q), BF16), pltpu.VMEM((2, NH, qr, f), F32), pltpu.VMEM((2, NH, cr, 2 * q), F32))

    dma = pltpu.SemaphoreType.DMA
    pl.run_scoped(rest, dma((2,)), dma((2,)), dma((4,)), dma((2,)), dma((2, 2)))


def put_kernel(a, b, u, v, sems):
    for i, (src, dst) in enumerate(((b, v), (a, u))):
        rows = src.shape[0] // 4
        for n in range(4):
            pltpu.make_async_copy(src.at[pl.ds(n * rows, rows)], dst.at[pl.ds(n * rows, rows)], sems.at[i]).start()
    for i, (src, dst) in enumerate(((b, v), (a, u))):
        pltpu.make_async_copy(src, dst, sems.at[i]).wait()


def solution(mesh):
    spec_act = P(("dp", "ro", "ri"), "co")
    spec_w = P(("ro", "ri"), "co")

    def local_step(x, w, g):
        tb, dcols = x.shape
        wrows, f = w.shape
        q = wrows // 2
        cr, qr = tb // NC, q // NC
        dma = lambda *s: pltpu.SemaphoreType.DMA(s)
        any_ = pl.BlockSpec(memory_space=pl.ANY)
        vmem = pl.BlockSpec(memory_space=pltpu.VMEM)
        shapes = [
            pltpu.VMEM((tb, dcols), BF16),
            pltpu.VMEM((wrows, f), F32),
            jax.ShapeDtypeStruct((4, 2, NC, cr, 2 * q), F32),
            jax.ShapeDtypeStruct((4, 2, NC, qr, f), F32),
            jax.ShapeDtypeStruct((4, 2, 2, tb, q), BF16),
            jax.ShapeDtypeStruct((4, 2, q, f), BF16),
            jax.ShapeDtypeStruct((3, 2, NC, cr, 2 * q), F32),
            jax.ShapeDtypeStruct((3, 2, NC, qr, f), F32),
        ]
        res = pl.pallas_call(
            kernel,
            out_shape=shapes,
            in_specs=[any_] * 3,
            out_specs=[vmem] * 2 + [any_] * (len(shapes) - 2),
            scratch_shapes=[
                pltpu.VMEM((2, tb, f), BF16),
                pltpu.VMEM((2, NH, cr, 2 * q), F32),
                dma(5), dma(1), dma(4, 2), dma(4, 2), dma(2, 2, 2), dma(2, 2), dma(2, 1 + NH), dma(2, 2), dma(2), pltpu.SemaphoreType.REGULAR,
            ],
            compiler_params=pltpu.CompilerParams(collective_id=0, has_side_effects=True, vmem_limit_bytes=52 << 20),
            name="linear_grads",
        )(x, w, g)
        return pl.pallas_call(
            put_kernel,
            out_shape=[jax.ShapeDtypeStruct(r.shape, r.dtype) for r in res[:2]],
            in_specs=[vmem] * 2,
            out_specs=[any_] * 2,
            scratch_shapes=[dma(2)],
            compiler_params=pltpu.CompilerParams(vmem_limit_bytes=16 << 20),
            name="put",
        )(res[0], res[1])

    return jax.shard_map(local_step, mesh=mesh, in_specs=(spec_act, spec_w, spec_act), out_specs=(spec_act, spec_act), check_vma=False)
```

```python
import functools

import jax
import jax.numpy as jnp
from jax import lax
from jax.experimental import pallas as pl
from jax.experimental.pallas import tpu as pltpu
from jax.sharding import PartitionSpec as P

MESH = pl.DeviceIdType.MESH
BF16, F32 = jnp.bfloat16, jnp.float32
NC = 8
NH = NC // 2


def kernel(x, w, g, dx, dw, pp, qq, xa, wa, rx, ry, gv, vx,
           ss, dr, wr, xr, opp_r, pure_r, xacc_r, yacc_r, fin_r, told):
    h, y, c = lax.axis_index("ro"), lax.axis_index("ri"), lax.axis_index("co")
    o = 1 - h
    tb, dcols = x.shape
    wrows, f = w.shape
    q = wrows // 2
    cr, qr = tb // NC, q // NC
    ft = f // 7
    yn = [lax.rem(y + 1, 4), lax.rem(y + 3, 4)]
    cn = [lax.rem(c + 1, 4), lax.rem(c + 3, 4)]
    y2, c2 = lax.rem(y + 2, 4), lax.rem(c + 2, 4)
    sib = {"ro": o}

    def rc(src, dst, ssem, rsem, dev):
        return pltpu.make_async_remote_copy(src_ref=src, dst_ref=dst, send_sem=ssem, recv_sem=rsem, device_id=dev, device_id_type=MESH)

    def lc(src, dst, sem):
        return pltpu.make_async_copy(src, dst, sem)

    def done(ref, sem):
        lc(ref, ref, sem).wait()

    def xor(a, b):
        return 2 * lax.rem(a // 2 + b // 2, 2) + lax.rem(lax.rem(a, 2) + lax.rem(b, 2), 2)

    bar = pltpu.get_barrier_semaphore()
    for e in range(2):
        pl.semaphore_signal(bar, 1, device_id={"co": cn[e]}, device_id_type=MESH)
    for e in range(2):
        pl.semaphore_signal(bar, 1, device_id={"ri": yn[e], "ro": 0}, device_id_type=MESH)

    @pl.when(h == 1)
    def _():
        pl.semaphore_signal(bar, 1, device_id=sib, device_id_type=MESH)
        pl.semaphore_wait(bar, 2)

    @pl.when(h == 0)
    def _():
        pl.semaphore_wait(bar, 7)
        pl.semaphore_signal(told, 1, device_id=sib, device_id_type=MESH)

    def xcols(i, k):
        return x.at[:, pl.ds(pl.multiple_of(i * 2 * q + k * q, q), q)]

    def wrow(k):
        return w.at[pl.ds(pl.multiple_of(k * q, q), q)]

    def x_send(e, k, i):
        return rc(xcols(i, k), xa.at[c, h, i], ss.at[1], xr.at[c, h, i], {"co": cn[e], "ro": k})

    for n in range(2):
        for e in range(2):
            x_send(e, h, n if e == 0 else 1 - n).start()

    pl.semaphore_wait(told, 1)

    @pl.when(h == 1)
    def _():
        pl.semaphore_signal(told, 1, device_id=sib, device_id_type=MESH)

    for n in range(2):
        for e in range(2):
            x_send(e, o, n if e == 0 else 1 - n).start()
    w_dir = [rc(wrow(k), wa.at[y, h], ss.at[0], wr.at[y, h], {"ri": yn[e], "ro": k}) for n in range(2) for e in range(2) for k in [h if n == e else o]]

    def rest(ring_s, fin, ls, outs, ads):
        w_d2d = rc(wrow(o), wa.at[y, h], ss.at[2], wr.at[y, h], sib)
        g_loc = lc(g, gv.at[h], ls.at[0])
        g_d2d = rc(g, gv.at[h], ss.at[3], dr.at[0], sib)
        x_d2d = [rc(xcols(i, o), xa.at[c, h, i], ss.at[4], xr.at[c, h, i], sib) for i in range(2)]
        for cp in [w_d2d, g_loc, g_d2d] + x_d2d:
            cp.start()
        for cp in w_dir:
            cp.start()

        w_fwd = [rc(wa.at[yn[1 - e], k], wa.at[yn[1 - e], k], ss.at[0], wr.at[yn[1 - e], k], {"ri": yn[e]}) for e, k in ((0, h), (1, o))]
        x_fwd = [rc(xa.at[cn[1 - e], t, e], xa.at[cn[1 - e], t, e], ss.at[1], xr.at[cn[1 - e], t, e], {"co": cn[e]}) for e in range(2) for t in range(2)]

        def got_w(yy, k):
            done(wa.at[yy, k], wr.at[yy, k])

        def got_x(cc, i):
            for t in range(2):
                done(xa.at[cc, t, i], xr.at[cc, t, i])

        def sends(a, part, recv, me, axis, nbr, d):
            k = lax.rem(d - me + 4, 4)

            @pl.when(k == 2)
            def _():
                for n in range(2):
                    for e in range(2):
                        half = pl.ds(n * NH, NH)
                        rc(part.at[d, e, half], recv.at[0, e, half], ring_s.at[a], opp_r.at[a, e, n], {axis: nbr[e]}).start()

            for e in range(2):
                @pl.when(k == 1 + 2 * e)
                def _():
                    rc(part.at[d, 1 - e], recv.at[1, e], ring_s.at[a], pure_r.at[a, e], {axis: nbr[e]}).start()

        x_sends = functools.partial(sends, 0, pp, rx, c, "co", cn)
        y_sends = functools.partial(sends, 1, qq, ry, y, "ri", yn)

        def compute(wv, xin, xt, pst, qst):
            for i in range(2):
                lc(xcols(i, h), xin.at[0, i], ls.at[2]).start()

            def p_out(slot, r, yy, m):
                s, ab, hf = 1 - m // 4, lax.rem(m // 2, 2), lax.rem(m, 2)
                return lc(pst.at[slot, r], pp.at[2 * r + yy // 2, ab, pl.ds(s * 4 + hf * 2, 2), :, pl.ds(pl.multiple_of(lax.rem(yy, 2) * q, q), q)], outs.at[slot])

            def p_step(yy, first):
                @pl.when(first)
                def _():
                    lc(wrow(h), wv.at[pl.ds(pl.multiple_of(h * q, q), q)], ls.at[1]).start()
                    lc(wa.at[yy, o], wv.at[pl.ds(pl.multiple_of(o * q, q), q)], ls.at[1]).start()

                @pl.when(jnp.logical_not(first))
                def _():
                    for r in range(2):
                        lc(wa.at[yy, r], wv.at[pl.ds(r * q, q)], ls.at[1]).start()

                done(wv, ls.at[1])

                @pl.loop(0, 8)
                def _(m):
                    @pl.when(first & (m == 4))
                    def _():
                        done(gv.at[o], dr.at[0])

                    s, ab, hf = 1 - m // 4, lax.rem(m // 2, 2), lax.rem(m, 2)
                    t = s * h + (1 - s) * o
                    row = pl.multiple_of(ab * (tb // 2) + hf * (tb // 4), tb // 4)
                    slot = lax.rem(m, 2)

                    @pl.when(m >= 2)
                    def _():
                        done(pst.at[slot], outs.at[slot])

                    res = lax.dot_general(gv[t, pl.ds(row, tb // 4), :], wv[...], (((1,), (1,)), ((), ())), preferred_element_type=F32)
                    for r in range(2):
                        pst[slot, r] = res[:, r * q:(r + 1) * q].reshape(2, cr, q)
                    for r in range(2):
                        p_out(slot, r, yy, m).start()

                for slot in range(2):
                    done(pst.at[slot], outs.at[slot])

            def q_out(slot, r, yy, n):
                s = r * h + (1 - r) * o
                return lc(qst.at[slot, r], qq.at[yy, :, pl.ds(s * 4, 4), :, pl.ds(pl.multiple_of(n * ft, ft), ft)], outs.at[slot])

            def q_step(yy):
                for r in range(2):
                    for t in range(2):
                        lc(xa.at[2 * r + yy // 2, t, lax.rem(yy, 2)], xin.at[r, t], ls.at[3]).start()
                done(xin, ls.at[3])

                @pl.loop(0, NC)
                def _(n):
                    at = pl.ds(pl.multiple_of(n * cr, cr), cr)
                    for r in range(2):
                        for t in range(2):
                            xt[t, r * q:(r + 1) * q, at] = xin[r, t, at, :].T

                @pl.loop(0, 7)
                def _(n):
                    slot = lax.rem(n, 2)

                    @pl.when(n >= 2)
                    def _():
                        done(qst.at[slot], outs.at[slot])

                    at = pl.ds(pl.multiple_of(n * ft, ft), ft)
                    res = jnp.dot(xt[0], gv[0, :, at], preferred_element_type=F32)
                    res += jnp.dot(xt[1], gv[1, :, at], preferred_element_type=F32)
                    for r in range(2):
                        qst[slot, r] = res[r * q:(r + 1) * q].reshape(2, 4, qr, ft)
                    for r in range(2):
                        q_out(slot, r, yy, n).start()

                for slot in range(2):
                    done(qst.at[slot], outs.at[slot])

            op = lax.rem(y // 2 + c + 1, 2)
            even = 1 - lax.rem(y, 2)
            rem1 = even * h + (1 - even) * o

            @pl.loop(0, 8)
            def _(step):
                @pl.when(step == 0)
                def _():
                    done(gv.at[h], ls.at[0])
                    got_w(y, o)

                @pl.when(step == 1)
                def _():
                    done(xin.at[0], ls.at[2])
                    for i in range(2):
                        lc(xin.at[0, i], xa.at[c, h, i], ls.at[2]).start()
                    got_w(yn[1], h)
                    w_fwd[0].start()
                    got_w(yn[0], o)
                    w_fwd[1].start()
                    got_x(cn[1], 0)
                    x_fwd[0].start()
                    x_fwd[1].start()
                    got_x(cn[0], 1)
                    x_fwd[2].start()
                    x_fwd[3].start()
                    got_w(xor(y, 1), rem1)

                @pl.when(step == 2)
                def _():
                    x_sends(y // 2)
                    x_sends(2 + y // 2)
                    got_x(cn[1], 1)
                    got_x(cn[0], 0)
                    done(xin.at[0], ls.at[2])

                @pl.when(step == 3)
                def _():
                    for i in range(2):
                        done(xa.at[c, o, i], xr.at[c, o, i])
                    got_x(c2, 0)
                    got_x(c2, 1)

                @pl.when(step == 5)
                def _():
                    got_w(3 - y, 1 - rem1)

                @pl.when(step == 6)
                def _():
                    got_w(y2, 0)
                    got_w(y2, 1)

                late = step // 5
                is_p = (step < 2) | ((step >= 5) & (step < 7))
                pn = step - 3 * late
                qn = step - 2 - 2 * (step // 7)
                pcode = pn + pn // 2 - 2 * (pn // 3)
                qa = qn // 2
                qcode = op * ((1 - qa) * (2 + qn) + qa * (3 - qn)) + (1 - op) * lax.rem(qn + 1, 4)

                @pl.when(is_p)
                def _():
                    p_step(xor(y, pcode), step == 0)

                @pl.when(jnp.logical_not(is_p))
                def _():
                    yy = xor(y, qcode)
                    q_step(yy)
                    y_sends(yy)

                @pl.when(step == 6)
                def _():
                    x_sends(1 - y // 2)
                    x_sends(3 - y // 2)

        pl.run_scoped(compute, pltpu.VMEM((2 * q, f), BF16), pltpu.VMEM((2, 2, tb, q), BF16), pltpu.VMEM((2, 2 * q, tb), BF16),
                      pltpu.VMEM((2, 2, 2, cr, q), F32), pltpu.VMEM((2, 2, 2, 4, qr, ft), F32))

        def reduce(ax, ay, bx, by, px, sx):
            rings = ((0, pp, rx, c, cn, "co", ax), (1, qq, ry, y, yn, "ri", ay))

            @pl.loop(0, 2)
            def _(n):
                for a, part, recv, me, nbr, axis, buf in rings:
                    for e in range(2):
                        done(recv.at[0, e, pl.ds(0, NH)], opp_r.at[a, e, n])

                @pl.loop(0, NH)
                def _(i):
                    j = n * NH + i
                    for a, part, recv, me, nbr, axis, buf in rings:
                        for e in range(2):
                            lc(part.at[nbr[e], e, j], buf.at[e, 0], ads.at[a, 0]).start()
                            lc(recv.at[0, e, j], buf.at[e, 1], ads.at[a, 0]).start()
                    def back(a):
                        _, part, recv, me, nbr, axis, buf = rings[a]
                        for e in range(2):
                            buf[e, 2] = buf[e, 0] + buf[e, 1]
                        for e in range(2):
                            lc(buf.at[e, 2], part.at[nbr[e], e, j], ads.at[a, 1]).start()
                        done(buf.at[:, 2], ads.at[a, 1])

                    for a in range(2):
                        done(rings[a][6].at[:, pl.ds(0, 2)], ads.at[a, 0])

                    @pl.when(n == 0)
                    def _():
                        back(0)

                    @pl.when(n == 1)
                    def _():
                        for e in range(2):
                            sx[e, i] = ax[e, 0] + ax[e, 1]
                        for e in range(2):
                            rc(sx.at[e, i], vx.at[e, i], ring_s.at[0], xacc_r.at[e, 1 + i], {"co": cn[e]}).start()

                    back(1)

                half = pl.ds(n * NH, NH)

                @pl.when(n == 0)
                def _():
                    for e in range(2):
                        rc(pp.at[cn[e], e, half], rx.at[2, e, half], ring_s.at[0], xacc_r.at[e, 0], {"co": cn[e]}).start()

                for e in range(2):
                    rc(qq.at[yn[e], e, half], ry.at[2, e, half], ring_s.at[1], yacc_r.at[e, n], {"ri": yn[e]}).start()

            def x_at(e, j, i):
                return (pl.ds(pl.multiple_of(e * (tb // 2) + j * cr, cr), cr), pl.ds(pl.multiple_of(i * 2 * q + h * q, q), q))

            def y_at(e, j):
                return pl.ds(pl.multiple_of(h * q + e * (q // 2) + j * qr, qr), qr)

            def load(ring, j, third):
                a, part, recv, me, nbr, axis, buf = ring
                for e in range(2):
                    lc(part.at[me, e, j], buf.at[e, 0], ads.at[a, 0]).start()
                    lc(recv.at[1, 1 - e, j], buf.at[e, 1], ads.at[a, 0]).start()
                    if third:
                        lc(recv.at[2, e, j], buf.at[e, 2], ads.at[a, 0]).start()
                done(buf if third else buf.at[:, pl.ds(0, 2)], ads.at[a, 0])

            for a, part, recv, me, nbr, axis, buf in rings:
                for e in range(2):
                    done(recv.at[1, e], pure_r.at[a, e])
            done(wa.at[pl.ds(0, 3)], ss.at[0])
            done(xa.at[pl.ds(0, 3)], ss.at[1])
            done(wa.at[0, 0], ss.at[2])
            done(gv.at[0], ss.at[3])
            done(xa.at[0, 0], ss.at[4])

            for e in range(2):
                done(ry.at[2, e, pl.ds(0, NH)], yacc_r.at[e, 0])

            @pl.loop(0, NH)
            def _(j):
                load(rings[1], j, True)
                for e in range(2):
                    by[e, j] = ay[e, 0] + ay[e, 1] + ay[e, 2]
                    rc(by.at[e, j], dw.at[y_at(e, j)], fin.at[1], fin_r.at[1], sib).start()
                load(rings[1], NH + j, False)
                for e in range(2):
                    dw[y_at(e, j)] = ay[e, 0] + ay[e, 1]

            for e in range(2):
                done(rx.at[2, e, pl.ds(0, NH)], xacc_r.at[e, 0])

            @pl.loop(0, NH)
            def _(j):
                load(rings[0], j, True)
                for e in range(2):
                    bx[e, j] = (ax[e, 0] + ax[e, 1] + ax[e, 2]).astype(BF16)
                    for i in range(2):
                        rc(bx.at[e, j, :, i * q:(i + 1) * q], dx.at[x_at(e, j, i)], fin.at[0], fin_r.at[0], sib).start()
                load(rings[0], NH + j, False)
                for e in range(2):
                    px[e, j] = ax[e, 0] + ax[e, 1]

            for e in range(2):
                done(ry.at[2, e, pl.ds(0, NH)], yacc_r.at[e, 1])

            @pl.loop(0, NH)
            def _(j):
                for e in range(2):
                    lc(ry.at[2, e, NH + j], ay.at[e, 2], ads.at[1, 0]).start()
                done(ay.at[:, 2], ads.at[1, 0])
                for e in range(2):
                    dw[y_at(e, j)] += ay[e, 2]

            for n, ref in enumerate((bx, by)):
                done(ref, fin.at[n])
                done(ref, fin_r.at[n])
            done(ry, ring_s.at[1])

            @pl.loop(0, NH)
            def _(j):
                for e in range(2):
                    done(vx.at[e, j], xacc_r.at[e, 1 + j])
                    tot = px[e, j] + vx[e, j]
                    for i in range(2):
                        dx[x_at(e, j, i)] = tot[:, i * q:(i + 1) * q].astype(BF16)

            done(rx, ring_s.at[0])

        pl.run_scoped(reduce, pltpu.VMEM((2, 3, cr, 2 * q), F32), pltpu.VMEM((2, 3, qr, f), F32),
                      pltpu.VMEM((2, NH, cr, 2 * q), BF16), pltpu.VMEM((2, NH, qr, f), F32), pltpu.VMEM((2, NH, cr, 2 * q), F32), pltpu.VMEM((2, NH, cr, 2 * q), F32))

    dma = pltpu.SemaphoreType.DMA
    pl.run_scoped(rest, dma((2,)), dma((2,)), dma((4,)), dma((2,)), dma((2, 2)))


def put_kernel(a, b, u, v, sems):
    for i, (src, dst) in enumerate(((b, v), (a, u))):
        rows = src.shape[0] // 4
        for n in range(4):
            pltpu.make_async_copy(src.at[pl.ds(n * rows, rows)], dst.at[pl.ds(n * rows, rows)], sems.at[i]).start()
    for i, (src, dst) in enumerate(((b, v), (a, u))):
        pltpu.make_async_copy(src, dst, sems.at[i]).wait()


def solution(mesh):
    spec_act = P(("dp", "ro", "ri"), "co")
    spec_w = P(("ro", "ri"), "co")

    def local_step(x, w, g):
        tb, dcols = x.shape
        wrows, f = w.shape
        q = wrows // 2
        cr, qr = tb // NC, q // NC
        dma = lambda *s: pltpu.SemaphoreType.DMA(s)
        any_ = pl.BlockSpec(memory_space=pl.ANY)
        vmem = pl.BlockSpec(memory_space=pltpu.VMEM)
        shapes = [
            pltpu.VMEM((tb, dcols), BF16),
            pltpu.VMEM((wrows, f), F32),
            jax.ShapeDtypeStruct((4, 2, NC, cr, 2 * q), F32),
            jax.ShapeDtypeStruct((4, 2, NC, qr, f), F32),
            jax.ShapeDtypeStruct((4, 2, 2, tb, q), BF16),
            jax.ShapeDtypeStruct((4, 2, q, f), BF16),
            jax.ShapeDtypeStruct((3, 2, NC, cr, 2 * q), F32),
            jax.ShapeDtypeStruct((3, 2, NC, qr, f), F32),
        ]
        res = pl.pallas_call(
            kernel,
            out_shape=shapes,
            in_specs=[any_] * 3,
            out_specs=[vmem] * 2 + [any_] * (len(shapes) - 2),
            scratch_shapes=[
                pltpu.VMEM((2, tb, f), BF16),
                pltpu.VMEM((2, NH, cr, 2 * q), F32),
                dma(5), dma(1), dma(4, 2), dma(4, 2, 2), dma(2, 2, 2), dma(2, 2), dma(2, 1 + NH), dma(2, 2), dma(2), pltpu.SemaphoreType.REGULAR,
            ],
            compiler_params=pltpu.CompilerParams(collective_id=0, has_side_effects=True, vmem_limit_bytes=52 << 20),
            name="linear_grads",
        )(x, w, g)
        return pl.pallas_call(
            put_kernel,
            out_shape=[jax.ShapeDtypeStruct(r.shape, r.dtype) for r in res[:2]],
            in_specs=[vmem] * 2,
            out_specs=[any_] * 2,
            scratch_shapes=[dma(2)],
            compiler_params=pltpu.CompilerParams(vmem_limit_bytes=16 << 20),
            name="put",
        )(res[0], res[1])

    return jax.shard_map(local_step, mesh=mesh, in_specs=(spec_act, spec_w, spec_act), out_specs=(spec_act, spec_act), check_vma=False)
```

```python
import functools

import jax
import jax.numpy as jnp
from jax import lax
from jax.experimental import pallas as pl
from jax.experimental.pallas import tpu as pltpu
from jax.sharding import PartitionSpec as P

MESH = pl.DeviceIdType.MESH
BF16, F32 = jnp.bfloat16, jnp.float32
NC = 8
NH = NC // 2


def kernel(x, w, g, dx, dw, pp, qq, xa, wa, rx, ry, gv, vx,
           ss, dr, xr, fin_r, told, inside):
    h, y, c = lax.axis_index("ro"), lax.axis_index("ri"), lax.axis_index("co")
    o = 1 - h
    tb, dcols = x.shape
    wrows, f = w.shape
    q = wrows // 2
    cr, qr = tb // NC, q // NC
    ft = f // 7
    yn = [lax.rem(y + 1, 4), lax.rem(y + 3, 4)]
    cn = [lax.rem(c + 1, 4), lax.rem(c + 3, 4)]
    y2, c2 = lax.rem(y + 2, 4), lax.rem(c + 2, 4)
    sib = {"ro": o}

    def rc(src, dst, ssem, rsem, dev):
        return pltpu.make_async_remote_copy(src_ref=src, dst_ref=dst, send_sem=ssem, recv_sem=rsem, device_id=dev, device_id_type=MESH)

    def lc(src, dst, sem):
        return pltpu.make_async_copy(src, dst, sem)

    def done(ref, sem):
        lc(ref, ref, sem).wait()

    def xor(a, b):
        return 2 * lax.rem(a // 2 + b // 2, 2) + lax.rem(lax.rem(a, 2) + lax.rem(b, 2), 2)

    bar = pltpu.get_barrier_semaphore()
    for e in range(2):
        pl.semaphore_signal(bar, 1, device_id={"co": cn[e]}, device_id_type=MESH)
    for e in range(2):
        pl.semaphore_signal(bar, 1, device_id={"ri": yn[e], "ro": 0}, device_id_type=MESH)

    @pl.when(h == 1)
    def _():
        pl.semaphore_signal(bar, 1, device_id=sib, device_id_type=MESH)
        pl.semaphore_wait(bar, 2)

    @pl.when(h == 0)
    def _():
        pl.semaphore_wait(bar, 7)
        pl.semaphore_signal(told, 1, device_id=sib, device_id_type=MESH)

    def xcols(i, k):
        return x.at[:, pl.ds(pl.multiple_of(i * 2 * q + k * q, q), q)]

    def wrow(k):
        return w.at[pl.ds(pl.multiple_of(k * q, q), q)]

    def x_send(e, k, i):
        return rc(xcols(i, k), xa.at[c, h, i], ss.at[1], xr.at[c, h, i], {"co": cn[e], "ro": k})

    for n in range(2):
        for e in range(2):
            x_send(e, h, n if e == 0 else 1 - n).start()

    pl.semaphore_wait(told, 1)

    @pl.when(h == 1)
    def _():
        pl.semaphore_signal(told, 1, device_id=sib, device_id_type=MESH)

    for n in range(2):
        for e in range(2):
            x_send(e, o, n if e == 0 else 1 - n).start()

    def rest(wr, opp_r, pure_r, xacc_r, yacc_r, ring_s, fin, ls, outs, ads):
        senders = [sib] + [{"ri": yn[e], "ro": k} for e in range(2) for k in range(2)] + [{"co": cn[e]} for e in range(2)]
        for dev in senders:
            pl.semaphore_signal(inside, 1, device_id=dev, device_id_type=MESH)
        w_dir = [rc(wrow(k), wa.at[y, h], ss.at[0], wr.at[y, h], {"ri": yn[e], "ro": k}) for n in range(2) for e in range(2) for k in [h if n == e else o]]
        w_d2d = rc(wrow(o), wa.at[y, h], ss.at[2], wr.at[y, h], sib)
        g_loc = lc(g, gv.at[h], ls.at[0])
        g_d2d = rc(g, gv.at[h], ss.at[3], dr.at[0], sib)
        x_d2d = [rc(xcols(i, o), xa.at[c, h, i], ss.at[4], xr.at[c, h, i], sib) for i in range(2)]
        for cp in [g_loc, g_d2d] + x_d2d:
            cp.start()
        pl.semaphore_wait(inside, len(senders))
        for cp in w_dir + [w_d2d]:
            cp.start()

        w_fwd = [rc(wa.at[yn[1 - e], k], wa.at[yn[1 - e], k], ss.at[0], wr.at[yn[1 - e], k], {"ri": yn[e]}) for e, k in ((0, h), (1, o))]
        x_fwd = [rc(xa.at[cn[1 - e], t, e], xa.at[cn[1 - e], t, e], ss.at[1], xr.at[cn[1 - e], t, e], {"co": cn[e]}) for e in range(2) for t in range(2)]

        def got_w(yy, k):
            done(wa.at[yy, k], wr.at[yy, k])

        def got_x(cc, i):
            for t in range(2):
                done(xa.at[cc, t, i], xr.at[cc, t, i])

        def sends(a, part, recv, me, axis, nbr, d):
            k = lax.rem(d - me + 4, 4)

            @pl.when(k == 2)
            def _():
                for n in range(2):
                    for e in range(2):
                        half = pl.ds(n * NH, NH)
                        rc(part.at[d, e, half], recv.at[0, e, half], ring_s.at[a], opp_r.at[a, e, n], {axis: nbr[e]}).start()

            for e in range(2):
                @pl.when(k == 1 + 2 * e)
                def _():
                    rc(part.at[d, 1 - e], recv.at[1, e], ring_s.at[a], pure_r.at[a, e], {axis: nbr[e]}).start()

        x_sends = functools.partial(sends, 0, pp, rx, c, "co", cn)
        y_sends = functools.partial(sends, 1, qq, ry, y, "ri", yn)

        def compute(wv, xin, xt, pst, qst):
            for i in range(2):
                lc(xcols(i, h), xin.at[0, i], ls.at[2]).start()

            def p_out(slot, r, yy, m):
                s, ab, hf = 1 - m // 4, lax.rem(m // 2, 2), lax.rem(m, 2)
                return lc(pst.at[slot, r], pp.at[2 * r + yy // 2, ab, pl.ds(s * 4 + hf * 2, 2), :, pl.ds(pl.multiple_of(lax.rem(yy, 2) * q, q), q)], outs.at[slot])

            def p_step(yy, first):
                @pl.when(first)
                def _():
                    lc(wrow(h), wv.at[pl.ds(pl.multiple_of(h * q, q), q)], ls.at[1]).start()
                    lc(wa.at[yy, o], wv.at[pl.ds(pl.multiple_of(o * q, q), q)], ls.at[1]).start()

                @pl.when(jnp.logical_not(first))
                def _():
                    for r in range(2):
                        lc(wa.at[yy, r], wv.at[pl.ds(r * q, q)], ls.at[1]).start()

                done(wv, ls.at[1])

                @pl.loop(0, 8)
                def _(m):
                    s, ab, hf = 1 - m // 4, lax.rem(m // 2, 2), lax.rem(m, 2)
                    t = s * h + (1 - s) * o
                    row = pl.multiple_of(ab * (tb // 2) + hf * (tb // 4), tb // 4)
                    slot = lax.rem(m, 2)

                    @pl.when(m >= 2)
                    def _():
                        done(pst.at[slot], outs.at[slot])

                    res = lax.dot_general(gv[t, pl.ds(row, tb // 4), :], wv[...], (((1,), (1,)), ((), ())), preferred_element_type=F32)
                    for r in range(2):
                        pst[slot, r] = res[:, r * q:(r + 1) * q].reshape(2, cr, q)
                    for r in range(2):
                        p_out(slot, r, yy, m).start()

                for slot in range(2):
                    done(pst.at[slot], outs.at[slot])

            def q_out(slot, r, yy, n):
                s = r * h + (1 - r) * o
                return lc(qst.at[slot, r], qq.at[yy, :, pl.ds(s * 4, 4), :, pl.ds(pl.multiple_of(n * ft, ft), ft)], outs.at[slot])

            def q_step(yy):
                for r in range(2):
                    for t in range(2):
                        lc(xa.at[2 * r + yy // 2, t, lax.rem(yy, 2)], xin.at[r, t], ls.at[3]).start()
                done(xin, ls.at[3])

                @pl.loop(0, NC)
                def _(n):
                    at = pl.ds(pl.multiple_of(n * cr, cr), cr)
                    for r in range(2):
                        for t in range(2):
                            xt[t, r * q:(r + 1) * q, at] = xin[r, t, at, :].T

                @pl.loop(0, 7)
                def _(n):
                    slot = lax.rem(n, 2)

                    @pl.when(n >= 2)
                    def _():
                        done(qst.at[slot], outs.at[slot])

                    at = pl.ds(pl.multiple_of(n * ft, ft), ft)
                    res = jnp.dot(xt[0], gv[0, :, at], preferred_element_type=F32)
                    res += jnp.dot(xt[1], gv[1, :, at], preferred_element_type=F32)
                    for r in range(2):
                        qst[slot, r] = res[r * q:(r + 1) * q].reshape(2, 4, qr, ft)
                    for r in range(2):
                        q_out(slot, r, yy, n).start()

                for slot in range(2):
                    done(qst.at[slot], outs.at[slot])

            op = lax.rem(y // 2 + c + 1, 2)
            even = 1 - lax.rem(y, 2)
            rem1 = even * h + (1 - even) * o

            @pl.loop(0, 8)
            def _(step):
                @pl.when(step == 0)
                def _():
                    got_w(y, o)
                    done(gv.at[o], dr.at[0])
                    done(gv.at[h], ls.at[0])

                @pl.when(step == 1)
                def _():
                    done(xin.at[0], ls.at[2])
                    for i in range(2):
                        lc(xin.at[0, i], xa.at[c, h, i], ls.at[2]).start()
                    got_w(yn[1], h)
                    w_fwd[0].start()
                    got_w(yn[0], o)
                    w_fwd[1].start()
                    got_x(cn[1], 0)
                    x_fwd[0].start()
                    x_fwd[1].start()
                    got_x(cn[0], 1)
                    x_fwd[2].start()
                    x_fwd[3].start()
                    got_w(xor(y, 1), rem1)

                @pl.when(step == 2)
                def _():
                    x_sends(y // 2)
                    x_sends(2 + y // 2)
                    got_x(cn[1], 1)
                    got_x(cn[0], 0)
                    done(xin.at[0], ls.at[2])

                @pl.when(step == 3)
                def _():
                    for i in range(2):
                        done(xa.at[c, o, i], xr.at[c, o, i])
                    got_x(c2, 0)
                    got_x(c2, 1)

                @pl.when(step == 5)
                def _():
                    got_w(3 - y, 1 - rem1)

                @pl.when(step == 6)
                def _():
                    got_w(y2, 0)
                    got_w(y2, 1)

                late = step // 5
                is_p = (step < 2) | ((step >= 5) & (step < 7))
                pn = step - 3 * late
                qn = step - 2 - 2 * (step // 7)
                pcode = pn + pn // 2 - 2 * (pn // 3)
                qa = qn // 2
                qcode = op * ((1 - qa) * (2 + qn) + qa * (3 - qn)) + (1 - op) * lax.rem(qn + 1, 4)

                @pl.when(is_p)
                def _():
                    p_step(xor(y, pcode), step == 0)

                @pl.when(jnp.logical_not(is_p))
                def _():
                    yy = xor(y, qcode)
                    q_step(yy)
                    y_sends(yy)

                @pl.when(step == 6)
                def _():
                    x_sends(1 - y // 2)
                    x_sends(3 - y // 2)

        pl.run_scoped(compute, pltpu.VMEM((2 * q, f), BF16), pltpu.VMEM((2, 2, tb, q), BF16), pltpu.VMEM((2, 2 * q, tb), BF16),
                      pltpu.VMEM((2, 2, 2, cr, q), F32), pltpu.VMEM((2, 2, 2, 4, qr, ft), F32))

        def reduce(ax, ay, bx, by, px, sx):
            rings = ((0, pp, rx, c, cn, "co", ax), (1, qq, ry, y, yn, "ri", ay))

            @pl.loop(0, 2)
            def _(n):
                for a, part, recv, me, nbr, axis, buf in rings:
                    for e in range(2):
                        done(recv.at[0, e, pl.ds(0, NH)], opp_r.at[a, e, n])

                @pl.loop(0, NH)
                def _(i):
                    j = n * NH + i
                    for a, part, recv, me, nbr, axis, buf in rings:
                        for e in range(2):
                            lc(part.at[nbr[e], e, j], buf.at[e, 0], ads.at[a, 0]).start()
                            lc(recv.at[0, e, j], buf.at[e, 1], ads.at[a, 0]).start()
                    def back(a):
                        _, part, recv, me, nbr, axis, buf = rings[a]
                        for e in range(2):
                            buf[e, 2] = buf[e, 0] + buf[e, 1]
                        for e in range(2):
                            lc(buf.at[e, 2], part.at[nbr[e], e, j], ads.at[a, 1]).start()
                        done(buf.at[:, 2], ads.at[a, 1])

                    for a in range(2):
                        done(rings[a][6].at[:, pl.ds(0, 2)], ads.at[a, 0])

                    @pl.when(n == 0)
                    def _():
                        back(0)

                    @pl.when(n == 1)
                    def _():
                        for e in range(2):
                            sx[e, i] = ax[e, 0] + ax[e, 1]
                        for e in range(2):
                            rc(sx.at[e, i], vx.at[e, i], ring_s.at[0], xacc_r.at[e, 1 + i], {"co": cn[e]}).start()

                    back(1)

                half = pl.ds(n * NH, NH)

                @pl.when(n == 0)
                def _():
                    for e in range(2):
                        rc(pp.at[cn[e], e, half], rx.at[2, e, half], ring_s.at[0], xacc_r.at[e, 0], {"co": cn[e]}).start()

                for e in range(2):
                    rc(qq.at[yn[e], e, half], ry.at[2, e, half], ring_s.at[1], yacc_r.at[e, n], {"ri": yn[e]}).start()

            def x_at(e, j, i):
                return (pl.ds(pl.multiple_of(e * (tb // 2) + j * cr, cr), cr), pl.ds(pl.multiple_of(i * 2 * q + h * q, q), q))

            def y_at(e, j):
                return pl.ds(pl.multiple_of(h * q + e * (q // 2) + j * qr, qr), qr)

            def load(ring, j, third):
                a, part, recv, me, nbr, axis, buf = ring
                for e in range(2):
                    lc(part.at[me, e, j], buf.at[e, 0], ads.at[a, 0]).start()
                    lc(recv.at[1, 1 - e, j], buf.at[e, 1], ads.at[a, 0]).start()
                    if third:
                        lc(recv.at[2, e, j], buf.at[e, 2], ads.at[a, 0]).start()
                done(buf if third else buf.at[:, pl.ds(0, 2)], ads.at[a, 0])

            for a, part, recv, me, nbr, axis, buf in rings:
                for e in range(2):
                    done(recv.at[1, e], pure_r.at[a, e])
            done(wa.at[pl.ds(0, 3)], ss.at[0])
            done(xa.at[pl.ds(0, 3)], ss.at[1])
            done(wa.at[0, 0], ss.at[2])
            done(gv.at[0], ss.at[3])
            done(xa.at[0, 0], ss.at[4])

            for e in range(2):
                done(ry.at[2, e, pl.ds(0, NH)], yacc_r.at[e, 0])

            @pl.loop(0, NH)
            def _(j):
                load(rings[1], j, True)
                for e in range(2):
                    by[e, j] = ay[e, 0] + ay[e, 1] + ay[e, 2]
                    rc(by.at[e, j], dw.at[y_at(e, j)], fin.at[1], fin_r.at[1], sib).start()
                load(rings[1], NH + j, False)
                for e in range(2):
                    dw[y_at(e, j)] = ay[e, 0] + ay[e, 1]

            for e in range(2):
                done(rx.at[2, e, pl.ds(0, NH)], xacc_r.at[e, 0])

            @pl.loop(0, NH)
            def _(j):
                load(rings[0], j, True)
                for e in range(2):
                    bx[e, j] = (ax[e, 0] + ax[e, 1] + ax[e, 2]).astype(BF16)
                    for i in range(2):
                        rc(bx.at[e, j, :, i * q:(i + 1) * q], dx.at[x_at(e, j, i)], fin.at[0], fin_r.at[0], sib).start()
                load(rings[0], NH + j, False)
                for e in range(2):
                    px[e, j] = ax[e, 0] + ax[e, 1]

            for e in range(2):
                done(ry.at[2, e, pl.ds(0, NH)], yacc_r.at[e, 1])

            @pl.loop(0, NH)
            def _(j):
                for e in range(2):
                    lc(ry.at[2, e, NH + j], ay.at[e, 2], ads.at[1, 0]).start()
                done(ay.at[:, 2], ads.at[1, 0])
                for e in range(2):
                    dw[y_at(e, j)] += ay[e, 2]

            for n, ref in enumerate((bx, by)):
                done(ref, fin.at[n])
                done(ref, fin_r.at[n])
            done(ry, ring_s.at[1])

            @pl.loop(0, NH)
            def _(j):
                for e in range(2):
                    done(vx.at[e, j], xacc_r.at[e, 1 + j])
                    tot = px[e, j] + vx[e, j]
                    for i in range(2):
                        dx[x_at(e, j, i)] = tot[:, i * q:(i + 1) * q].astype(BF16)

            done(rx, ring_s.at[0])

        pl.run_scoped(reduce, pltpu.VMEM((2, 3, cr, 2 * q), F32), pltpu.VMEM((2, 3, qr, f), F32),
                      pltpu.VMEM((2, NH, cr, 2 * q), BF16), pltpu.VMEM((2, NH, qr, f), F32), pltpu.VMEM((2, NH, cr, 2 * q), F32), pltpu.VMEM((2, NH, cr, 2 * q), F32))

    dma = pltpu.SemaphoreType.DMA
    pl.run_scoped(rest, dma((4, 2)), dma((2, 2, 2)), dma((2, 2)), dma((2, 1 + NH)), dma((2, 2)), dma((2,)), dma((2,)), dma((4,)), dma((2,)), dma((2, 2)))


def put_kernel(a, b, u, v, sems):
    for i, (src, dst) in enumerate(((b, v), (a, u))):
        rows = src.shape[0] // 8
        for n in range(8):
            pltpu.make_async_copy(src.at[pl.ds(n * rows, rows)], dst.at[pl.ds(n * rows, rows)], sems.at[i]).start()
    for i, (src, dst) in enumerate(((b, v), (a, u))):
        pltpu.make_async_copy(src, dst, sems.at[i]).wait()


def solution(mesh):
    spec_act = P(("dp", "ro", "ri"), "co")
    spec_w = P(("ro", "ri"), "co")

    def local_step(x, w, g):
        tb, dcols = x.shape
        wrows, f = w.shape
        q = wrows // 2
        cr, qr = tb // NC, q // NC
        dma = lambda *s: pltpu.SemaphoreType.DMA(s)
        any_ = pl.BlockSpec(memory_space=pl.ANY)
        vmem = pl.BlockSpec(memory_space=pltpu.VMEM)
        shapes = [
            pltpu.VMEM((tb, dcols), BF16),
            pltpu.VMEM((wrows, f), F32),
            jax.ShapeDtypeStruct((4, 2, NC, cr, 2 * q), F32),
            jax.ShapeDtypeStruct((4, 2, NC, qr, f), F32),
            jax.ShapeDtypeStruct((4, 2, 2, tb, q), BF16),
            jax.ShapeDtypeStruct((4, 2, q, f), BF16),
            jax.ShapeDtypeStruct((3, 2, NC, cr, 2 * q), F32),
            jax.ShapeDtypeStruct((3, 2, NC, qr, f), F32),
        ]
        res = pl.pallas_call(
            kernel,
            out_shape=shapes,
            in_specs=[any_] * 3,
            out_specs=[vmem] * 2 + [any_] * (len(shapes) - 2),
            scratch_shapes=[
                pltpu.VMEM((2, tb, f), BF16),
                pltpu.VMEM((2, NH, cr, 2 * q), F32),
                dma(5), dma(1), dma(4, 2, 2), dma(2), pltpu.SemaphoreType.REGULAR, pltpu.SemaphoreType.REGULAR,
            ],
            compiler_params=pltpu.CompilerParams(collective_id=0, has_side_effects=True, vmem_limit_bytes=52 << 20),
            name="linear_grads",
        )(x, w, g)
        return pl.pallas_call(
            put_kernel,
            out_shape=[jax.ShapeDtypeStruct(r.shape, r.dtype) for r in res[:2]],
            in_specs=[vmem] * 2,
            out_specs=[any_] * 2,
            scratch_shapes=[dma(2)],
            compiler_params=pltpu.CompilerParams(vmem_limit_bytes=16 << 20),
            name="put",
        )(res[0], res[1])

    return jax.shard_map(local_step, mesh=mesh, in_specs=(spec_act, spec_w, spec_act), out_specs=(spec_act, spec_act), check_vma=False)
```

```python
import functools

import jax
import jax.numpy as jnp
from jax import lax
from jax.experimental import pallas as pl
from jax.experimental.pallas import tpu as pltpu
from jax.sharding import PartitionSpec as P

MESH = pl.DeviceIdType.MESH
BF16, F32 = jnp.bfloat16, jnp.float32
NC = 8
NH = NC // 2


def kernel(x, w, g, dx, dw, pp, qq, xa, wa, rx, ry, gv, vx,
           xs, xr, told, inside):
    h, y, c = lax.axis_index("ro"), lax.axis_index("ri"), lax.axis_index("co")
    o = 1 - h
    tb, dcols = x.shape
    wrows, f = w.shape
    q = wrows // 2
    cr, qr = tb // NC, q // NC
    ft = f // 7
    yn = [lax.rem(y + 1, 4), lax.rem(y + 3, 4)]
    cn = [lax.rem(c + 1, 4), lax.rem(c + 3, 4)]
    y2, c2 = lax.rem(y + 2, 4), lax.rem(c + 2, 4)
    sib = {"ro": o}

    def rc(src, dst, ssem, rsem, dev):
        return pltpu.make_async_remote_copy(src_ref=src, dst_ref=dst, send_sem=ssem, recv_sem=rsem, device_id=dev, device_id_type=MESH)

    def lc(src, dst, sem):
        return pltpu.make_async_copy(src, dst, sem)

    def done(ref, sem):
        lc(ref, ref, sem).wait()

    def xor(a, b):
        return 2 * lax.rem(a // 2 + b // 2, 2) + lax.rem(lax.rem(a, 2) + lax.rem(b, 2), 2)

    def xcols(i, k):
        return x.at[:, pl.ds(pl.multiple_of(i * 2 * q + k * q, q), q)]

    def wrow(k):
        return w.at[pl.ds(pl.multiple_of(k * q, q), q)]

    bar = pltpu.get_barrier_semaphore()
    for e in range(2):
        pl.semaphore_signal(bar, 1, device_id={"co": cn[e]}, device_id_type=MESH)
    for e in range(2):
        pl.semaphore_signal(bar, 1, device_id={"ri": yn[e], "ro": 0}, device_id_type=MESH)

    @pl.when(h == 1)
    def _():
        pl.semaphore_signal(bar, 1, device_id=sib, device_id_type=MESH)
        pl.semaphore_wait(bar, 2)

    @pl.when(h == 0)
    def _():
        pl.semaphore_wait(bar, 7)
        pl.semaphore_signal(told, 1, device_id=sib, device_id_type=MESH)

    def x_send(e, k, i):
        return rc(xcols(i, k), xa.at[c, h, i], xs.at[0], xr.at[c, h, i], {"co": cn[e], "ro": k})

    for n in range(2):
        for e in range(2):
            x_send(e, h, n if e == 0 else 1 - n).start()

    pl.semaphore_wait(told, 1)

    @pl.when(h == 1)
    def _():
        pl.semaphore_signal(told, 1, device_id=sib, device_id_type=MESH)

    for n in range(2):
        for e in range(2):
            x_send(e, o, n if e == 0 else 1 - n).start()

    def rest(wr, dr, opp_r, pure_r, xacc_r, yacc_r, fin_r, ss, ring_s, fin, ls, outs, ads):
        senders = [sib] + [{"ri": yn[e], "ro": k} for e in range(2) for k in range(2)] + [{"co": cn[e]} for e in range(2)]
        for dev in senders:
            pl.semaphore_signal(inside, 1, device_id=dev, device_id_type=MESH)
        w_dir = [rc(wrow(k), wa.at[y, h], ss.at[0], wr.at[y, h], {"ri": yn[e], "ro": k}) for n in range(2) for e in range(2) for k in [h if n == e else o]]
        w_d2d = rc(wrow(o), wa.at[y, h], ss.at[2], wr.at[y, h], sib)
        g_loc = lc(g, gv.at[h], ls.at[0])
        g_d2d = rc(g, gv.at[h], ss.at[3], dr.at[0], sib)
        x_d2d = [rc(xcols(i, o), xa.at[c, h, i], ss.at[1], xr.at[c, h, i], sib) for i in range(2)]
        for cp in [g_loc] + x_d2d:
            cp.start()
        pl.semaphore_wait(inside, len(senders))
        for cp in w_dir + [w_d2d, g_d2d]:
            cp.start()

        w_fwd = [rc(wa.at[yn[1 - e], k], wa.at[yn[1 - e], k], ss.at[0], wr.at[yn[1 - e], k], {"ri": yn[e]}) for e, k in ((0, h), (1, o))]
        x_fwd = [rc(xa.at[cn[1 - e], t, e], xa.at[cn[1 - e], t, e], xs.at[0], xr.at[cn[1 - e], t, e], {"co": cn[e]}) for e in range(2) for t in range(2)]

        def got_w(yy, k):
            done(wa.at[yy, k], wr.at[yy, k])

        def got_x(cc, i):
            for t in range(2):
                done(xa.at[cc, t, i], xr.at[cc, t, i])

        def sends(a, part, recv, me, axis, nbr, d):
            k = lax.rem(d - me + 4, 4)

            @pl.when(k == 2)
            def _():
                for n in range(2):
                    for e in range(2):
                        half = pl.ds(n * NH, NH)
                        rc(part.at[d, e, half], recv.at[0, e, half], ring_s.at[a], opp_r.at[a, e, n], {axis: nbr[e]}).start()

            for e in range(2):
                @pl.when(k == 1 + 2 * e)
                def _():
                    rc(part.at[d, 1 - e], recv.at[1, e], ring_s.at[a], pure_r.at[a, e], {axis: nbr[e]}).start()

        x_sends = functools.partial(sends, 0, pp, rx, c, "co", cn)
        y_sends = functools.partial(sends, 1, qq, ry, y, "ri", yn)

        def compute(wv, xin, xt, pst, qst):
            for i in range(2):
                lc(xcols(i, h), xin.at[0, i], ls.at[3]).start()

            def p_out(slot, r, yy, m):
                s, ab, hf = 1 - m // 4, lax.rem(m // 2, 2), lax.rem(m, 2)
                return lc(pst.at[slot, r], pp.at[2 * r + yy // 2, ab, pl.ds(s * 4 + hf * 2, 2), :, pl.ds(pl.multiple_of(lax.rem(yy, 2) * q, q), q)], outs.at[slot])

            def load_w(yy, r):
                lc(wa.at[yy, r], wv.at[pl.ds(pl.multiple_of(r * q, q), q)], ls.at[1]).start()

            def p_step(yy):
                done(wv, ls.at[1])

                @pl.loop(0, 8)
                def _(m):
                    s, ab, hf = 1 - m // 4, lax.rem(m // 2, 2), lax.rem(m, 2)
                    t = s * h + (1 - s) * o
                    row = pl.multiple_of(ab * (tb // 2) + hf * (tb // 4), tb // 4)
                    slot = lax.rem(m, 2)

                    @pl.when(m >= 2)
                    def _():
                        done(pst.at[slot], outs.at[slot])

                    res = lax.dot_general(gv[t, pl.ds(row, tb // 4), :], wv[...], (((1,), (1,)), ((), ())), preferred_element_type=F32)
                    for r in range(2):
                        pst[slot, r] = res[:, r * q:(r + 1) * q].reshape(2, cr, q)
                    for r in range(2):
                        p_out(slot, r, yy, m).start()

                for slot in range(2):
                    done(pst.at[slot], outs.at[slot])

            def q_out(slot, r, yy, n):
                s = r * h + (1 - r) * o
                return lc(qst.at[slot, r], qq.at[yy, :, pl.ds(s * 4, 4), :, pl.ds(pl.multiple_of(n * ft, ft), ft)], outs.at[slot])

            def load_x(yy):
                for r in range(2):
                    for t in range(2):
                        lc(xa.at[2 * r + yy // 2, t, lax.rem(yy, 2)], xin.at[r, t], ls.at[4]).start()

            def q_step(yy, yy_next, qn):
                @pl.when(qn < 2)
                def _():
                    load_x(yy)

                done(xin, ls.at[4])

                @pl.loop(0, NC)
                def _(n):
                    at = pl.ds(pl.multiple_of(n * cr, cr), cr)
                    for r in range(2):
                        for t in range(2):
                            xt[t, r * q:(r + 1) * q, at] = xin[r, t, at, :].T

                @pl.when((qn == 1) | (qn == 2))
                def _():
                    load_x(yy_next)

                @pl.loop(0, 7)
                def _(n):
                    slot = lax.rem(n, 2)

                    @pl.when(n >= 2)
                    def _():
                        done(qst.at[slot], outs.at[slot])

                    at = pl.ds(pl.multiple_of(n * ft, ft), ft)
                    res = jnp.dot(xt[0], gv[0, :, at], preferred_element_type=F32)
                    res += jnp.dot(xt[1], gv[1, :, at], preferred_element_type=F32)
                    for r in range(2):
                        qst[slot, r] = res[r * q:(r + 1) * q].reshape(2, 4, qr, ft)
                    for r in range(2):
                        q_out(slot, r, yy, n).start()

                for slot in range(2):
                    done(qst.at[slot], outs.at[slot])

            op = lax.rem(y // 2 + c + 1, 2)

            def qcode(n):
                return op * ((1 - n // 2) * (2 + n) + n // 2 * (3 - n)) + (1 - op) * lax.rem(n + 1, 4)

            even = 1 - lax.rem(y, 2)
            rem1 = even * h + (1 - even) * o

            @pl.loop(0, 8)
            def _(step):
                @pl.when(step == 0)
                def _():
                    lc(wrow(h), wv.at[pl.ds(pl.multiple_of(h * q, q), q)], ls.at[1]).start()
                    got_w(y, o)
                    load_w(y, o)
                    done(gv.at[o], dr.at[0])
                    done(gv.at[h], ls.at[0])

                @pl.when(step == 1)
                def _():
                    done(xin.at[0], ls.at[3])
                    for i in range(2):
                        lc(xin.at[0, i], xa.at[c, h, i], ls.at[3]).start()
                    got_w(yn[1], h)
                    w_fwd[0].start()
                    got_w(yn[0], o)
                    w_fwd[1].start()
                    got_x(cn[1], 0)
                    x_fwd[0].start()
                    x_fwd[1].start()
                    got_x(cn[0], 1)
                    x_fwd[2].start()
                    x_fwd[3].start()
                    load_w(xor(y, 1), 1 - rem1)
                    got_w(xor(y, 1), rem1)
                    load_w(xor(y, 1), rem1)

                @pl.when(step == 2)
                def _():
                    x_sends(y // 2)
                    x_sends(2 + y // 2)
                    got_x(cn[1], 1)
                    got_x(cn[0], 0)
                    done(xin.at[0], ls.at[3])

                @pl.when(step == 3)
                def _():
                    for i in range(2):
                        done(xa.at[c, o, i], xr.at[c, o, i])
                    got_x(c2, 0)
                    got_x(c2, 1)
                    got_w(3 - y, 1 - rem1)
                    for r in range(2):
                        load_w(3 - y, r)
                        got_w(y2, r)

                @pl.when(step == 6)
                def _():
                    for r in range(2):
                        load_w(y2, r)

                late = step // 5
                is_p = (step < 2) | ((step >= 5) & (step < 7))
                pn = step - 3 * late
                qn = step - 2 - 2 * (step // 7)
                pcode = pn + pn // 2 - 2 * (pn // 3)
                @pl.when(is_p)
                def _():
                    p_step(xor(y, pcode))

                @pl.when(jnp.logical_not(is_p))
                def _():
                    yy = xor(y, qcode(qn))
                    q_step(yy, xor(y, qcode(lax.rem(qn + 1, 4))), qn)
                    y_sends(yy)

                @pl.when(step == 6)
                def _():
                    x_sends(1 - y // 2)
                    x_sends(3 - y // 2)

        pl.run_scoped(compute, pltpu.VMEM((2 * q, f), BF16), pltpu.VMEM((2, 2, tb, q), BF16), pltpu.VMEM((2, 2 * q, tb), BF16),
                      pltpu.VMEM((2, 2, 2, cr, q), F32), pltpu.VMEM((2, 2, 2, 4, qr, ft), F32))

        def reduce(ax, ay, bx, by, px, sx):
            rings = ((0, pp, rx, c, cn, "co", ax), (1, qq, ry, y, yn, "ri", ay))

            def x_at(e, j, i):
                return (pl.ds(pl.multiple_of(e * (tb // 2) + j * cr, cr), cr), pl.ds(pl.multiple_of(i * 2 * q + h * q, q), q))

            def y_at(e, j):
                return pl.ds(pl.multiple_of(h * q + e * (q // 2) + j * qr, qr), qr)

            for e in range(2):
                lc(pp.at[c, e, pl.ds(NH, NH)], px.at[e], ls.at[0]).start()
                lc(qq.at[y, e, pl.ds(0, NH)], by.at[e], ls.at[1]).start()
                for j in range(NH):
                    lc(qq.at[y, e, NH + j], dw.at[y_at(e, j)], ls.at[2]).start()

            @pl.loop(0, 2)
            def _(n):
                for a, part, recv, me, nbr, axis, buf in rings:
                    for e in range(2):
                        done(recv.at[0, e, pl.ds(0, NH)], opp_r.at[a, e, n])

                @pl.loop(0, NH)
                def _(i):
                    j = n * NH + i
                    for a, part, recv, me, nbr, axis, buf in rings:
                        for e in range(2):
                            lc(part.at[nbr[e], e, j], buf.at[e, 0], ads.at[a, 0]).start()
                            lc(recv.at[0, e, j], buf.at[e, 1], ads.at[a, 0]).start()
                    def back(a):
                        _, part, recv, me, nbr, axis, buf = rings[a]
                        for e in range(2):
                            buf[e, 2] = buf[e, 0] + buf[e, 1]
                        for e in range(2):
                            lc(buf.at[e, 2], part.at[nbr[e], e, j], ads.at[a, 1]).start()
                        done(buf.at[:, 2], ads.at[a, 1])

                    for a in range(2):
                        done(rings[a][6].at[:, pl.ds(0, 2)], ads.at[a, 0])

                    @pl.when(n == 0)
                    def _():
                        back(0)

                    @pl.when(n == 1)
                    def _():
                        for e in range(2):
                            sx[e, i] = ax[e, 0] + ax[e, 1]
                        for e in range(2):
                            rc(sx.at[e, i], vx.at[e, i], ring_s.at[0], xacc_r.at[e, 1 + i], {"co": cn[e]}).start()

                    back(1)

                half = pl.ds(n * NH, NH)

                @pl.when(n == 0)
                def _():
                    for e in range(2):
                        rc(pp.at[cn[e], e, half], rx.at[2, e, half], ring_s.at[0], xacc_r.at[e, 0], {"co": cn[e]}).start()

                for e in range(2):
                    rc(qq.at[yn[e], e, half], ry.at[2, e, half], ring_s.at[1], yacc_r.at[e, n], {"ri": yn[e]}).start()

            for a, part, recv, me, nbr, axis, buf in rings:
                for e in range(2):
                    done(recv.at[1, e], pure_r.at[a, e])
            done(wa.at[pl.ds(0, 3)], ss.at[0])
            done(xa.at[pl.ds(0, 3)], xs.at[0])
            done(wa.at[0, 0], ss.at[2])
            done(gv.at[0], ss.at[3])
            done(xa.at[0, 0], ss.at[1])

            done(px, ls.at[0])
            done(by, ls.at[1])
            done(by, ls.at[2])

            for e in range(2):
                done(ry.at[2, e, pl.ds(0, NH)], yacc_r.at[e, 0])

            @pl.loop(0, NH)
            def _(j):
                for e in range(2):
                    lc(ry.at[1, 1 - e, NH + j], ay.at[e, 0], ads.at[1, 0]).start()
                    lc(ry.at[1, 1 - e, j], ay.at[e, 1], ads.at[1, 0]).start()
                    lc(ry.at[2, e, j], ay.at[e, 2], ads.at[1, 0]).start()
                    lc(rx.at[1, 1 - e, NH + j], ax.at[e, 0], ads.at[0, 0]).start()
                done(ay, ads.at[1, 0])
                for e in range(2):
                    by[e, j] = by[e, j] + ay[e, 1] + ay[e, 2]
                    rc(by.at[e, j], dw.at[y_at(e, j)], fin.at[1], fin_r.at[1], sib).start()
                for e in range(2):
                    dw[y_at(e, j)] += ay[e, 0]
                done(ax.at[:, 0], ads.at[0, 0])
                for e in range(2):
                    px[e, j] += ax[e, 0]

            for e in range(2):
                done(rx.at[2, e, pl.ds(0, NH)], xacc_r.at[e, 0])

            @pl.loop(0, NH)
            def _(j):
                for e in range(2):
                    lc(pp.at[c, e, j], ax.at[e, 0], ads.at[0, 0]).start()
                    lc(rx.at[1, 1 - e, j], ax.at[e, 1], ads.at[0, 0]).start()
                    lc(rx.at[2, e, j], ax.at[e, 2], ads.at[0, 0]).start()
                done(ax, ads.at[0, 0])
                for e in range(2):
                    bx[e, j] = (ax[e, 0] + ax[e, 1] + ax[e, 2]).astype(BF16)
                    for i in range(2):
                        rc(bx.at[e, j, :, i * q:(i + 1) * q], dx.at[x_at(e, j, i)], fin.at[0], fin_r.at[0], sib).start()

            for e in range(2):
                done(ry.at[2, e, pl.ds(0, NH)], yacc_r.at[e, 1])

            @pl.loop(0, NH)
            def _(j):
                for e in range(2):
                    lc(ry.at[2, e, NH + j], ay.at[e, 2], ads.at[1, 0]).start()
                done(ay.at[:, 2], ads.at[1, 0])
                for e in range(2):
                    dw[y_at(e, j)] += ay[e, 2]

            for n, ref in enumerate((bx, by)):
                done(ref, fin.at[n])
                done(ref, fin_r.at[n])
            done(ry, ring_s.at[1])

            @pl.loop(0, NH)
            def _(j):
                for e in range(2):
                    done(vx.at[e, j], xacc_r.at[e, 1 + j])
                    tot = px[e, j] + vx[e, j]
                    for i in range(2):
                        dx[x_at(e, j, i)] = tot[:, i * q:(i + 1) * q].astype(BF16)

            done(rx, ring_s.at[0])

        pl.run_scoped(reduce, pltpu.VMEM((2, 3, cr, 2 * q), F32), pltpu.VMEM((2, 3, qr, f), F32),
                      pltpu.VMEM((2, NH, cr, 2 * q), BF16), pltpu.VMEM((2, NH, qr, f), F32), pltpu.VMEM((2, NH, cr, 2 * q), F32), pltpu.VMEM((2, NH, cr, 2 * q), F32))

    dma = pltpu.SemaphoreType.DMA
    pl.run_scoped(rest, dma((4, 2)), dma((1,)), dma((2, 2, 2)), dma((2, 2)), dma((2, 1 + NH)), dma((2, 2)), dma((2,)), dma((4,)), dma((2,)), dma((2,)), dma((5,)), dma((2,)), dma((2, 2)))


def put_kernel(a, b, u, v, sems):
    for i, (src, dst) in enumerate(((b, v), (a, u))):
        rows = src.shape[0] // 8
        for n in range(8):
            pltpu.make_async_copy(src.at[pl.ds(n * rows, rows)], dst.at[pl.ds(n * rows, rows)], sems.at[i]).start()
    for i, (src, dst) in enumerate(((b, v), (a, u))):
        pltpu.make_async_copy(src, dst, sems.at[i]).wait()


def solution(mesh):
    spec_act = P(("dp", "ro", "ri"), "co")
    spec_w = P(("ro", "ri"), "co")

    def local_step(x, w, g):
        tb, dcols = x.shape
        wrows, f = w.shape
        q = wrows // 2
        cr, qr = tb // NC, q // NC
        dma = lambda *s: pltpu.SemaphoreType.DMA(s)
        any_ = pl.BlockSpec(memory_space=pl.ANY)
        vmem = pl.BlockSpec(memory_space=pltpu.VMEM)
        shapes = [
            pltpu.VMEM((tb, dcols), BF16),
            pltpu.VMEM((wrows, f), F32),
            jax.ShapeDtypeStruct((4, 2, NC, cr, 2 * q), F32),
            jax.ShapeDtypeStruct((4, 2, NC, qr, f), F32),
            jax.ShapeDtypeStruct((4, 2, 2, tb, q), BF16),
            jax.ShapeDtypeStruct((4, 2, q, f), BF16),
            jax.ShapeDtypeStruct((3, 2, NC, cr, 2 * q), F32),
            jax.ShapeDtypeStruct((3, 2, NC, qr, f), F32),
        ]
        res = pl.pallas_call(
            kernel,
            out_shape=shapes,
            in_specs=[any_] * 3,
            out_specs=[vmem] * 2 + [any_] * (len(shapes) - 2),
            scratch_shapes=[
                pltpu.VMEM((2, tb, f), BF16),
                pltpu.VMEM((2, NH, cr, 2 * q), F32),
                dma(1), dma(4, 2, 2), pltpu.SemaphoreType.REGULAR, pltpu.SemaphoreType.REGULAR,
            ],
            compiler_params=pltpu.CompilerParams(collective_id=0, has_side_effects=True, vmem_limit_bytes=52 << 20),
            name="linear_grads",
        )(x, w, g)
        return pl.pallas_call(
            put_kernel,
            out_shape=[jax.ShapeDtypeStruct(r.shape, r.dtype) for r in res[:2]],
            in_specs=[vmem] * 2,
            out_specs=[any_] * 2,
            scratch_shapes=[dma(2)],
            compiler_params=pltpu.CompilerParams(vmem_limit_bytes=16 << 20),
            name="put",
        )(res[0], res[1])

    return jax.shard_map(local_step, mesh=mesh, in_specs=(spec_act, spec_w, spec_act), out_specs=(spec_act, spec_act), check_vma=False)
```

```python
import functools

import jax
import jax.numpy as jnp
from jax import lax
from jax.experimental import pallas as pl
from jax.experimental.pallas import tpu as pltpu
from jax.sharding import PartitionSpec as P

MESH = pl.DeviceIdType.MESH
BF16, F32 = jnp.bfloat16, jnp.float32
NC = 8
NH = NC // 2


def kernel(x, w, g, dx, dw, pp, qq, xa, wa, rx, ry, vx,
           xs, xr, told, inside, ready):
    h, y, c = lax.axis_index("ro"), lax.axis_index("ri"), lax.axis_index("co")
    o = 1 - h
    tb, dcols = x.shape
    wrows, f = w.shape
    q = wrows // 2
    cr, qr = tb // NC, q // NC
    ft = f // 7
    yn = [lax.rem(y + 1, 4), lax.rem(y + 3, 4)]
    cn = [lax.rem(c + 1, 4), lax.rem(c + 3, 4)]
    y2, c2 = lax.rem(y + 2, 4), lax.rem(c + 2, 4)
    sib = {"ro": o}

    def rc(src, dst, ssem, rsem, dev):
        return pltpu.make_async_remote_copy(src_ref=src, dst_ref=dst, send_sem=ssem, recv_sem=rsem, device_id=dev, device_id_type=MESH)

    def lc(src, dst, sem):
        return pltpu.make_async_copy(src, dst, sem)

    def done(ref, sem):
        lc(ref, ref, sem).wait()

    def xor(a, b):
        return 2 * lax.rem(a // 2 + b // 2, 2) + lax.rem(lax.rem(a, 2) + lax.rem(b, 2), 2)

    def xcols(i, k):
        return x.at[:, pl.ds(pl.multiple_of(i * 2 * q + k * q, q), q)]

    def wrow(k):
        return w.at[pl.ds(pl.multiple_of(k * q, q), q)]

    bar = pltpu.get_barrier_semaphore()
    for e in range(2):
        pl.semaphore_signal(bar, 1, device_id={"co": cn[e]}, device_id_type=MESH)
    for e in range(2):
        pl.semaphore_signal(bar, 1, device_id={"ri": yn[e], "ro": 0}, device_id_type=MESH)

    @pl.when(h == 1)
    def _():
        pl.semaphore_signal(bar, 1, device_id=sib, device_id_type=MESH)
        pl.semaphore_wait(bar, 2)

    @pl.when(h == 0)
    def _():
        pl.semaphore_wait(bar, 7)
        pl.semaphore_signal(told, 1, device_id=sib, device_id_type=MESH)

    def x_send(e, k, i):
        return rc(xcols(i, k), xa.at[c, h, i], xs.at[0], xr.at[c, h, i], {"co": cn[e], "ro": k})

    for n in range(2):
        for e in range(2):
            x_send(e, h, n if e == 0 else 1 - n).start()

    pl.semaphore_wait(told, 1)

    @pl.when(h == 1)
    def _():
        pl.semaphore_signal(told, 1, device_id=sib, device_id_type=MESH)

    for n in range(2):
        for e in range(2):
            x_send(e, o, n if e == 0 else 1 - n).start()

    def rest(wr, dr, opp_r, pure_r, xacc_r, yacc_r, fin_r, ss, ring_s, fin, ls, outs, ads):
        senders = [sib] + [{"ri": yn[e], "ro": k} for e in range(2) for k in range(2)] + [{"co": cn[e]} for e in range(2)]
        for dev in senders:
            pl.semaphore_signal(inside, 1, device_id=dev, device_id_type=MESH)
        w_dir = [rc(wrow(k), wa.at[y, h], ss.at[0], wr.at[y, h], {"ri": yn[e], "ro": k}) for n in range(2) for e in range(2) for k in [h if n == e else o]]
        w_d2d = rc(wrow(o), wa.at[y, h], ss.at[2], wr.at[y, h], sib)
        x_d2d = [rc(xcols(i, o), xa.at[c, h, i], ss.at[1], xr.at[c, h, i], sib) for i in range(2)]
        for cp in x_d2d:
            cp.start()
        pl.semaphore_wait(inside, len(senders))
        for cp in w_dir + [w_d2d]:
            cp.start()

        w_fwd = [rc(wa.at[yn[1 - e], k], wa.at[yn[1 - e], k], ss.at[0], wr.at[yn[1 - e], k], {"ri": yn[e]}) for e, k in ((0, h), (1, o))]
        x_fwd = [rc(xa.at[cn[1 - e], t, e], xa.at[cn[1 - e], t, e], xs.at[0], xr.at[cn[1 - e], t, e], {"co": cn[e]}) for e in range(2) for t in range(2)]

        def got_w(yy, k):
            done(wa.at[yy, k], wr.at[yy, k])

        def got_x(cc, i):
            for t in range(2):
                done(xa.at[cc, t, i], xr.at[cc, t, i])

        def sends(a, part, recv, me, axis, nbr, d):
            k = lax.rem(d - me + 4, 4)

            @pl.when(k == 2)
            def _():
                for n in range(2):
                    for e in range(2):
                        half = pl.ds(n * NH, NH)
                        rc(part.at[d, e, half], recv.at[0, e, half], ring_s.at[a], opp_r.at[a, e, n], {axis: nbr[e]}).start()

            for e in range(2):
                @pl.when(k == 1 + 2 * e)
                def _():
                    rc(part.at[d, 1 - e], recv.at[1, e], ring_s.at[a], pure_r.at[a, e], {axis: nbr[e]}).start()

        x_sends = functools.partial(sends, 0, pp, rx, c, "co", cn)
        y_sends = functools.partial(sends, 1, qq, ry, y, "ri", yn)

        def compute(gv, wv, xin, xt, pst, qst):
            pl.semaphore_signal(ready, 1, device_id=sib, device_id_type=MESH)
            lc(g, gv.at[h], ls.at[0]).start()
            pl.semaphore_wait(ready, 1)
            rc(g, gv.at[h], ss.at[3], dr.at[0], sib).start()
            for i in range(2):
                lc(xcols(i, h), xin.at[0, i], ls.at[3]).start()

            def p_out(slot, r, yy, m):
                s, ab, hf = 1 - m // 4, lax.rem(m // 2, 2), lax.rem(m, 2)
                return lc(pst.at[slot, r], pp.at[2 * r + yy // 2, ab, pl.ds(s * 4 + hf * 2, 2), :, pl.ds(pl.multiple_of(lax.rem(yy, 2) * q, q), q)], outs.at[slot])

            def load_w(yy, r):
                lc(wa.at[yy, r], wv.at[pl.ds(pl.multiple_of(r * q, q), q)], ls.at[1]).start()

            def p_step(yy):
                done(wv, ls.at[1])

                @pl.loop(0, 8)
                def _(m):
                    s, ab, hf = 1 - m // 4, lax.rem(m // 2, 2), lax.rem(m, 2)
                    t = s * h + (1 - s) * o
                    row = pl.multiple_of(ab * (tb // 2) + hf * (tb // 4), tb // 4)
                    slot = lax.rem(m, 2)

                    @pl.when(m >= 2)
                    def _():
                        done(pst.at[slot], outs.at[slot])

                    res = lax.dot_general(gv[t, pl.ds(row, tb // 4), :], wv[...], (((1,), (1,)), ((), ())), preferred_element_type=F32)
                    for r in range(2):
                        pst[slot, r] = res[:, r * q:(r + 1) * q].reshape(2, cr, q)
                    for r in range(2):
                        p_out(slot, r, yy, m).start()

                for slot in range(2):
                    done(pst.at[slot], outs.at[slot])

            def q_out(slot, r, yy, n):
                s = r * h + (1 - r) * o
                return lc(qst.at[slot, r], qq.at[yy, :, pl.ds(s * 4, 4), :, pl.ds(pl.multiple_of(n * ft, ft), ft)], outs.at[slot])

            def load_x(yy):
                for r in range(2):
                    for t in range(2):
                        lc(xa.at[2 * r + yy // 2, t, lax.rem(yy, 2)], xin.at[r, t], ls.at[4]).start()

            def q_step(yy, yy_next, qn):
                @pl.when(qn < 2)
                def _():
                    load_x(yy)

                done(xin, ls.at[4])

                @pl.loop(0, NC)
                def _(n):
                    at = pl.ds(pl.multiple_of(n * cr, cr), cr)
                    for r in range(2):
                        for t in range(2):
                            xt[t, r * q:(r + 1) * q, at] = xin[r, t, at, :].T

                @pl.when((qn == 1) | (qn == 2))
                def _():
                    load_x(yy_next)

                @pl.loop(0, 7)
                def _(n):
                    slot = lax.rem(n, 2)

                    @pl.when(n >= 2)
                    def _():
                        done(qst.at[slot], outs.at[slot])

                    at = pl.ds(pl.multiple_of(n * ft, ft), ft)
                    res = jnp.dot(xt[0], gv[0, :, at], preferred_element_type=F32)
                    res += jnp.dot(xt[1], gv[1, :, at], preferred_element_type=F32)
                    for r in range(2):
                        qst[slot, r] = res[r * q:(r + 1) * q].reshape(2, 4, qr, ft)
                    for r in range(2):
                        q_out(slot, r, yy, n).start()

                for slot in range(2):
                    done(qst.at[slot], outs.at[slot])

            op = lax.rem(y // 2 + c + 1, 2)

            def qcode(n):
                return op * ((1 - n // 2) * (2 + n) + n // 2 * (3 - n)) + (1 - op) * lax.rem(n + 1, 4)

            even = 1 - lax.rem(y, 2)
            rem1 = even * h + (1 - even) * o

            @pl.loop(0, 8)
            def _(step):
                @pl.when(step == 0)
                def _():
                    lc(wrow(h), wv.at[pl.ds(pl.multiple_of(h * q, q), q)], ls.at[1]).start()
                    got_w(y, o)
                    load_w(y, o)
                    done(gv.at[o], dr.at[0])
                    done(gv.at[h], ls.at[0])

                @pl.when(step == 1)
                def _():
                    done(xin.at[0], ls.at[3])
                    for i in range(2):
                        lc(xin.at[0, i], xa.at[c, h, i], ls.at[3]).start()
                    got_w(yn[1], h)
                    w_fwd[0].start()
                    got_w(yn[0], o)
                    w_fwd[1].start()
                    got_x(cn[1], 0)
                    x_fwd[0].start()
                    x_fwd[1].start()
                    got_x(cn[0], 1)
                    x_fwd[2].start()
                    x_fwd[3].start()
                    load_w(xor(y, 1), 1 - rem1)
                    got_w(xor(y, 1), rem1)
                    load_w(xor(y, 1), rem1)

                @pl.when(step == 2)
                def _():
                    x_sends(y // 2)
                    x_sends(2 + y // 2)
                    got_x(cn[1], 1)
                    got_x(cn[0], 0)
                    done(xin.at[0], ls.at[3])

                @pl.when(step == 3)
                def _():
                    for i in range(2):
                        done(xa.at[c, o, i], xr.at[c, o, i])
                    got_x(c2, 0)
                    got_x(c2, 1)
                    got_w(3 - y, 1 - rem1)
                    for r in range(2):
                        load_w(3 - y, r)
                        got_w(y2, r)

                @pl.when(step == 6)
                def _():
                    for r in range(2):
                        load_w(y2, r)

                late = step // 5
                is_p = (step < 2) | ((step >= 5) & (step < 7))
                pn = step - 3 * late
                qn = step - 2 - 2 * (step // 7)
                pcode = pn + pn // 2 - 2 * (pn // 3)
                @pl.when(is_p)
                def _():
                    p_step(xor(y, pcode))

                @pl.when(jnp.logical_not(is_p))
                def _():
                    yy = xor(y, qcode(qn))
                    q_step(yy, xor(y, qcode(lax.rem(qn + 1, 4))), qn)
                    y_sends(yy)

                @pl.when(step == 6)
                def _():
                    x_sends(1 - y // 2)
                    x_sends(3 - y // 2)

        pl.run_scoped(compute, pltpu.VMEM((2, tb, f), BF16), pltpu.VMEM((2 * q, f), BF16), pltpu.VMEM((2, 2, tb, q), BF16), pltpu.VMEM((2, 2 * q, tb), BF16),
                      pltpu.VMEM((2, 2, 2, cr, q), F32), pltpu.VMEM((2, 2, 2, 4, qr, ft), F32))

        def reduce(accx, tmpx, nxtx, ownx, sibx, outx, accy, tmpy, nxty, siby):
            rings = ((0, pp, rx, c, cn, "co", accx, tmpx, nxtx), (1, qq, ry, y, yn, "ri", accy, tmpy, nxty))
            low, high = pl.ds(0, NH), pl.ds(NH, NH)

            def x_at(e, j, i):
                return (pl.ds(pl.multiple_of(e * (tb // 2) + j * cr, cr), cr), pl.ds(pl.multiple_of(i * 2 * q + h * q, q), q))

            def y_at(e, j):
                return pl.ds(pl.multiple_of(h * q + e * (q // 2) + j * qr, qr), qr)

            for a, part, recv, me, nbr, axis, acc, tmp, nxt in rings:
                for e in range(2):
                    lc(part.at[nbr[e], e], acc.at[e], ls.at[a]).start()
            for e in range(2):
                lc(pp.at[c, e, low], sibx.at[e], ls.at[2]).start()
                lc(pp.at[c, e, high], ownx.at[e], ls.at[2]).start()
                lc(qq.at[y, e, low], siby.at[e], ls.at[3]).start()
                for j in range(NH):
                    lc(qq.at[y, e, NH + j], dw.at[y_at(e, j)], ls.at[3]).start()

            @pl.loop(0, 2)
            def _(n):
                half = pl.ds(n * NH, NH)
                for a, part, recv, me, nbr, axis, acc, tmp, nxt in rings:
                    for e in range(2):
                        done(recv.at[0, e, low], opp_r.at[a, e, n])
                        lc(recv.at[0, e, half], tmp.at[e], ads.at[a]).start()

                @pl.when(n == 0)
                def _():
                    done(accx, ls.at[0])
                    done(accy, ls.at[1])

                for a, part, recv, me, nbr, axis, acc, tmp, nxt in rings:
                    done(tmp, ads.at[a])

                    @pl.loop(0, NH)
                    def _(i):
                        for e in range(2):
                            acc[e, n * NH + i] += tmp[e, i]

                @pl.when(n == 0)
                def _():
                    for e in range(2):
                        rc(accx.at[e, low], rx.at[2, e, low], ring_s.at[0], xacc_r.at[e, 0], {"co": cn[e]}).start()

                @pl.when(n == 1)
                def _():
                    for i in range(NH):
                        for e in range(2):
                            rc(accx.at[e, NH + i], vx.at[e, i], ring_s.at[0], xacc_r.at[e, 1 + i], {"co": cn[e]}).start()

                for e in range(2):
                    rc(accy.at[e, half], ry.at[2, e, half], ring_s.at[1], yacc_r.at[e, n], {"ri": yn[e]}).start()

            for a, part, recv, me, nbr, axis, acc, tmp, nxt in rings:
                for e in range(2):
                    done(recv.at[1, e], pure_r.at[a, e])
                for e in range(2):
                    lc(recv.at[1, 1 - e, low], tmp.at[e], ads.at[a]).start()
                    lc(recv.at[1, 1 - e, high], nxt.at[e], ads.at[a]).start()
            done(wa.at[pl.ds(0, 3)], ss.at[0])
            done(xa.at[pl.ds(0, 3)], xs.at[0])
            done(wa.at[0, 0], ss.at[2])
            done(g, ss.at[3])
            done(xa.at[0, 0], ss.at[1])
            done(accx, ls.at[2])
            done(accy, ls.at[3])

            for e in range(2):
                done(ry.at[2, e, low], yacc_r.at[e, 0])
            done(accy, ads.at[1])

            @pl.loop(0, NH)
            def _(i):
                for e in range(2):
                    siby[e, i] += tmpy[e, i]
                    dw[y_at(e, i)] += nxty[e, i]

            for e in range(2):
                lc(ry.at[2, e, low], tmpy.at[e], ads.at[1]).start()
            done(accx, ads.at[0])

            @pl.loop(0, NH)
            def _(i):
                for e in range(2):
                    sibx[e, i] += tmpx[e, i]
                    ownx[e, i] += nxtx[e, i]

            done(tmpy, ads.at[1])

            @pl.loop(0, NH)
            def _(i):
                for e in range(2):
                    siby[e, i] += tmpy[e, i]

            for e in range(2):
                for i in range(NH):
                    rc(siby.at[e, i], dw.at[y_at(e, i)], fin.at[1], fin_r.at[1], sib).start()

            for e in range(2):
                done(rx.at[2, e, low], xacc_r.at[e, 0])
                lc(rx.at[2, e, low], tmpx.at[e], ads.at[0]).start()
            done(tmpx, ads.at[0])

            @pl.loop(0, NH)
            def _(j):
                for e in range(2):
                    outx[e, j] = (sibx[e, j] + tmpx[e, j]).astype(BF16)

            @pl.loop(0, NH)
            def _(j):
                for e in range(2):
                    for i in range(2):
                        rc(outx.at[e, j, :, i * q:(i + 1) * q], dx.at[x_at(e, j, i)], fin.at[0], fin_r.at[0], sib).start()

            for e in range(2):
                done(ry.at[2, e, low], yacc_r.at[e, 1])
                lc(ry.at[2, e, high], tmpy.at[e], ads.at[1]).start()
            done(tmpy, ads.at[1])

            @pl.loop(0, NH)
            def _(j):
                for e in range(2):
                    dw[y_at(e, j)] += tmpy[e, j]

            for n, ref in enumerate((outx, siby)):
                done(ref, fin.at[n])
                done(ref, fin_r.at[n])
            done(ry, ring_s.at[1])

            @pl.loop(0, NH)
            def _(j):
                for e in range(2):
                    done(vx.at[e, j], xacc_r.at[e, 1 + j])
                    tot = ownx[e, j] + vx[e, j]
                    for i in range(2):
                        dx[x_at(e, j, i)] = tot[:, i * q:(i + 1) * q].astype(BF16)

            done(rx, ring_s.at[0])

        x_half, y_half = (2, NH, cr, 2 * q), (2, NH, qr, f)
        pl.run_scoped(reduce, pltpu.VMEM((2, NC, cr, 2 * q), F32), *[pltpu.VMEM(x_half, F32)] * 4, pltpu.VMEM(x_half, BF16),
                      pltpu.VMEM((2, NC, qr, f), F32), *[pltpu.VMEM(y_half, F32)] * 3)

    dma = pltpu.SemaphoreType.DMA
    pl.run_scoped(rest, dma((4, 2)), dma((1,)), dma((2, 2, 2)), dma((2, 2)), dma((2, 1 + NH)), dma((2, 2)), dma((2,)), dma((4,)), dma((2,)), dma((2,)), dma((5,)), dma((2,)), dma((2,)))


def put_kernel(a, b, u, v, sems):
    for i, (src, dst) in enumerate(((b, v), (a, u))):
        rows = src.shape[0] // 8
        for n in range(8):
            pltpu.make_async_copy(src.at[pl.ds(n * rows, rows)], dst.at[pl.ds(n * rows, rows)], sems.at[i]).start()
    for i, (src, dst) in enumerate(((b, v), (a, u))):
        pltpu.make_async_copy(src, dst, sems.at[i]).wait()


def solution(mesh):
    spec_act = P(("dp", "ro", "ri"), "co")
    spec_w = P(("ro", "ri"), "co")

    def local_step(x, w, g):
        tb, dcols = x.shape
        wrows, f = w.shape
        q = wrows // 2
        cr, qr = tb // NC, q // NC
        dma = lambda *s: pltpu.SemaphoreType.DMA(s)
        any_ = pl.BlockSpec(memory_space=pl.ANY)
        vmem = pl.BlockSpec(memory_space=pltpu.VMEM)
        shapes = [
            pltpu.VMEM((tb, dcols), BF16),
            pltpu.VMEM((wrows, f), F32),
            jax.ShapeDtypeStruct((4, 2, NC, cr, 2 * q), F32),
            jax.ShapeDtypeStruct((4, 2, NC, qr, f), F32),
            jax.ShapeDtypeStruct((4, 2, 2, tb, q), BF16),
            jax.ShapeDtypeStruct((4, 2, q, f), BF16),
            jax.ShapeDtypeStruct((3, 2, NC, cr, 2 * q), F32),
            jax.ShapeDtypeStruct((3, 2, NC, qr, f), F32),
        ]
        res = pl.pallas_call(
            kernel,
            out_shape=shapes,
            in_specs=[any_] * 3,
            out_specs=[vmem] * 2 + [any_] * (len(shapes) - 2),
            scratch_shapes=[
                pltpu.VMEM((2, NH, cr, 2 * q), F32),
                dma(1), dma(4, 2, 2), pltpu.SemaphoreType.REGULAR, pltpu.SemaphoreType.REGULAR, pltpu.SemaphoreType.REGULAR,
            ],
            compiler_params=pltpu.CompilerParams(collective_id=0, has_side_effects=True, vmem_limit_bytes=52 << 20),
            name="linear_grads",
        )(x, w, g)
        return pl.pallas_call(
            put_kernel,
            out_shape=[jax.ShapeDtypeStruct(r.shape, r.dtype) for r in res[:2]],
            in_specs=[vmem] * 2,
            out_specs=[any_] * 2,
            scratch_shapes=[dma(2)],
            compiler_params=pltpu.CompilerParams(vmem_limit_bytes=16 << 20),
            name="put",
        )(res[0], res[1])

    return jax.shard_map(local_step, mesh=mesh, in_specs=(spec_act, spec_w, spec_act), out_specs=(spec_act, spec_act), check_vma=False)
```

```python
import functools

import jax
import jax.numpy as jnp
from jax import lax
from jax.experimental import pallas as pl
from jax.experimental.pallas import tpu as pltpu
from jax.sharding import PartitionSpec as P

MESH = pl.DeviceIdType.MESH
BF16, F32 = jnp.bfloat16, jnp.float32
NC = 8
NH = NC // 2


def kernel(x, w, g, dx, dw, pp, qq, xa, wa, rx, ry, vx,
           xs, xr, told, inside, ready):
    h, y, c = lax.axis_index("ro"), lax.axis_index("ri"), lax.axis_index("co")
    o = 1 - h
    tb, dcols = x.shape
    wrows, f = w.shape
    q = wrows // 2
    cr, qr = tb // NC, q // NC
    ft = f // 7
    yn = [lax.rem(y + 1, 4), lax.rem(y + 3, 4)]
    cn = [lax.rem(c + 1, 4), lax.rem(c + 3, 4)]
    y2, c2 = lax.rem(y + 2, 4), lax.rem(c + 2, 4)
    sib = {"ro": o}

    def rc(src, dst, ssem, rsem, dev):
        return pltpu.make_async_remote_copy(src_ref=src, dst_ref=dst, send_sem=ssem, recv_sem=rsem, device_id=dev, device_id_type=MESH)

    def lc(src, dst, sem):
        return pltpu.make_async_copy(src, dst, sem)

    def done(ref, sem):
        lc(ref, ref, sem).wait()

    def xor(a, b):
        return 2 * lax.rem(a // 2 + b // 2, 2) + lax.rem(lax.rem(a, 2) + lax.rem(b, 2), 2)

    def xcols(i, k):
        return x.at[:, pl.ds(pl.multiple_of(i * 2 * q + k * q, q), q)]

    def wrow(k):
        return w.at[pl.ds(pl.multiple_of(k * q, q), q)]

    bar = pltpu.get_barrier_semaphore()
    for e in range(2):
        pl.semaphore_signal(bar, 1, device_id={"co": cn[e]}, device_id_type=MESH)
    for e in range(2):
        pl.semaphore_signal(bar, 1, device_id={"ri": yn[e], "ro": 0}, device_id_type=MESH)

    @pl.when(h == 1)
    def _():
        pl.semaphore_signal(bar, 1, device_id=sib, device_id_type=MESH)
        pl.semaphore_wait(bar, 2)

    @pl.when(h == 0)
    def _():
        pl.semaphore_wait(bar, 7)
        pl.semaphore_signal(told, 1, device_id=sib, device_id_type=MESH)

    def x_send(e, k, i):
        return rc(xcols(i, k), xa.at[c, h, i], xs.at[0], xr.at[e, h, i], {"co": cn[e], "ro": k})

    for n in range(2):
        for e in range(2):
            x_send(e, h, n if e == 0 else 1 - n).start()

    pl.semaphore_wait(told, 1)

    @pl.when(h == 1)
    def _():
        pl.semaphore_signal(told, 1, device_id=sib, device_id_type=MESH)

    for n in range(2):
        for e in range(2):
            x_send(e, o, n if e == 0 else 1 - n).start()

    def rest(xf, xd, wr, dr, opp_r, pure_r, xacc_r, yacc_r, fin_r, ss, ring_s, fin, ls, outs, ads):
        senders = [sib] + [{"ri": yn[e], "ro": k} for e in range(2) for k in range(2)] + [{"co": cn[e]} for e in range(2)]
        for dev in senders:
            pl.semaphore_signal(inside, 1, device_id=dev, device_id_type=MESH)
        w_dir = [rc(wrow(k), wa.at[y, h], ss.at[0], wr.at[y, h], {"ri": yn[e], "ro": k}) for n in range(2) for e in range(2) for k in [h if n == e else o]]
        w_d2d = rc(wrow(o), wa.at[y, h], ss.at[2], wr.at[y, h], sib)
        x_d2d = [rc(xcols(i, o), xa.at[c, h, i], ss.at[1], xd.at[0], sib) for i in range(2)]
        pl.semaphore_wait(inside, len(senders))
        for cp in w_dir + [w_d2d] + x_d2d:
            cp.start()

        w_fwd = [rc(wa.at[yn[1 - e], k], wa.at[yn[1 - e], k], ss.at[0], wr.at[yn[1 - e], k], {"ri": yn[e]}) for e, k in ((0, h), (1, o))]
        x_fwd = [rc(xa.at[cn[1 - e], t, e], xa.at[cn[1 - e], t, e], xs.at[0], xf.at[t, e], {"co": cn[e]}) for e in range(2) for t in range(2)]

        def got_w(yy, k):
            done(wa.at[yy, k], wr.at[yy, k])

        def got_x(e, i):
            for t in range(2):
                done(xa.at[cn[1 - e], t, i], xr.at[e, t, i])

        def sends(a, part, recv, me, axis, nbr, d):
            k = lax.rem(d - me + 4, 4)

            @pl.when(k == 2)
            def _():
                for n in range(2):
                    for e in range(2):
                        half = pl.ds(n * NH, NH)
                        rc(part.at[d, e, half], recv.at[0, e, half], ring_s.at[a], opp_r.at[a, e, n], {axis: nbr[e]}).start()

            for e in range(2):
                @pl.when(k == 1 + 2 * e)
                def _():
                    rc(part.at[d, 1 - e], recv.at[1, e], ring_s.at[a], pure_r.at[a, e], {axis: nbr[e]}).start()

        x_sends = functools.partial(sends, 0, pp, rx, c, "co", cn)
        y_sends = functools.partial(sends, 1, qq, ry, y, "ri", yn)

        def compute(gv, wv, xin, xt, pst, qst):
            pl.semaphore_signal(ready, 1, device_id=sib, device_id_type=MESH)
            lc(g, gv.at[h], ls.at[0]).start()
            pl.semaphore_wait(ready, 1)
            rc(g, gv.at[h], ss.at[3], dr.at[0], sib).start()
            for i in range(2):
                lc(xcols(i, h), xin.at[0, i], ls.at[3]).start()

            def p_out(slot, r, yy, m):
                s, ab, hf = 1 - m // 4, lax.rem(m // 2, 2), lax.rem(m, 2)
                return lc(pst.at[slot, r], pp.at[2 * r + yy // 2, ab, pl.ds(s * 4 + hf * 2, 2), :, pl.ds(pl.multiple_of(lax.rem(yy, 2) * q, q), q)], outs.at[slot])

            def load_w(yy, r):
                lc(wa.at[yy, r], wv.at[pl.ds(pl.multiple_of(r * q, q), q)], ls.at[1]).start()

            def p_step(yy):
                done(wv, ls.at[1])

                @pl.loop(0, 8)
                def _(m):
                    s, ab, hf = 1 - m // 4, lax.rem(m // 2, 2), lax.rem(m, 2)
                    t = s * h + (1 - s) * o
                    row = pl.multiple_of(ab * (tb // 2) + hf * (tb // 4), tb // 4)
                    slot = lax.rem(m, 2)

                    @pl.when(m >= 2)
                    def _():
                        done(pst.at[slot], outs.at[slot])

                    res = lax.dot_general(gv[t, pl.ds(row, tb // 4), :], wv[...], (((1,), (1,)), ((), ())), preferred_element_type=F32)
                    for r in range(2):
                        pst[slot, r] = res[:, r * q:(r + 1) * q].reshape(2, cr, q)
                    for r in range(2):
                        p_out(slot, r, yy, m).start()

                for slot in range(2):
                    done(pst.at[slot], outs.at[slot])

            def q_out(slot, r, yy, n):
                s = r * h + (1 - r) * o
                return lc(qst.at[slot, r], qq.at[yy, :, pl.ds(s * 4, 4), :, pl.ds(pl.multiple_of(n * ft, ft), ft)], outs.at[slot])

            def load_x(yy):
                for r in range(2):
                    for t in range(2):
                        lc(xa.at[2 * r + yy // 2, t, lax.rem(yy, 2)], xin.at[r, t], ls.at[4]).start()

            def q_step(yy, yy_next, qn):
                @pl.when(qn < 2)
                def _():
                    load_x(yy)

                done(xin, ls.at[4])

                @pl.loop(0, NC)
                def _(n):
                    at = pl.ds(pl.multiple_of(n * cr, cr), cr)
                    for r in range(2):
                        for t in range(2):
                            xt[t, r * q:(r + 1) * q, at] = xin[r, t, at, :].T

                @pl.when((qn == 1) | (qn == 2))
                def _():
                    load_x(yy_next)

                @pl.loop(0, 7)
                def _(n):
                    slot = lax.rem(n, 2)

                    @pl.when(n >= 2)
                    def _():
                        done(qst.at[slot], outs.at[slot])

                    at = pl.ds(pl.multiple_of(n * ft, ft), ft)
                    res = jnp.dot(xt[0], gv[0, :, at], preferred_element_type=F32)
                    res += jnp.dot(xt[1], gv[1, :, at], preferred_element_type=F32)
                    for r in range(2):
                        qst[slot, r] = res[r * q:(r + 1) * q].reshape(2, 4, qr, ft)
                    for r in range(2):
                        q_out(slot, r, yy, n).start()

                for slot in range(2):
                    done(qst.at[slot], outs.at[slot])

            op = lax.rem(y // 2 + c + 1, 2)

            def qcode(n):
                return op * ((1 - n // 2) * (2 + n) + n // 2 * (3 - n)) + (1 - op) * lax.rem(n + 1, 4)

            even = 1 - lax.rem(y, 2)
            rem1 = even * h + (1 - even) * o

            @pl.loop(0, 8)
            def _(step):
                @pl.when(step == 0)
                def _():
                    lc(wrow(h), wv.at[pl.ds(pl.multiple_of(h * q, q), q)], ls.at[1]).start()
                    got_w(y, o)
                    load_w(y, o)
                    done(gv.at[o], dr.at[0])
                    done(gv.at[h], ls.at[0])

                @pl.when(step == 1)
                def _():
                    done(xin.at[0], ls.at[3])
                    for i in range(2):
                        lc(xin.at[0, i], xa.at[c, h, i], ls.at[3]).start()
                    got_w(yn[1], h)
                    w_fwd[0].start()
                    got_w(yn[0], o)
                    w_fwd[1].start()
                    got_x(0, 0)
                    x_fwd[0].start()
                    x_fwd[1].start()
                    got_x(1, 1)
                    x_fwd[2].start()
                    x_fwd[3].start()
                    load_w(xor(y, 1), 1 - rem1)
                    got_w(xor(y, 1), rem1)
                    load_w(xor(y, 1), rem1)

                @pl.when(step == 2)
                def _():
                    x_sends(y // 2)
                    x_sends(2 + y // 2)
                    got_x(0, 1)
                    got_x(1, 0)
                    done(xin.at[0], ls.at[3])

                @pl.when(step == 3)
                def _():
                    done(xa.at[c, o], xd.at[0])
                    for t in range(2):
                        for i in range(2):
                            done(xa.at[c2, t, i], xf.at[t, i])
                    got_w(3 - y, 1 - rem1)
                    for r in range(2):
                        load_w(3 - y, r)
                        got_w(y2, r)

                @pl.when(step == 6)
                def _():
                    for r in range(2):
                        load_w(y2, r)

                late = step // 5
                is_p = (step < 2) | ((step >= 5) & (step < 7))
                pn = step - 3 * late
                qn = step - 2 - 2 * (step // 7)
                pcode = pn + pn // 2 - 2 * (pn // 3)
                @pl.when(is_p)
                def _():
                    p_step(xor(y, pcode))

                @pl.when(jnp.logical_not(is_p))
                def _():
                    yy = xor(y, qcode(qn))
                    q_step(yy, xor(y, qcode(lax.rem(qn + 1, 4))), qn)
                    y_sends(yy)

                @pl.when(step == 6)
                def _():
                    x_sends(1 - y // 2)
                    x_sends(3 - y // 2)

        pl.run_scoped(compute, pltpu.VMEM((2, tb, f), BF16), pltpu.VMEM((2 * q, f), BF16), pltpu.VMEM((2, 2, tb, q), BF16), pltpu.VMEM((2, 2 * q, tb), BF16),
                      pltpu.VMEM((2, 2, 2, cr, q), F32), pltpu.VMEM((2, 2, 2, 4, qr, ft), F32))

        def reduce(accx, tmpx, nxtx, ownx, sibx, outx, accy, tmpy, nxty, siby):
            rings = ((0, pp, rx, c, cn, "co", accx, tmpx, nxtx), (1, qq, ry, y, yn, "ri", accy, tmpy, nxty))
            low, high = pl.ds(0, NH), pl.ds(NH, NH)

            def x_at(e, j, i):
                return (pl.ds(pl.multiple_of(e * (tb // 2) + j * cr, cr), cr), pl.ds(pl.multiple_of(i * 2 * q + h * q, q), q))

            def y_at(e, j):
                return pl.ds(pl.multiple_of(h * q + e * (q // 2) + j * qr, qr), qr)

            for a, part, recv, me, nbr, axis, acc, tmp, nxt in rings:
                for e in range(2):
                    lc(part.at[nbr[e], e], acc.at[e], ls.at[a]).start()
            for e in range(2):
                lc(pp.at[c, e, low], sibx.at[e], ls.at[2]).start()
                lc(pp.at[c, e, high], ownx.at[e], ls.at[2]).start()
                lc(qq.at[y, e, low], siby.at[e], ls.at[3]).start()
                for j in range(NH):
                    lc(qq.at[y, e, NH + j], dw.at[y_at(e, j)], ls.at[3]).start()

            @pl.loop(0, 2)
            def _(n):
                half = pl.ds(n * NH, NH)
                for a, part, recv, me, nbr, axis, acc, tmp, nxt in rings[::-1]:
                    for e in range(2):
                        done(recv.at[0, e, low], opp_r.at[a, e, n])
                        lc(recv.at[0, e, half], tmp.at[e], ads.at[a]).start()

                @pl.when(n == 0)
                def _():
                    done(accx, ls.at[0])
                    done(accy, ls.at[1])

                for a, part, recv, me, nbr, axis, acc, tmp, nxt in rings:
                    done(tmp, ads.at[a])

                    @pl.loop(0, NH)
                    def _(i):
                        for e in range(2):
                            acc[e, n * NH + i] += tmp[e, i]

                @pl.when(n == 0)
                def _():
                    for e in range(2):
                        rc(accx.at[e, low], rx.at[2, e, low], ring_s.at[0], xacc_r.at[e, 0], {"co": cn[e]}).start()

                @pl.when(n == 1)
                def _():
                    for i in range(NH):
                        for e in range(2):
                            rc(accx.at[e, NH + i], vx.at[e, i], ring_s.at[0], xacc_r.at[e, 1 + i], {"co": cn[e]}).start()

                for e in range(2):
                    rc(accy.at[e, half], ry.at[2, e, half], ring_s.at[1], yacc_r.at[e, n], {"ri": yn[e]}).start()

            for a, part, recv, me, nbr, axis, acc, tmp, nxt in rings[::-1]:
                for e in range(2):
                    done(recv.at[1, e], pure_r.at[a, e])
                for e in range(2):
                    lc(recv.at[1, 1 - e, low], tmp.at[e], ads.at[a]).start()
                    lc(recv.at[1, 1 - e, high], nxt.at[e], ads.at[a]).start()
            done(wa.at[pl.ds(0, 3)], ss.at[0])
            done(xa.at[pl.ds(0, 3)], xs.at[0])
            done(wa.at[0, 0], ss.at[2])
            done(g, ss.at[3])
            done(xa.at[0, 0], ss.at[1])
            done(accx, ls.at[2])
            done(accy, ls.at[3])

            for e in range(2):
                done(ry.at[2, e, low], yacc_r.at[e, 0])
            done(accy, ads.at[1])

            @pl.loop(0, NH)
            def _(i):
                for e in range(2):
                    siby[e, i] += tmpy[e, i]
                    dw[y_at(e, i)] += nxty[e, i]

            for e in range(2):
                lc(ry.at[2, e, low], tmpy.at[e], ads.at[1]).start()
            done(accx, ads.at[0])

            @pl.loop(0, NH)
            def _(i):
                for e in range(2):
                    sibx[e, i] += tmpx[e, i]
                    ownx[e, i] += nxtx[e, i]

            done(tmpy, ads.at[1])

            @pl.loop(0, NH)
            def _(i):
                for e in range(2):
                    siby[e, i] += tmpy[e, i]

            for e in range(2):
                for i in range(NH):
                    rc(siby.at[e, i], dw.at[y_at(e, i)], fin.at[1], fin_r.at[1], sib).start()

            for e in range(2):
                done(rx.at[2, e, low], xacc_r.at[e, 0])
                lc(rx.at[2, e, low], tmpx.at[e], ads.at[0]).start()
            done(tmpx, ads.at[0])

            @pl.loop(0, NH)
            def _(j):
                for e in range(2):
                    outx[e, j] = (sibx[e, j] + tmpx[e, j]).astype(BF16)

            @pl.loop(0, NH)
            def _(j):
                for e in range(2):
                    for i in range(2):
                        rc(outx.at[e, j, :, i * q:(i + 1) * q], dx.at[x_at(e, j, i)], fin.at[0], fin_r.at[0], sib).start()

            for e in range(2):
                done(ry.at[2, e, low], yacc_r.at[e, 1])
                lc(ry.at[2, e, high], tmpy.at[e], ads.at[1]).start()
            done(tmpy, ads.at[1])

            @pl.loop(0, NH)
            def _(j):
                for e in range(2):
                    dw[y_at(e, j)] += tmpy[e, j]

            for n, ref in enumerate((outx, siby)):
                done(ref, fin.at[n])
                done(ref, fin_r.at[n])
            done(ry, ring_s.at[1])

            @pl.loop(0, NH)
            def _(j):
                for e in range(2):
                    done(vx.at[e, j], xacc_r.at[e, 1 + j])
                    tot = ownx[e, j] + vx[e, j]
                    for i in range(2):
                        dx[x_at(e, j, i)] = tot[:, i * q:(i + 1) * q].astype(BF16)

            done(rx, ring_s.at[0])

        x_half, y_half = (2, NH, cr, 2 * q), (2, NH, qr, f)
        pl.run_scoped(reduce, pltpu.VMEM((2, NC, cr, 2 * q), F32), *[pltpu.VMEM(x_half, F32)] * 4, pltpu.VMEM(x_half, BF16),
                      pltpu.VMEM((2, NC, qr, f), F32), *[pltpu.VMEM(y_half, F32)] * 3)

    dma = pltpu.SemaphoreType.DMA
    pl.run_scoped(rest, dma((2, 2)), dma((1,)), dma((4, 2)), dma((1,)), dma((2, 2, 2)), dma((2, 2)), dma((2, 1 + NH)), dma((2, 2)), dma((2,)), dma((4,)), dma((2,)), dma((2,)), dma((5,)), dma((2,)), dma((2,)))


def put_kernel(a, b, u, v, sems):
    for i, (src, dst) in enumerate(((b, v), (a, u))):
        rows = src.shape[0] // 8
        for n in range(8):
            pltpu.make_async_copy(src.at[pl.ds(n * rows, rows)], dst.at[pl.ds(n * rows, rows)], sems.at[i]).start()
    for i, (src, dst) in enumerate(((b, v), (a, u))):
        pltpu.make_async_copy(src, dst, sems.at[i]).wait()


def solution(mesh):
    spec_act = P(("dp", "ro", "ri"), "co")
    spec_w = P(("ro", "ri"), "co")

    def local_step(x, w, g):
        tb, dcols = x.shape
        wrows, f = w.shape
        q = wrows // 2
        cr, qr = tb // NC, q // NC
        dma = lambda *s: pltpu.SemaphoreType.DMA(s)
        any_ = pl.BlockSpec(memory_space=pl.ANY)
        vmem = pl.BlockSpec(memory_space=pltpu.VMEM)
        shapes = [
            pltpu.VMEM((tb, dcols), BF16),
            pltpu.VMEM((wrows, f), F32),
            jax.ShapeDtypeStruct((4, 2, NC, cr, 2 * q), F32),
            jax.ShapeDtypeStruct((4, 2, NC, qr, f), F32),
            jax.ShapeDtypeStruct((4, 2, 2, tb, q), BF16),
            jax.ShapeDtypeStruct((4, 2, q, f), BF16),
            jax.ShapeDtypeStruct((3, 2, NC, cr, 2 * q), F32),
            jax.ShapeDtypeStruct((3, 2, NC, qr, f), F32),
        ]
        res = pl.pallas_call(
            kernel,
            out_shape=shapes,
            in_specs=[any_] * 3,
            out_specs=[vmem] * 2 + [any_] * (len(shapes) - 2),
            scratch_shapes=[
                pltpu.VMEM((2, NH, cr, 2 * q), F32),
                dma(1), dma(2, 2, 2), pltpu.SemaphoreType.REGULAR, pltpu.SemaphoreType.REGULAR, pltpu.SemaphoreType.REGULAR,
            ],
            compiler_params=pltpu.CompilerParams(collective_id=0, has_side_effects=True, vmem_limit_bytes=52 << 20),
            name="linear_grads",
        )(x, w, g)
        return pl.pallas_call(
            put_kernel,
            out_shape=[jax.ShapeDtypeStruct(r.shape, r.dtype) for r in res[:2]],
            in_specs=[vmem] * 2,
            out_specs=[any_] * 2,
            scratch_shapes=[dma(2)],
            compiler_params=pltpu.CompilerParams(vmem_limit_bytes=16 << 20),
            name="put",
        )(res[0], res[1])

    return jax.shard_map(local_step, mesh=mesh, in_specs=(spec_act, spec_w, spec_act), out_specs=(spec_act, spec_act), check_vma=False)
```

```python
import functools

import jax
import jax.numpy as jnp
from jax import lax
from jax.experimental import pallas as pl
from jax.experimental.pallas import tpu as pltpu
from jax.sharding import PartitionSpec as P

MESH = pl.DeviceIdType.MESH
BF16, F32 = jnp.bfloat16, jnp.float32
NC = 8
NH = NC // 2


def kernel(x, w, g, dx, dw, pp, qq, xa, wa, rx, ry, vx,
           xs, xr, told, inside, ready):
    h, y, c = lax.axis_index("ro"), lax.axis_index("ri"), lax.axis_index("co")
    o = 1 - h
    tb, dcols = x.shape
    wrows, f = w.shape
    q = wrows // 2
    cr, qr = tb // NC, q // NC
    ft = f // 7
    yn = [lax.rem(y + 1, 4), lax.rem(y + 3, 4)]
    cn = [lax.rem(c + 1, 4), lax.rem(c + 3, 4)]
    y2, c2 = lax.rem(y + 2, 4), lax.rem(c + 2, 4)
    sib = {"ro": o}

    def rc(src, dst, ssem, rsem, dev):
        return pltpu.make_async_remote_copy(src_ref=src, dst_ref=dst, send_sem=ssem, recv_sem=rsem, device_id=dev, device_id_type=MESH)

    def lc(src, dst, sem):
        return pltpu.make_async_copy(src, dst, sem)

    def done(ref, sem):
        lc(ref, ref, sem).wait()

    def xor(a, b):
        return 2 * lax.rem(a // 2 + b // 2, 2) + lax.rem(lax.rem(a, 2) + lax.rem(b, 2), 2)

    def xcols(i, k):
        return x.at[:, pl.ds(pl.multiple_of(i * 2 * q + k * q, q), q)]

    def wrow(k):
        return w.at[pl.ds(pl.multiple_of(k * q, q), q)]

    bar = pltpu.get_barrier_semaphore()
    for e in range(2):
        pl.semaphore_signal(bar, 1, device_id={"co": cn[e]}, device_id_type=MESH)
    for e in range(2):
        pl.semaphore_signal(bar, 1, device_id={"ri": yn[e], "ro": 0}, device_id_type=MESH)

    @pl.when(h == 1)
    def _():
        pl.semaphore_signal(bar, 1, device_id=sib, device_id_type=MESH)
        pl.semaphore_wait(bar, 2)

    @pl.when(h == 0)
    def _():
        pl.semaphore_wait(bar, 7)
        pl.semaphore_signal(told, 1, device_id=sib, device_id_type=MESH)

    def x_send(e, k, i):
        return rc(xcols(i, k), xa.at[c, h, i], xs.at[0], xr.at[e, h, i], {"co": cn[e], "ro": k})

    for n in range(2):
        for e in range(2):
            x_send(e, h, n if e == 0 else 1 - n).start()

    pl.semaphore_wait(told, 1)

    @pl.when(h == 1)
    def _():
        pl.semaphore_signal(told, 1, device_id=sib, device_id_type=MESH)

    for n in range(2):
        for e in range(2):
            x_send(e, o, n if e == 0 else 1 - n).start()

    def rest(xf, xd, wr, dr, opp_r, pure_r, xacc_r, yacc_r, fin_r, ss, ring_s, fin, ls, outs, ads):
        senders = [sib] + [{"ri": yn[e], "ro": k} for e in range(2) for k in range(2)] + [{"co": cn[e]} for e in range(2)]
        for dev in senders:
            pl.semaphore_signal(inside, 1, device_id=dev, device_id_type=MESH)
        w_dir = [rc(wrow(k), wa.at[y, h], ss.at[0], wr.at[y, h], {"ri": yn[e], "ro": k}) for n in range(2) for e in range(2) for k in [h if n == e else o]]
        w_d2d = rc(wrow(o), wa.at[y, h], ss.at[2], wr.at[y, h], sib)
        x_d2d = [rc(xcols(i, o), xa.at[c, h, i], ss.at[1], xd.at[0], sib) for i in range(2)]
        pl.semaphore_wait(inside, len(senders))
        for cp in w_dir + [w_d2d] + x_d2d:
            cp.start()

        w_fwd = [rc(wa.at[yn[1 - e], k], wa.at[yn[1 - e], k], ss.at[0], wr.at[yn[1 - e], k], {"ri": yn[e]}) for e, k in ((0, h), (1, o))]
        x_fwd = [rc(xa.at[cn[1 - e], t, e], xa.at[cn[1 - e], t, e], xs.at[0], xf.at[t, e], {"co": cn[e]}) for e in range(2) for t in range(2)]

        def got_w(yy, k):
            done(wa.at[yy, k], wr.at[yy, k])

        def got_x(e, i):
            for t in range(2):
                done(xa.at[cn[1 - e], t, i], xr.at[e, t, i])

        def sends(a, part, recv, me, axis, nbr, d):
            k = lax.rem(d - me + 4, 4)

            @pl.when(k == 2)
            def _():
                for n in range(2):
                    for e in range(2):
                        half = pl.ds(n * NH, NH)
                        rc(part.at[d, e, half], recv.at[0, e, half], ring_s.at[a], opp_r.at[a, e, n], {axis: nbr[e]}).start()

            for e in range(2):
                @pl.when(k == 1 + 2 * e)
                def _():
                    rc(part.at[d, 1 - e], recv.at[1, e], ring_s.at[a], pure_r.at[a, e], {axis: nbr[e]}).start()

        x_sends = functools.partial(sends, 0, pp, rx, c, "co", cn)
        y_sends = functools.partial(sends, 1, qq, ry, y, "ri", yn)

        def compute(gv, wv, xin, xt, pst, qst):
            pl.semaphore_signal(ready, 1, device_id=sib, device_id_type=MESH)
            lc(g, gv.at[h], ls.at[0]).start()
            pl.semaphore_wait(ready, 1)
            rc(g, gv.at[h], ss.at[3], dr.at[0], sib).start()
            for i in range(2):
                lc(xcols(i, h), xin.at[0, i], ls.at[3]).start()

            def p_out(slot, r, yy, m):
                s, ab, hf = 1 - m // 4, lax.rem(m // 2, 2), lax.rem(m, 2)
                return lc(pst.at[slot, r], pp.at[2 * r + yy // 2, ab, pl.ds(s * 4 + hf * 2, 2), :, pl.ds(pl.multiple_of(lax.rem(yy, 2) * q, q), q)], outs.at[slot])

            def load_w(yy, r):
                lc(wa.at[yy, r], wv.at[pl.ds(pl.multiple_of(r * q, q), q)], ls.at[1]).start()

            def p_step(yy):
                done(wv, ls.at[1])

                @pl.loop(0, 8)
                def _(m):
                    s, ab, hf = 1 - m // 4, lax.rem(m // 2, 2), lax.rem(m, 2)
                    t = s * h + (1 - s) * o
                    row = pl.multiple_of(ab * (tb // 2) + hf * (tb // 4), tb // 4)
                    slot = lax.rem(m, 2)

                    @pl.when(m >= 2)
                    def _():
                        done(pst.at[slot], outs.at[slot])

                    res = lax.dot_general(gv[t, pl.ds(row, tb // 4), :], wv[...], (((1,), (1,)), ((), ())), preferred_element_type=F32)
                    for r in range(2):
                        pst[slot, r] = res[:, r * q:(r + 1) * q].reshape(2, cr, q)
                    for r in range(2):
                        p_out(slot, r, yy, m).start()

                for slot in range(2):
                    done(pst.at[slot], outs.at[slot])

            def q_out(slot, r, yy, n):
                s = r * h + (1 - r) * o
                return lc(qst.at[slot, r], qq.at[yy, :, pl.ds(s * 4, 4), :, pl.ds(pl.multiple_of(n * ft, ft), ft)], outs.at[slot])

            def load_x(yy):
                for r in range(2):
                    for t in range(2):
                        lc(xa.at[2 * r + yy // 2, t, lax.rem(yy, 2)], xin.at[r, t], ls.at[4]).start()

            def q_step(yy, yy_next, qn):
                @pl.when(qn < 2)
                def _():
                    load_x(yy)

                done(xin, ls.at[4])

                @pl.loop(0, NC)
                def _(n):
                    at = pl.ds(pl.multiple_of(n * cr, cr), cr)
                    for r in range(2):
                        for t in range(2):
                            xt[t, r * q:(r + 1) * q, at] = xin[r, t, at, :].T

                @pl.when((qn == 1) | (qn == 2))
                def _():
                    load_x(yy_next)

                @pl.loop(0, 7)
                def _(n):
                    slot = lax.rem(n, 2)

                    @pl.when(n >= 2)
                    def _():
                        done(qst.at[slot], outs.at[slot])

                    at = pl.ds(pl.multiple_of(n * ft, ft), ft)
                    res = jnp.dot(xt[0], gv[0, :, at], preferred_element_type=F32)
                    res += jnp.dot(xt[1], gv[1, :, at], preferred_element_type=F32)
                    for r in range(2):
                        qst[slot, r] = res[r * q:(r + 1) * q].reshape(2, 4, qr, ft)
                    for r in range(2):
                        q_out(slot, r, yy, n).start()

                for slot in range(2):
                    done(qst.at[slot], outs.at[slot])

            op = lax.rem(y // 2 + c + 1, 2)

            def qcode(n):
                return op * ((1 - n // 2) * (2 + n) + n // 2 * (3 - n)) + (1 - op) * lax.rem(n + 1, 4)

            even = 1 - lax.rem(y, 2)
            rem1 = even * h + (1 - even) * o

            @pl.loop(0, 8)
            def _(step):
                @pl.when(step == 0)
                def _():
                    lc(wrow(h), wv.at[pl.ds(pl.multiple_of(h * q, q), q)], ls.at[1]).start()
                    got_w(y, o)
                    load_w(y, o)
                    done(gv.at[o], dr.at[0])
                    done(gv.at[h], ls.at[0])

                @pl.when(step == 1)
                def _():
                    done(xin.at[0], ls.at[3])
                    for i in range(2):
                        lc(xin.at[0, i], xa.at[c, h, i], ls.at[3]).start()
                    got_w(yn[1], h)
                    w_fwd[0].start()
                    got_w(yn[0], o)
                    w_fwd[1].start()
                    got_x(0, 0)
                    x_fwd[0].start()
                    x_fwd[1].start()
                    got_x(1, 1)
                    x_fwd[2].start()
                    x_fwd[3].start()
                    load_w(xor(y, 1), 1 - rem1)
                    got_w(xor(y, 1), rem1)
                    load_w(xor(y, 1), rem1)

                @pl.when(step == 2)
                def _():
                    x_sends(y // 2)
                    x_sends(2 + y // 2)
                    got_x(0, 1)
                    got_x(1, 0)
                    done(xin.at[0], ls.at[3])

                @pl.when(step == 3)
                def _():
                    done(xa.at[c, o], xd.at[0])
                    for t in range(2):
                        for i in range(2):
                            done(xa.at[c2, t, i], xf.at[t, i])
                    got_w(3 - y, 1 - rem1)
                    for r in range(2):
                        load_w(3 - y, r)
                        got_w(y2, r)

                @pl.when(step == 6)
                def _():
                    for r in range(2):
                        load_w(y2, r)

                late = step // 5
                is_p = (step < 2) | ((step >= 5) & (step < 7))
                pn = step - 3 * late
                qn = step - 2 - 2 * (step // 7)
                pcode = pn + pn // 2 - 2 * (pn // 3)
                @pl.when(is_p)
                def _():
                    p_step(xor(y, pcode))

                @pl.when(jnp.logical_not(is_p))
                def _():
                    yy = xor(y, qcode(qn))
                    q_step(yy, xor(y, qcode(lax.rem(qn + 1, 4))), qn)
                    y_sends(yy)

                @pl.when(step == 6)
                def _():
                    x_sends(1 - y // 2)
                    x_sends(3 - y // 2)

        pl.run_scoped(compute, pltpu.VMEM((2, tb, f), BF16), pltpu.VMEM((2 * q, f), BF16), pltpu.VMEM((2, 2, tb, q), BF16), pltpu.VMEM((2, 2 * q, tb), BF16),
                      pltpu.VMEM((2, 2, 2, cr, q), F32), pltpu.VMEM((2, 2, 2, 4, qr, ft), F32))

        def reduce(accx, tmpx, nxtx, ownx, sibx, outx, accy, tmpy, nxty, siby):
            rings = ((0, pp, rx, c, cn, "co", accx, tmpx, nxtx), (1, qq, ry, y, yn, "ri", accy, tmpy, nxty))
            low, high = pl.ds(0, NH), pl.ds(NH, NH)

            def x_at(e, j, i):
                return (pl.ds(pl.multiple_of(e * (tb // 2) + j * cr, cr), cr), pl.ds(pl.multiple_of(i * 2 * q + h * q, q), q))

            def y_at(e, j):
                return pl.ds(pl.multiple_of(h * q + e * (q // 2) + j * qr, qr), qr)

            for a, part, recv, me, nbr, axis, acc, tmp, nxt in rings:
                for e in range(2):
                    lc(part.at[nbr[e], e], acc.at[e], ls.at[a]).start()
            for e in range(2):
                lc(pp.at[c, e, low], sibx.at[e], ls.at[2]).start()
                lc(pp.at[c, e, high], ownx.at[e], ls.at[2]).start()
                lc(qq.at[y, e, low], siby.at[e], ls.at[3]).start()
                for j in range(NH):
                    lc(qq.at[y, e, NH + j], dw.at[y_at(e, j)], ls.at[3]).start()

            @pl.loop(0, 2)
            def _(n):
                half = pl.ds(n * NH, NH)
                for a, part, recv, me, nbr, axis, acc, tmp, nxt in rings[::-1]:
                    for e in range(2):
                        done(recv.at[0, e, low], opp_r.at[a, e, n])
                        lc(recv.at[0, e, half], tmp.at[e], ads.at[a]).start()

                @pl.when(n == 0)
                def _():
                    done(accx, ls.at[0])
                    done(accy, ls.at[1])

                for a, part, recv, me, nbr, axis, acc, tmp, nxt in rings:
                    done(tmp, ads.at[a])

                    @pl.loop(0, NH)
                    def _(i):
                        for e in range(2):
                            acc[e, n * NH + i] += tmp[e, i]

                @pl.when(n == 0)
                def _():
                    for e in range(2):
                        rc(accx.at[e, low], rx.at[2, e, low], ring_s.at[0], xacc_r.at[e, 0], {"co": cn[e]}).start()

                @pl.when(n == 1)
                def _():
                    for i in range(NH):
                        for e in range(2):
                            rc(accx.at[e, NH + i], vx.at[e, i], ring_s.at[0], xacc_r.at[e, 1 + i], {"co": cn[e]}).start()

                for e in range(2):
                    rc(accy.at[e, half], ry.at[2, e, half], ring_s.at[1], yacc_r.at[e, n], {"ri": yn[e]}).start()

            for a, part, recv, me, nbr, axis, acc, tmp, nxt in rings[::-1]:
                for e in range(2):
                    done(recv.at[1, e], pure_r.at[a, e])
                for e in range(2):
                    lc(recv.at[1, 1 - e, low], tmp.at[e], ads.at[a]).start()
                    lc(recv.at[1, 1 - e, high], nxt.at[e], ads.at[a]).start()
            done(wa.at[pl.ds(0, 3)], ss.at[0])
            done(xa.at[pl.ds(0, 3)], xs.at[0])
            done(wa.at[0, 0], ss.at[2])
            done(g, ss.at[3])
            done(xa.at[0, 0], ss.at[1])
            done(accx, ls.at[2])
            done(accy, ls.at[3])

            for e in range(2):
                done(ry.at[2, e, low], yacc_r.at[e, 0])
            done(accy, ads.at[1])

            @pl.loop(0, NH)
            def _(i):
                for e in range(2):
                    siby[e, i] += tmpy[e, i]
                    dw[y_at(e, i)] += nxty[e, i]

            for e in range(2):
                lc(ry.at[2, e, low], tmpy.at[e], ads.at[1]).start()
            done(accx, ads.at[0])

            @pl.loop(0, NH)
            def _(i):
                for e in range(2):
                    sibx[e, i] += tmpx[e, i]
                    ownx[e, i] += nxtx[e, i]

            done(tmpy, ads.at[1])

            @pl.loop(0, NH)
            def _(i):
                for e in range(2):
                    siby[e, i] += tmpy[e, i]

            for e in range(2):
                for i in range(NH):
                    rc(siby.at[e, i], dw.at[y_at(e, i)], fin.at[1], fin_r.at[1], sib).start()

            for e in range(2):
                done(rx.at[2, e, low], xacc_r.at[e, 0])
                lc(rx.at[2, e, low], tmpx.at[e], ads.at[0]).start()
            done(tmpx, ads.at[0])

            @pl.loop(0, NH)
            def _(j):
                for e in range(2):
                    outx[e, j] = (sibx[e, j] + tmpx[e, j]).astype(BF16)

            @pl.loop(0, NH)
            def _(j):
                for e in range(2):
                    for i in range(2):
                        rc(outx.at[e, j, :, i * q:(i + 1) * q], dx.at[x_at(e, j, i)], fin.at[0], fin_r.at[0], sib).start()

            for e in range(2):
                done(ry.at[2, e, low], yacc_r.at[e, 1])
                lc(ry.at[2, e, high], tmpy.at[e], ads.at[1]).start()
            done(tmpy, ads.at[1])

            @pl.loop(0, NH)
            def _(j):
                for e in range(2):
                    dw[y_at(e, j)] += tmpy[e, j]

            for n, ref in enumerate((outx, siby)):
                done(ref, fin.at[n])
                done(ref, fin_r.at[n])
            done(ry, ring_s.at[1])

            @pl.loop(0, NH)
            def _(j):
                for e in range(2):
                    done(vx.at[e, j], xacc_r.at[e, 1 + j])
                    tot = ownx[e, j] + vx[e, j]
                    for i in range(2):
                        dx[x_at(e, j, i)] = tot[:, i * q:(i + 1) * q].astype(BF16)

            done(rx, ring_s.at[0])

        x_half, y_half = (2, NH, cr, 2 * q), (2, NH, qr, f)
        pl.run_scoped(reduce, pltpu.VMEM((2, NC, cr, 2 * q), F32), *[pltpu.VMEM(x_half, F32)] * 4, pltpu.VMEM(x_half, BF16),
                      pltpu.VMEM((2, NC, qr, f), F32), *[pltpu.VMEM(y_half, F32)] * 3)

    dma = pltpu.SemaphoreType.DMA
    pl.run_scoped(rest, dma((2, 2)), dma((1,)), dma((4, 2)), dma((1,)), dma((2, 2, 2)), dma((2, 2)), dma((2, 1 + NH)), dma((2, 2)), dma((2,)), dma((4,)), dma((2,)), dma((2,)), dma((5,)), dma((2,)), dma((2,)))


def put_kernel(a, b, u, v, sems):
    for i, (src, dst) in enumerate(((b, v), (a, u))):
        rows = src.shape[0] // 16
        for n in range(16):
            pltpu.make_async_copy(src.at[pl.ds(n * rows, rows)], dst.at[pl.ds(n * rows, rows)], sems.at[i]).start()
    for i, (src, dst) in enumerate(((b, v), (a, u))):
        pltpu.make_async_copy(src, dst, sems.at[i]).wait()


def solution(mesh):
    spec_act = P(("dp", "ro", "ri"), "co")
    spec_w = P(("ro", "ri"), "co")

    def local_step(x, w, g):
        tb, dcols = x.shape
        wrows, f = w.shape
        q = wrows // 2
        cr, qr = tb // NC, q // NC
        dma = lambda *s: pltpu.SemaphoreType.DMA(s)
        any_ = pl.BlockSpec(memory_space=pl.ANY)
        vmem = pl.BlockSpec(memory_space=pltpu.VMEM)
        shapes = [
            pltpu.VMEM((tb, dcols), BF16),
            pltpu.VMEM((wrows, f), F32),
            jax.ShapeDtypeStruct((4, 2, NC, cr, 2 * q), F32),
            jax.ShapeDtypeStruct((4, 2, NC, qr, f), F32),
            jax.ShapeDtypeStruct((4, 2, 2, tb, q), BF16),
            jax.ShapeDtypeStruct((4, 2, q, f), BF16),
            jax.ShapeDtypeStruct((3, 2, NC, cr, 2 * q), F32),
            jax.ShapeDtypeStruct((3, 2, NC, qr, f), F32),
        ]
        res = pl.pallas_call(
            kernel,
            out_shape=shapes,
            in_specs=[any_] * 3,
            out_specs=[vmem] * 2 + [any_] * (len(shapes) - 2),
            scratch_shapes=[
                pltpu.VMEM((2, NH, cr, 2 * q), F32),
                dma(1), dma(2, 2, 2), pltpu.SemaphoreType.REGULAR, pltpu.SemaphoreType.REGULAR, pltpu.SemaphoreType.REGULAR,
            ],
            compiler_params=pltpu.CompilerParams(collective_id=0, has_side_effects=True, vmem_limit_bytes=52 << 20),
            name="linear_grads",
        )(x, w, g)
        return pl.pallas_call(
            put_kernel,
            out_shape=[jax.ShapeDtypeStruct(r.shape, r.dtype) for r in res[:2]],
            in_specs=[vmem] * 2,
            out_specs=[any_] * 2,
            scratch_shapes=[dma(2)],
            compiler_params=pltpu.CompilerParams(vmem_limit_bytes=16 << 20),
            name="put",
        )(res[0], res[1])

    return jax.shard_map(local_step, mesh=mesh, in_specs=(spec_act, spec_w, spec_act), out_specs=(spec_act, spec_act), check_vma=False)
```

```python
import functools

import jax
import jax.numpy as jnp
from jax import lax
from jax.experimental import pallas as pl
from jax.experimental.pallas import tpu as pltpu
from jax.sharding import PartitionSpec as P

MESH = pl.DeviceIdType.MESH
BF16, F32 = jnp.bfloat16, jnp.float32
NC = 8
NH = NC // 2


def kernel(x, w, g, dx, dw, pp, qq, xa, wa, rx, ry, vx,
           xs, xr, told, inside, ready):
    h, y, c = lax.axis_index("ro"), lax.axis_index("ri"), lax.axis_index("co")
    o = 1 - h
    tb, dcols = x.shape
    wrows, f = w.shape
    q = wrows // 2
    cr, qr = tb // NC, q // NC
    ft = f // 7
    yn = [lax.rem(y + 1, 4), lax.rem(y + 3, 4)]
    cn = [lax.rem(c + 1, 4), lax.rem(c + 3, 4)]
    y2, c2 = lax.rem(y + 2, 4), lax.rem(c + 2, 4)
    sib = {"ro": o}

    def rc(src, dst, ssem, rsem, dev):
        return pltpu.make_async_remote_copy(src_ref=src, dst_ref=dst, send_sem=ssem, recv_sem=rsem, device_id=dev, device_id_type=MESH)

    def lc(src, dst, sem):
        return pltpu.make_async_copy(src, dst, sem)

    def done(ref, sem):
        lc(ref, ref, sem).wait()

    def xor(a, b):
        return 2 * lax.rem(a // 2 + b // 2, 2) + lax.rem(lax.rem(a, 2) + lax.rem(b, 2), 2)

    def xcols(i, k):
        return x.at[:, pl.ds(pl.multiple_of(i * 2 * q + k * q, q), q)]

    def wrow(k):
        return w.at[pl.ds(pl.multiple_of(k * q, q), q)]

    bar = pltpu.get_barrier_semaphore()
    for e in range(2):
        pl.semaphore_signal(bar, 1, device_id={"co": cn[e]}, device_id_type=MESH)
    for e in range(2):
        pl.semaphore_signal(bar, 1, device_id={"ri": yn[e], "ro": 0}, device_id_type=MESH)

    @pl.when(h == 1)
    def _():
        pl.semaphore_signal(bar, 1, device_id=sib, device_id_type=MESH)
        pl.semaphore_wait(bar, 2)

    @pl.when(h == 0)
    def _():
        pl.semaphore_wait(bar, 7)
        pl.semaphore_signal(told, 1, device_id=sib, device_id_type=MESH)

    def x_send(e, k, i):
        return rc(xcols(i, k), xa.at[c, h, i], xs.at[0], xr.at[e, h, i], {"co": cn[e], "ro": k})

    for n in range(2):
        for e in range(2):
            x_send(e, h, n if e == 0 else 1 - n).start()

    pl.semaphore_wait(told, 1)

    @pl.when(h == 1)
    def _():
        pl.semaphore_signal(told, 1, device_id=sib, device_id_type=MESH)

    for n in range(2):
        for e in range(2):
            x_send(e, o, n if e == 0 else 1 - n).start()

    def rest(xf, xd, wr, dr, opp_r, pure_r, xacc_r, yacc_r, fin_r, ss, ring_s, fin, ls, outs, ads):
        senders = [sib] + [{"ri": yn[e], "ro": k} for e in range(2) for k in range(2)] + [{"co": cn[e]} for e in range(2)]
        for dev in senders:
            pl.semaphore_signal(inside, 1, device_id=dev, device_id_type=MESH)
        w_dir = [rc(wrow(k), wa.at[y, h], ss.at[0], wr.at[y, h], {"ri": yn[e], "ro": k}) for n in range(2) for e in range(2) for k in [h if n == e else o]]
        w_d2d = rc(wrow(o), wa.at[y, h], ss.at[2], wr.at[y, h], sib)
        x_d2d = [rc(xcols(i, o), xa.at[c, h, i], ss.at[1], xd.at[0], sib) for i in range(2)]
        pl.semaphore_wait(inside, len(senders))
        for cp in w_dir + [w_d2d] + x_d2d:
            cp.start()

        w_fwd = [rc(wa.at[yn[1 - e], k], wa.at[yn[1 - e], k], ss.at[0], wr.at[yn[1 - e], k], {"ri": yn[e]}) for e, k in ((0, h), (1, o))]
        x_fwd = [rc(xa.at[cn[1 - e], t, e], xa.at[cn[1 - e], t, e], xs.at[0], xf.at[t, e], {"co": cn[e]}) for e in range(2) for t in range(2)]

        def got_w(yy, k):
            done(wa.at[yy, k], wr.at[yy, k])

        def got_x(e, i):
            for t in range(2):
                done(xa.at[cn[1 - e], t, i], xr.at[e, t, i])

        def sends(a, part, recv, me, axis, nbr, d):
            k = lax.rem(d - me + 4, 4)

            @pl.when(k == 2)
            def _():
                for n in range(2):
                    for e in range(2):
                        half = pl.ds(n * NH, NH)
                        rc(part.at[d, e, half], recv.at[0, e, half], ring_s.at[a], opp_r.at[a, e, n], {axis: nbr[e]}).start()

            for e in range(2):
                @pl.when(k == 1 + 2 * e)
                def _():
                    rc(part.at[d, 1 - e], recv.at[1, e], ring_s.at[a], pure_r.at[a, e], {axis: nbr[e]}).start()

        x_sends = functools.partial(sends, 0, pp, rx, c, "co", cn)
        y_sends = functools.partial(sends, 1, qq, ry, y, "ri", yn)

        def compute(gv, wv, xin, xt, pst, qst):
            pl.semaphore_signal(ready, 1, device_id=sib, device_id_type=MESH)
            lc(g, gv.at[h], ls.at[0]).start()
            pl.semaphore_wait(ready, 1)
            rc(g, gv.at[h], ss.at[3], dr.at[0], sib).start()
            for i in range(2):
                lc(xcols(i, h), xin.at[0, i], ls.at[3]).start()

            def p_out(slot, r, yy, m):
                s, ab, hf = 1 - m // 4, lax.rem(m // 2, 2), lax.rem(m, 2)
                return lc(pst.at[slot, r], pp.at[2 * r + yy // 2, ab, pl.ds(s * 4 + hf * 2, 2), :, pl.ds(pl.multiple_of(lax.rem(yy, 2) * q, q), q)], outs.at[slot])

            def load_w(yy, r):
                lc(wa.at[yy, r], wv.at[pl.ds(pl.multiple_of(r * q, q), q)], ls.at[1]).start()

            def p_step(yy):
                done(wv, ls.at[1])

                @pl.loop(0, 8)
                def _(m):
                    s, ab, hf = 1 - m // 4, lax.rem(m // 2, 2), lax.rem(m, 2)
                    t = s * h + (1 - s) * o
                    row = pl.multiple_of(ab * (tb // 2) + hf * (tb // 4), tb // 4)
                    slot = lax.rem(m, 2)

                    @pl.when(m >= 2)
                    def _():
                        done(pst.at[slot], outs.at[slot])

                    res = lax.dot_general(gv[t, pl.ds(row, tb // 4), :], wv[...], (((1,), (1,)), ((), ())), preferred_element_type=F32)
                    for r in range(2):
                        pst[slot, r] = res[:, r * q:(r + 1) * q].reshape(2, cr, q)
                    for r in range(2):
                        p_out(slot, r, yy, m).start()

                for slot in range(2):
                    done(pst.at[slot], outs.at[slot])

            def q_out(slot, r, yy, n):
                s = r * h + (1 - r) * o
                return lc(qst.at[slot, r], qq.at[yy, :, pl.ds(s * 4, 4), :, pl.ds(pl.multiple_of(n * ft, ft), ft)], outs.at[slot])

            def load_x(yy):
                for r in range(2):
                    for t in range(2):
                        lc(xa.at[2 * r + yy // 2, t, lax.rem(yy, 2)], xin.at[r, t], ls.at[4]).start()

            def q_step(yy, yy_next, qn):
                @pl.when(qn < 2)
                def _():
                    load_x(yy)

                done(xin, ls.at[4])

                @pl.loop(0, NC)
                def _(n):
                    at = pl.ds(pl.multiple_of(n * cr, cr), cr)
                    for r in range(2):
                        for t in range(2):
                            xt[t, r * q:(r + 1) * q, at] = xin[r, t, at, :].T

                @pl.when((qn == 1) | (qn == 2))
                def _():
                    load_x(yy_next)

                @pl.loop(0, 7)
                def _(n):
                    slot = lax.rem(n, 2)

                    @pl.when(n >= 2)
                    def _():
                        done(qst.at[slot], outs.at[slot])

                    at = pl.ds(pl.multiple_of(n * ft, ft), ft)
                    res = jnp.dot(xt[0], gv[0, :, at], preferred_element_type=F32)
                    res += jnp.dot(xt[1], gv[1, :, at], preferred_element_type=F32)
                    for r in range(2):
                        qst[slot, r] = res[r * q:(r + 1) * q].reshape(2, 4, qr, ft)
                    for r in range(2):
                        q_out(slot, r, yy, n).start()

                for slot in range(2):
                    done(qst.at[slot], outs.at[slot])

            op = lax.rem(y // 2 + c + 1, 2)

            def qcode(n):
                return op * ((1 - n // 2) * (2 + n) + n // 2 * (3 - n)) + (1 - op) * lax.rem(n + 1, 4)

            even = 1 - lax.rem(y, 2)
            rem1 = even * h + (1 - even) * o

            @pl.loop(0, 8)
            def _(step):
                @pl.when(step == 0)
                def _():
                    lc(wrow(h), wv.at[pl.ds(pl.multiple_of(h * q, q), q)], ls.at[1]).start()
                    got_w(y, o)
                    load_w(y, o)
                    done(gv.at[o], dr.at[0])
                    done(gv.at[h], ls.at[0])

                @pl.when(step == 1)
                def _():
                    done(xin.at[0], ls.at[3])
                    for i in range(2):
                        lc(xin.at[0, i], xa.at[c, h, i], ls.at[3]).start()
                    got_w(yn[1], h)
                    w_fwd[0].start()
                    got_w(yn[0], o)
                    w_fwd[1].start()
                    got_x(0, 0)
                    x_fwd[0].start()
                    x_fwd[1].start()
                    got_x(1, 1)
                    x_fwd[2].start()
                    x_fwd[3].start()
                    load_w(xor(y, 1), 1 - rem1)
                    got_w(xor(y, 1), rem1)
                    load_w(xor(y, 1), rem1)

                @pl.when(step == 2)
                def _():
                    x_sends(y // 2)
                    x_sends(2 + y // 2)
                    got_x(0, 1)
                    got_x(1, 0)
                    done(xin.at[0], ls.at[3])

                @pl.when(step == 3)
                def _():
                    done(xa.at[c, o], xd.at[0])
                    for t in range(2):
                        for i in range(2):
                            done(xa.at[c2, t, i], xf.at[t, i])
                    got_w(3 - y, 1 - rem1)
                    for r in range(2):
                        load_w(3 - y, r)
                        got_w(y2, r)

                @pl.when(step == 6)
                def _():
                    for r in range(2):
                        load_w(y2, r)

                late = step // 5
                is_p = (step < 2) | ((step >= 5) & (step < 7))
                pn = step - 3 * late
                qn = step - 2 - 2 * (step // 7)
                pcode = pn + pn // 2 - 2 * (pn // 3)
                @pl.when(is_p)
                def _():
                    p_step(xor(y, pcode))

                @pl.when(jnp.logical_not(is_p))
                def _():
                    yy = xor(y, qcode(qn))
                    q_step(yy, xor(y, qcode(lax.rem(qn + 1, 4))), qn)
                    y_sends(yy)

                @pl.when(step == 6)
                def _():
                    x_sends(1 - y // 2)
                    x_sends(3 - y // 2)

        pl.run_scoped(compute, pltpu.VMEM((2, tb, f), BF16), pltpu.VMEM((2 * q, f), BF16), pltpu.VMEM((2, 2, tb, q), BF16), pltpu.VMEM((2, 2 * q, tb), BF16),
                      pltpu.VMEM((2, 2, 2, cr, q), F32), pltpu.VMEM((2, 2, 2, 4, qr, ft), F32))

        def reduce(accx, tmpx, nxtx, ownx, sibx, outx, accy, tmpy, nxty, siby):
            rings = ((0, pp, rx, c, cn, "co", accx, tmpx, nxtx), (1, qq, ry, y, yn, "ri", accy, tmpy, nxty))
            low, high = pl.ds(0, NH), pl.ds(NH, NH)

            def x_at(e, j, i):
                return (pl.ds(pl.multiple_of(e * (tb // 2) + j * cr, cr), cr), pl.ds(pl.multiple_of(i * 2 * q + h * q, q), q))

            def y_at(e, j):
                return pl.ds(pl.multiple_of(h * q + e * (q // 2) + j * qr, qr), qr)

            for a, part, recv, me, nbr, axis, acc, tmp, nxt in rings:
                for e in range(2):
                    lc(part.at[nbr[e], e], acc.at[e], ls.at[a]).start()
            for e in range(2):
                lc(pp.at[c, e, low], sibx.at[e], ls.at[2]).start()
                lc(pp.at[c, e, high], ownx.at[e], ls.at[2]).start()
                lc(qq.at[y, e, low], siby.at[e], ls.at[3]).start()
                for j in range(NH):
                    lc(qq.at[y, e, NH + j], dw.at[y_at(e, j)], ls.at[3]).start()

            @pl.loop(0, 2)
            def _(n):
                half = pl.ds(n * NH, NH)
                for a, part, recv, me, nbr, axis, acc, tmp, nxt in rings[::-1]:
                    for e in range(2):
                        done(recv.at[0, e, low], opp_r.at[a, e, n])
                        lc(recv.at[0, e, half], tmp.at[e], ads.at[a]).start()

                @pl.when(n == 0)
                def _():
                    done(accx, ls.at[0])
                    done(accy, ls.at[1])

                for a, part, recv, me, nbr, axis, acc, tmp, nxt in rings:
                    done(tmp, ads.at[a])

                    @pl.loop(0, NH)
                    def _(i):
                        for e in range(2):
                            acc[e, n * NH + i] += tmp[e, i]

                @pl.when(n == 0)
                def _():
                    for e in range(2):
                        rc(accx.at[e, low], rx.at[2, e, low], ring_s.at[0], xacc_r.at[e, 0], {"co": cn[e]}).start()

                @pl.when(n == 1)
                def _():
                    for i in range(NH):
                        for e in range(2):
                            rc(accx.at[e, NH + i], vx.at[e, i], ring_s.at[0], xacc_r.at[e, 1 + i], {"co": cn[e]}).start()

                for e in range(2):
                    rc(accy.at[e, half], ry.at[2, e, half], ring_s.at[1], yacc_r.at[e, n], {"ri": yn[e]}).start()

            for a, part, recv, me, nbr, axis, acc, tmp, nxt in rings[::-1]:
                for e in range(2):
                    done(recv.at[1, e], pure_r.at[a, e])
                for e in range(2):
                    lc(recv.at[1, 1 - e, low], tmp.at[e], ads.at[a]).start()
                    lc(recv.at[1, 1 - e, high], nxt.at[e], ads.at[a]).start()
            done(wa.at[pl.ds(0, 3)], ss.at[0])
            done(xa.at[pl.ds(0, 3)], xs.at[0])
            done(wa.at[0, 0], ss.at[2])
            done(g, ss.at[3])
            done(xa.at[0, 0], ss.at[1])
            done(accx, ls.at[2])
            done(accy, ls.at[3])

            for e in range(2):
                done(ry.at[2, e, low], yacc_r.at[e, 0])
            done(accy, ads.at[1])

            @pl.loop(0, NH)
            def _(i):
                for e in range(2):
                    siby[e, i] += tmpy[e, i]
                    dw[y_at(e, i)] += nxty[e, i]

            for e in range(2):
                lc(ry.at[2, e, low], tmpy.at[e], ads.at[1]).start()
            done(accx, ads.at[0])

            @pl.loop(0, NH)
            def _(i):
                for e in range(2):
                    sibx[e, i] += tmpx[e, i]
                    ownx[e, i] += nxtx[e, i]

            done(tmpy, ads.at[1])

            @pl.loop(0, NH)
            def _(i):
                for e in range(2):
                    siby[e, i] += tmpy[e, i]

            for e in range(2):
                for i in range(NH):
                    rc(siby.at[e, i], dw.at[y_at(e, i)], fin.at[1], fin_r.at[1], sib).start()

            for e in range(2):
                done(rx.at[2, e, low], xacc_r.at[e, 0])
                lc(rx.at[2, e, low], tmpx.at[e], ads.at[0]).start()
            done(tmpx, ads.at[0])

            @pl.loop(0, NH)
            def _(j):
                for e in range(2):
                    outx[e, j] = (sibx[e, j] + tmpx[e, j]).astype(BF16)

            @pl.loop(0, NH)
            def _(j):
                for e in range(2):
                    for i in range(2):
                        rc(outx.at[e, j, :, i * q:(i + 1) * q], dx.at[x_at(e, j, i)], fin.at[0], fin_r.at[0], sib).start()

            for e in range(2):
                done(ry.at[2, e, low], yacc_r.at[e, 1])
                lc(ry.at[2, e, high], tmpy.at[e], ads.at[1]).start()
            done(tmpy, ads.at[1])

            @pl.loop(0, NH)
            def _(j):
                for e in range(2):
                    dw[y_at(e, j)] += tmpy[e, j]

            for n, ref in enumerate((outx, siby)):
                done(ref, fin.at[n])
                done(ref, fin_r.at[n])
            done(ry, ring_s.at[1])

            @pl.loop(0, NH)
            def _(j):
                for e in range(2):
                    done(vx.at[e, j], xacc_r.at[e, 1 + j])
                    tot = ownx[e, j] + vx[e, j]
                    for i in range(2):
                        dx[x_at(e, j, i)] = tot[:, i * q:(i + 1) * q].astype(BF16)

            done(rx, ring_s.at[0])

        x_half, y_half = (2, NH, cr, 2 * q), (2, NH, qr, f)
        pl.run_scoped(reduce, pltpu.VMEM((2, NC, cr, 2 * q), F32), *[pltpu.VMEM(x_half, F32)] * 4, pltpu.VMEM(x_half, BF16),
                      pltpu.VMEM((2, NC, qr, f), F32), *[pltpu.VMEM(y_half, F32)] * 3)

    dma = pltpu.SemaphoreType.DMA
    pl.run_scoped(rest, dma((2, 2)), dma((1,)), dma((4, 2)), dma((1,)), dma((2, 2, 2)), dma((2, 2)), dma((2, 1 + NH)), dma((2, 2)), dma((2,)), dma((4,)), dma((2,)), dma((2,)), dma((5,)), dma((2,)), dma((2,)))


def put_kernel(a, b, u, v, sems):
    for i, (src, dst) in enumerate(((b, v), (a, u))):
        rows = src.shape[0] // 32
        for n in range(32):
            pltpu.make_async_copy(src.at[pl.ds(n * rows, rows)], dst.at[pl.ds(n * rows, rows)], sems.at[i]).start()
    for i, (src, dst) in enumerate(((b, v), (a, u))):
        pltpu.make_async_copy(src, dst, sems.at[i]).wait()


def solution(mesh):
    spec_act = P(("dp", "ro", "ri"), "co")
    spec_w = P(("ro", "ri"), "co")

    def local_step(x, w, g):
        tb, dcols = x.shape
        wrows, f = w.shape
        q = wrows // 2
        cr, qr = tb // NC, q // NC
        dma = lambda *s: pltpu.SemaphoreType.DMA(s)
        any_ = pl.BlockSpec(memory_space=pl.ANY)
        vmem = pl.BlockSpec(memory_space=pltpu.VMEM)
        shapes = [
            pltpu.VMEM((tb, dcols), BF16),
            pltpu.VMEM((wrows, f), F32),
            jax.ShapeDtypeStruct((4, 2, NC, cr, 2 * q), F32),
            jax.ShapeDtypeStruct((4, 2, NC, qr, f), F32),
            jax.ShapeDtypeStruct((4, 2, 2, tb, q), BF16),
            jax.ShapeDtypeStruct((4, 2, q, f), BF16),
            jax.ShapeDtypeStruct((3, 2, NC, cr, 2 * q), F32),
            jax.ShapeDtypeStruct((3, 2, NC, qr, f), F32),
        ]
        res = pl.pallas_call(
            kernel,
            out_shape=shapes,
            in_specs=[any_] * 3,
            out_specs=[vmem] * 2 + [any_] * (len(shapes) - 2),
            scratch_shapes=[
                pltpu.VMEM((2, NH, cr, 2 * q), F32),
                dma(1), dma(2, 2, 2), pltpu.SemaphoreType.REGULAR, pltpu.SemaphoreType.REGULAR, pltpu.SemaphoreType.REGULAR,
            ],
            compiler_params=pltpu.CompilerParams(collective_id=0, has_side_effects=True, vmem_limit_bytes=52 << 20),
            name="linear_grads",
        )(x, w, g)
        return pl.pallas_call(
            put_kernel,
            out_shape=[jax.ShapeDtypeStruct(r.shape, r.dtype) for r in res[:2]],
            in_specs=[vmem] * 2,
            out_specs=[any_] * 2,
            scratch_shapes=[dma(2)],
            compiler_params=pltpu.CompilerParams(vmem_limit_bytes=16 << 20),
            name="put",
        )(res[0], res[1])

    return jax.shard_map(local_step, mesh=mesh, in_specs=(spec_act, spec_w, spec_act), out_specs=(spec_act, spec_act), check_vma=False)
```
